128 devices in a mesh: sub: 32 (over z, y, core), rve: 4 (over x).
Axes of the slice: x: 4, y: 4, z: 4, core: 2. Of those that a mesh axis runs over, the one named last changes fastest.
Arguments:
- displacement: float32 [3, 32, 8, 8], P(None, 'sub', 'rve'), may hold values from -4 to 4
- load: float32 [3, 32, 8, 8], P(None, 'sub', 'rve'), may hold values from -6 to 6
- home_slot: int32 [16384], P(('sub', 'rve')), may hold values from 0 to 16383, as said below
- micro_state: float32 [7, 3, 216, 16384], P(None, None, None, ('sub', 'rve')), may hold values from -6 to 6
- state_slot: int32 [16384], P(('sub', 'rve')), may hold values from 0 to 16383, as said below
- phases: int32 [216, 16384], P(None, ('sub', 'rve')), may hold values from 0 to 2
- phase_moduli: float32 [2, 3], replicated, may hold values from 0.5 to 8
Outputs:
- new_state: float32 [7, 3, 216, 16384], P(None, None, None, ('sub', 'rve'))
- displaced: float32 [3, 32, 8, 8], P(None, 'sub', 'rve')
- residual: float32 [3, 32, 8, 8], P(None, 'sub', 'rve')
- rel_norm: float32 [], replicated
The draws below stay inside these ranges and needn't reach their ends.
Inputs may be any that keep to these rules, and one draw needn't show every extreme that they name: `home_slot`: A permutation of 0 to 16383. The 128 entries held by device s (devices numbered in sub+rve order) contain, for every device d, exactly one value, d * 128 + s, in an order drawn at random; so each device sends exactly one Gauss point to every device. `state_slot`: A permutation of 0 to 16383 with the same structure: the 128 entries held by device s contain, for every device d, exactly one value, d * 128 + s, in an order drawn at random.
All inputs are finite; a program needn't handle non-finite values.
Results may differ from the reference program's by a relative error of at most 0.0003.
Values sent between devices are 32-bit elements; how exact they have to be, the bound alone decides.
No kernel may reach another device: no remote copies, remote signals or barrier semaphores. Data moves between devices by JAX's collectives and lax.ppermute only.
A program may use at most 128 MiB of HBM per device.

```python
import math
import jax
import jax.numpy as jnp
import numpy as np
from jax import lax

R = 6
V = 216
CASES = 7
CG_STEPS = 2
NPH = 3
MX = 8
LY = 2
LZ = 1
GP_DEV = 128
PAIR = 1
GPS = 16384
NX = 8
NY = 8
NZ = 32
N_SUB = 32
N_RVE = 4


def slot_law(key):
    device_count = GPS // GP_DEV
    keys = jax.random.split(key, device_count)
    orders = jax.vmap(lambda single: jax.random.permutation(single, GP_DEV))(keys)
    source = jnp.arange(device_count, dtype=jnp.int32)[:, None]
    target = orders // PAIR
    within = orders % PAIR
    return (target * GP_DEV + source * PAIR + within).reshape(-1).astype(jnp.int32)


def draw_home_slot(key, part):
    return slot_law(jax.random.fold_in(key, 11))


def draw_state_slot(key, part):
    return slot_law(jax.random.fold_in(key, 23))


def plant(array, rng, low, largest):
    longest = array.shape.index(max(array.shape))
    spots = []
    for shift in (0, 1):
        where = [jax.random.randint(jax.random.fold_in(rng, axis), (), 0, length) for axis, length in enumerate(array.shape)]
        where[longest] = (where[longest] + shift) % array.shape[longest]
        spots.append(tuple(where))
    return array.at[spots[0]].set(low).at[spots[1]].set(largest)


def level_of(own_key, extent, shards, low, high):
    def one(position, shards_of):
        draws = jax.random.uniform(jax.random.fold_in(jax.random.fold_in(own_key, 6), position), (shards_of,), jnp.float32, low / len(shards), high / len(shards))
        return jnp.repeat(jnp.exp(draws), extent[position] // shards_of).reshape((-1,) + (1,) * (len(extent) - position - 1))

    level = one(*shards[0])
    for cut in shards[1:]:
        level = level * one(*cut)
    return level


def bell_draw(rng, shape, scale, most, shards=(), kind=jnp.bfloat16):
    entries = jax.random.normal(rng, shape, jnp.float32) * scale
    if len(shards) > 0:
        entries = level_of(rng, shape, shards, -0.22, 0.18) * entries
    return jnp.clip(entries, min=-most, max=most).astype(kind)


def setup_inputs(seed: int = 0) -> dict:
    seeds = jax.random.split(jax.random.key(seed), 8)
    displacement = bell_draw(seeds[0], (3, NZ, NY, NX), 0.3, 4.0, ((1, 32), (2, 4)), jnp.float32)
    load = bell_draw(seeds[1], (3, NZ, NY, NX), 1.0, 6.0, ((1, 32), (2, 4)), jnp.float32)
    home_slot = draw_home_slot(jax.random.fold_in(seeds[7], 71), 0)
    micro_state = bell_draw(seeds[3], (CASES, 3, V, GPS), 0.5, 6.0, ((3, 128),), jnp.float32)
    state_slot = draw_state_slot(jax.random.fold_in(seeds[7], 71), 0)
    phases = plant(jax.random.randint(seeds[5], (V, GPS), 0, NPH), jax.random.fold_in(seeds[5], 1), 0, NPH - 1).astype(jnp.int32)
    phase_moduli = jnp.clip(jnp.exp(jax.random.uniform(seeds[6], (2, NPH), jnp.float32, math.log(0.5), math.log(8.0))), 0.5, 8.0)
    return dict(displacement=displacement, load=load, home_slot=home_slot, micro_state=micro_state, state_slot=state_slot, phases=phases, phase_moduli=phase_moduli)


STAB = 0.1
FLOOR = 1.0
voigt_pairs = ((0, 5, 4), (5, 1, 3), (4, 3, 2))
HIGHEST = lax.Precision.HIGHEST

def shape_tables():
    offset = 0.5 / math.sqrt(3.0)
    places = (0.5 - offset, 0.5 + offset)
    slope_table = np.zeros((8, 8, 3))
    for gauss_point in range(8):
        coords = (places[gauss_point % 2], places[gauss_point // 2 % 2], places[gauss_point // 4])
        for corner in range(8):
            corner_bits = (corner % 2, corner // 2 % 2, corner // 4)
            weights = [coords[direction] if corner_bits[direction] == 1 else 1.0 - coords[direction] for direction in range(3)]
            slopes = [1.0 if corner_bits[direction] == 1 else -1.0 for direction in range(3)]
            slope_table[gauss_point, corner, 0] = slopes[0] * weights[1] * weights[2]
            slope_table[gauss_point, corner, 1] = weights[0] * slopes[1] * weights[2]
            slope_table[gauss_point, corner, 2] = weights[0] * weights[1] * slopes[2]
    strain_table = np.zeros((8, 8, 3, 6))
    strain_table[:, :, 0, 0] = slope_table[:, :, 0]
    strain_table[:, :, 0, 4] = slope_table[:, :, 2]
    strain_table[:, :, 0, 5] = slope_table[:, :, 1]
    strain_table[:, :, 1, 1] = slope_table[:, :, 1]
    strain_table[:, :, 1, 3] = slope_table[:, :, 2]
    strain_table[:, :, 1, 5] = slope_table[:, :, 0]
    strain_table[:, :, 2, 2] = slope_table[:, :, 2]
    strain_table[:, :, 2, 3] = slope_table[:, :, 1]
    strain_table[:, :, 2, 4] = slope_table[:, :, 0]
    outer_table = strain_table[:, :, :, :, None] * strain_table[:, :, :, None, :]
    return (jnp.asarray(strain_table, jnp.float32), jnp.asarray(outer_table, jnp.float32))

def voxel_moduli(phases, phase_moduli):
    batch_size = phases.shape[1]
    onehot = (phases[None, :, :] == jnp.arange(NPH, dtype=jnp.int32)[:, None, None]).astype(jnp.float32)
    lame_first = lax.optimization_barrier(jnp.sum(onehot * phase_moduli[0][:, None, None], axis=0))
    lame_second = lax.optimization_barrier(jnp.sum(onehot * phase_moduli[1][:, None, None], axis=0))
    return (lame_first.reshape(R, R, R, batch_size), lame_second.reshape(R, R, R, batch_size))

def micro_stress(voxel_field, imposed, lame_first, lame_second):
    gradients = [[jnp.roll(voxel_field[:, component], -1, axis=1 + direction) - voxel_field[:, component] for direction in range(3)] for component in range(3)]
    strains = []
    for voigt_index, axis_pair in enumerate(((0, 0), (1, 1), (2, 2), (1, 2), (0, 2), (0, 1))):
        left_axis, right_axis = axis_pair
        applied = imposed[:, voigt_index][:, None, None, None, :]
        if left_axis == right_axis:
            strains.append(gradients[left_axis][left_axis] + applied)
        else:
            strains.append(0.5 * (gradients[left_axis][right_axis] + gradients[right_axis][left_axis] + applied))
    volume_change = strains[0] + strains[1] + strains[2]
    stresses = []
    for voigt_index in range(6):
        shear_part = 2.0 * lame_second * strains[voigt_index]
        if voigt_index < 3:
            stresses.append(lame_first * volume_change + shear_part)
        else:
            stresses.append(shear_part)
    return stresses

def divergence(stresses):
    columns_out = []
    for component in range(3):
        summed = 0.0
        for direction in range(3):
            member = stresses[voigt_pairs[direction][component]]
            summed = summed + (jnp.roll(member, 1, axis=1 + direction) - member)
        columns_out.append(summed)
    return jnp.stack(columns_out, axis=1)

def micro_solve(field, imposed, lame_first, lame_second):
    case_count = field.shape[0]
    voxels = field.shape[2]
    batch_size = field.shape[3]
    voxel_field = field.reshape(case_count, 3, R, R, R, batch_size)
    zero_strain = jnp.zeros_like(imposed)

    def apply_force(values, strain):
        return divergence(micro_stress(values, strain, lame_first, lame_second)) + STAB * values
    remainder = -apply_force(voxel_field, imposed)
    search = remainder
    square_sum = lax.optimization_barrier(jnp.sum(remainder * remainder, axis=(1, 2, 3, 4)))
    for step_number in range(CG_STEPS):
        operator_image = apply_force(search, zero_strain)
        curvature = lax.optimization_barrier(jnp.sum(search * operator_image, axis=(1, 2, 3, 4)))
        step_size = (square_sum / curvature)[:, None, None, None, None, :]
        voxel_field = voxel_field + step_size * search
        remainder = remainder - step_size * operator_image
        next_square = lax.optimization_barrier(jnp.sum(remainder * remainder, axis=(1, 2, 3, 4)))
        search = remainder + (next_square / square_sum)[:, None, None, None, None, :] * search
        square_sum = next_square
    stresses = micro_stress(voxel_field, imposed, lame_first, lame_second)
    averaged = jnp.stack([lax.optimization_barrier(jnp.mean(member, axis=(1, 2, 3))) for member in stresses], axis=1)
    return (voxel_field.reshape(case_count, 3, voxels, batch_size), averaged)

def assemble_global(corner_terms):
    summed = jnp.zeros((3, NZ + 1, NY, NX), jnp.float32)
    for corner in range(8):
        shifted = jnp.roll(jnp.roll(corner_terms[corner], corner // 2 % 2, axis=2), corner % 2, axis=3)
        summed = summed.at[:, corner // 4:corner // 4 + NZ].add(shifted)
    return summed[:, :NZ]

def reference(displacement, load, home_slot, micro_state, state_slot, phases, phase_moduli):
    strain_table, outer_table = shape_tables()
    padded = jnp.concatenate([displacement, jnp.zeros((3, 1, NY, NX), jnp.float32)], axis=1)
    corners = jnp.stack([jnp.roll(jnp.roll(padded[:, corner // 4:corner // 4 + NZ], -(corner // 2 % 2), axis=2), -(corner % 2), axis=3) for corner in range(8)])
    gauss_strain = jnp.einsum('qaim,aizyx->qmzyx', strain_table, corners, precision=HIGHEST)
    macro_strain = gauss_strain.reshape(8, 6, N_SUB, LZ, N_RVE, LY, MX).transpose(1, 2, 4, 3, 5, 6, 0).reshape(6, GPS)
    unit_cases = jnp.broadcast_to(jnp.eye(6, dtype=jnp.float32)[:, :, None], (6, 6, GPS))
    imposed = jnp.concatenate([macro_strain[None], unit_cases], axis=0)
    counting = jnp.arange(GPS, dtype=jnp.int32)
    from_home = jnp.zeros((GPS,), jnp.int32).at[home_slot].set(counting)
    from_state = jnp.zeros((GPS,), jnp.int32).at[state_slot].set(counting)
    imposed_slot = imposed[:, :, from_home]

    def solve_block(block_index):
        offset_rows = block_index * GP_DEV
        chosen = lax.dynamic_slice_in_dim(from_state, offset_rows, GP_DEV)
        start_field = jnp.take(micro_state, chosen, axis=3)
        block_imposed = lax.dynamic_slice_in_dim(imposed_slot, offset_rows, GP_DEV, axis=2)
        block_phases = lax.dynamic_slice_in_dim(phases, offset_rows, GP_DEV, axis=1)
        lame_first, lame_second = voxel_moduli(block_phases, phase_moduli)
        return micro_solve(start_field, block_imposed, lame_first, lame_second)
    fields, averaged = lax.map(solve_block, jnp.arange(N_SUB * N_RVE, dtype=jnp.int32))
    new_state = fields.transpose(1, 2, 3, 0, 4).reshape(CASES, 3, V, GPS)
    averaged = averaged.transpose(1, 2, 0, 3).reshape(CASES, 6, GPS)
    at_home = averaged[:, :, home_slot]
    stress = at_home[0].reshape(6, N_SUB, N_RVE, LZ, LY, MX, 8).transpose(0, 6, 1, 3, 2, 4, 5).reshape(6, 8, NZ, NY, NX)
    tangent = at_home[1:].transpose(1, 0, 2).reshape(6, 6, N_SUB, N_RVE, LZ, LY, MX, 8)
    tangent = tangent.transpose(0, 1, 7, 2, 4, 3, 5, 6).reshape(6, 6, 8, NZ, NY, NX)
    force_corner = 0.125 * jnp.einsum('qaim,mqzyx->aizyx', strain_table, stress, precision=HIGHEST)
    diag_corner = 0.125 * jnp.einsum('qaimn,mnqzyx->aizyx', outer_table, tangent, precision=HIGHEST)
    force_int = assemble_global(force_corner)
    stiff_diag = assemble_global(diag_corner)
    residual = load - force_int
    displaced = displacement + residual / jnp.maximum(stiff_diag, FLOOR)
    rel_norm = jnp.sqrt(jnp.sum(residual * residual) / jnp.sum(load * load))
    return (new_state, displaced, residual, rel_norm)
```

```python
import math

import jax
import jax.numpy as jnp
import numpy as np
from jax import lax
from jax.experimental import pallas as pl
from jax.experimental.pallas import tpu as pltpu
from jax.sharding import PartitionSpec as P

R = 6
VOX = R * R * R
ROWS = 3 * VOX
CASES = 7
DEV = 128
LANES = 128
CHUNKS = 36
WIDE = CHUNKS * LANES
TAIL = CASES * ROWS - (CHUNKS - 1) * LANES
NODES = 48
STAB = 0.1
FLOOR = 1.0
AXES = ("sub", "rve")
PAIRS = ((0, 5, 4), (5, 1, 3), (4, 3, 2))
STRAIN_OF = ((0, 4, 5), (5, 1, 3), (4, 3, 2))
OFF_DIAGONAL = ((0, 4), (0, 5), (4, 5), (1, 3), (1, 5), (3, 5), (2, 3), (2, 4), (3, 4))
LOW = 0.5 - 0.5 / math.sqrt(3.0)
HIGH = 0.5 + 0.5 / math.sqrt(3.0)
HIGHEST = lax.Precision.HIGHEST
VMEM = pl.BlockSpec(memory_space=pltpu.VMEM)
SMEM = pl.BlockSpec(memory_space=pltpu.SMEM)


def strain_table():
    places = (LOW, HIGH)
    table = np.zeros((8, 8, 3, 6))
    for gauss in range(8):
        at = (places[gauss % 2], places[gauss // 2 % 2], places[gauss // 4])
        for corner in range(8):
            bits = (corner % 2, corner // 2 % 2, corner // 4)
            weight = [at[k] if bits[k] else 1.0 - at[k] for k in range(3)]
            sign = [1.0 if bits[k] else -1.0 for k in range(3)]
            dx = sign[0] * weight[1] * weight[2]
            dy = weight[0] * sign[1] * weight[2]
            dz = weight[0] * weight[1] * sign[2]
            table[gauss, corner, 0, [0, 4, 5]] = (dx, dz, dy)
            table[gauss, corner, 1, [1, 3, 5]] = (dy, dz, dx)
            table[gauss, corner, 2, [2, 3, 4]] = (dz, dy, dx)
    return table


def term_index(first, second):
    if first == second:
        return first
    return 6 + OFF_DIAGONAL.index((min(first, second), max(first, second)))


def diagonal_terms(component):
    m = STRAIN_OF[component]
    pairs = [(m[0], m[0]), (m[1], m[1]), (m[2], m[2]), (m[0], m[1]), (m[0], m[2]), (m[1], m[2])]
    return [(a, b, term_index(a, b)) for a, b in pairs]


def assembly_tables():
    table = strain_table()
    force = np.zeros((6, LANES, 2 * LANES), np.float32)
    weights = np.zeros((3, 6, 8, LANES), np.float32)
    place = np.zeros((4, LANES, LANES), np.float32)
    for j in range(LANES):
        ly, ex, gauss = j // 64, j // 8 % 8, j % 8
        for corner in range(8):
            az, row, col = corner // 4, ly + corner // 2 % 2, (ex + corner % 2) % 8
            for i in range(3):
                lane = az * LANES + (NODES if row == 2 else 0) + i * 16 + row % 2 * 8 + col
                for m in STRAIN_OF[i]:
                    force[m, j, lane] += 0.125 * table[gauss, corner, i, m]
                for n, (first, second, _) in enumerate(diagonal_terms(i)):
                    weights[i, n, corner, j] = (
                        0.125 * table[gauss, corner, i, first] * table[gauss, corner, i, second]
                    )
            place[az * 2 + (1 if row == 2 else 0), j, corner * 16 + row % 2 * 8 + col] = 1.0
    return force.reshape(6 * LANES, 2 * LANES), weights.reshape(18 * 8, LANES), place


def lane_iota(rows=1):
    return lax.broadcasted_iota(jnp.int32, (rows, LANES), 1)


def sublane_iota(rows=8):
    return lax.broadcasted_iota(jnp.int32, (rows, LANES), 0)


def node_row(ref, scratch, offset):
    scratch[...] = jnp.zeros((8, LANES), jnp.float32)
    for i in range(3):
        scratch[2 * i : 2 * i + 2, 0:8] = ref[i, 0]
    tile = scratch[...]
    total = jnp.zeros((1, LANES), jnp.float32)
    for row in range(6):
        total = total + pltpu.roll(tile[row : row + 1], offset + 8 * row, 1)
    return total


def previous_row_lanes(value):
    lane = lane_iota(value.shape[0])
    return jnp.where(lane % 4 == 0, pltpu.roll(value, LANES - 3, 1), pltpu.roll(value, 1, 1))


def next_row_lanes(value):
    lane = lane_iota(value.shape[0])
    return jnp.where(lane % 4 == 3, pltpu.roll(value, 3, 1), pltpu.roll(value, LANES - 1, 1))


def below_lanes(value):
    return jnp.where(lane_iota(value.shape[0]) < 4, 0.0, pltpu.roll(value, 4, 1))


def above_lanes(value):
    return jnp.where(lane_iota(value.shape[0]) >= 124, 0.0, pltpu.roll(value, LANES - 4, 1))


def pack_kernel(state_ref, state_slot_ref, home_slot_ref, disp_ref, out_ref, scratch):
    owner = sublane_iota(DEV)
    lane = lane_iota(DEV)
    chosen = (state_slot_ref[...] >> 7) == owner
    choose = chosen.astype(jnp.float32)
    for k in range(CHUNKS):
        if k < CHUNKS - 1:
            block = state_ref[k * LANES : (k + 1) * LANES, :]
        else:
            block = jnp.concatenate(
                [
                    state_ref[k * LANES : k * LANES + TAIL, :],
                    jnp.zeros((LANES - TAIL, LANES), jnp.float32),
                ],
                axis=0,
            )
        turned = lax.dot_general(
            choose,
            block,
            (((1,), (1,)), ((), ())),
            precision=HIGHEST,
            preferred_element_type=jnp.float32,
        )
        if k == CHUNKS - 1:
            home = (home_slot_ref[...] >> 7) == owner
            local = jnp.sum(jnp.where(home, lane, 0).astype(jnp.float32), axis=1, keepdims=True)
            extra = node_row(disp_ref, scratch, TAIL)
            turned = turned + extra + jnp.where(lane == TAIL + NODES, local, 0.0)
        out_ref[:, 0, k * LANES : (k + 1) * LANES] = turned


def macro_strain_rows(tail):
    local = tail[TAIL + NODES : TAIL + NODES + 1].astype(jnp.int32)
    upper = (local >> 6) == 1
    ex = (local >> 3) & 7
    point = [jnp.where(((local >> k) & 1) == 1, HIGH, LOW) for k in range(3)]
    shape = [(1.0 - point[k], point[k]) for k in range(3)]
    sub = sublane_iota()
    hits = (sub == ex, sub == ((ex + 1) & 7))
    slopes = []
    for i in range(3):
        own = [tail[TAIL + 16 * i + 8 * y : TAIL + 16 * i + 8 * y + 8] for y in range(2)]
        rows = [own[0], own[1], next_row_lanes(own[0])]
        planes = [rows, [above_lanes(row) for row in rows]]
        at = {}
        for az in range(2):
            for ay in range(2):
                chosen = jnp.where(upper, planes[az][ay + 1], planes[az][ay])
                for ax in range(2):
                    at[az, ay, ax] = jnp.sum(
                        jnp.where(hits[ax], chosen, 0.0), axis=0, keepdims=True
                    )
        sx, sy, sz = shape
        slope = [0.0, 0.0, 0.0]
        for first in range(2):
            for second in range(2):
                slope[0] = slope[0] + sz[first] * sy[second] * (
                    at[first, second, 1] - at[first, second, 0]
                )
                slope[1] = slope[1] + sz[first] * sx[second] * (
                    at[first, 1, second] - at[first, 0, second]
                )
                slope[2] = slope[2] + sy[first] * sx[second] * (
                    at[1, first, second] - at[0, first, second]
                )
        slopes.append(slope)
    return [
        slopes[0][0],
        slopes[1][1],
        slopes[2][2],
        slopes[1][2] + slopes[2][1],
        slopes[0][2] + slopes[2][0],
        slopes[0][1] + slopes[1][0],
    ]


def tile_at(ref, base, row):
    return ref[pl.ds(base + row * 8, 8), :]


def solve_kernel(
    recv_ref,
    phase_ref,
    moduli_ref,
    slot_ref,
    load_ref,
    ret_ref,
    w_ref,
    p_ref,
    q_ref,
    step_ref,
    sig_ref,
    lam_ref,
    mu_ref,
    mu2_ref,
    scratch,
):
    zero = jnp.zeros((8, LANES), jnp.float32)
    phase = phase_ref[...]
    mu = jnp.where(
        phase == 0, moduli_ref[1, 0], jnp.where(phase == 1, moduli_ref[1, 1], moduli_ref[1, 2])
    )
    lam_ref[...] = jnp.where(
        phase == 0, moduli_ref[0, 0], jnp.where(phase == 1, moduli_ref[0, 1], moduli_ref[0, 2])
    )
    mu_ref[...] = mu
    mu2_ref[...] = mu + mu
    w_ref[pl.ds(7, ROWS, stride=8), :] = jnp.zeros((ROWS, LANES), jnp.float32)
    tail = None
    for k in range(CHUNKS):
        turned = recv_ref[:, 0, k * LANES : (k + 1) * LANES].T
        start, stop = k * LANES, min((k + 1) * LANES, CASES * ROWS)
        while start < stop:
            case = start // ROWS
            end = min(stop, (case + 1) * ROWS)
            w_ref[pl.ds((start - case * ROWS) * 8 + case, end - start, stride=8), :] = turned[
                start - k * LANES : end - k * LANES
            ]
            start = end
        tail = turned
    macro = macro_strain_rows(tail)
    sub = sublane_iota()
    imposed = [
        jnp.where(sub == 0, macro[m], jnp.where(sub == m + 1, 1.0, 0.0)) for m in range(6)
    ]

    def stress_pass(src, strain, keep, energy):
        def plane(a, carry):
            sums, work = list(carry[0]), carry[1]
            base = pl.multiple_of(a * 288, 8)
            ahead = pl.multiple_of(jnp.where(a == R - 1, 0, (a + 1) * 288), 8)
            voxel = a * 36
            line = [[tile_at(src, base, i * VOX + c) for c in range(R)] for i in range(3)]
            for b in range(R):
                nb = (b + 1) % R
                below = [
                    [tile_at(src, base, i * VOX + nb * R + c) for c in range(R)] for i in range(3)
                ]
                for c in range(R):
                    at = b * R + c
                    here = [line[i][c] for i in range(3)]
                    grad = [
                        [
                            tile_at(src, ahead, i * VOX + at) - here[i],
                            below[i][c] - here[i],
                            line[i][(c + 1) % R] - here[i],
                        ]
                        for i in range(3)
                    ]
                    eps = [
                        grad[0][0],
                        grad[1][1],
                        grad[2][2],
                        grad[1][2] + grad[2][1],
                        grad[0][2] + grad[2][0],
                        grad[0][1] + grad[1][0],
                    ]
                    if strain is not None:
                        eps = [eps[m] + strain[m] for m in range(6)]
                    lam = lam_ref[pl.ds(voxel + at, 8, stride=0), :]
                    mu1 = mu_ref[pl.ds(voxel + at, 8, stride=0), :]
                    mu2 = mu2_ref[pl.ds(voxel + at, 8, stride=0), :]
                    bulk = lam * (eps[0] + eps[1] + eps[2])
                    sig = [bulk + mu2 * eps[m] for m in range(3)]
                    sig += [mu1 * eps[m] for m in range(3, 6)]
                    for m in range(6):
                        sums[m] = sums[m] + sig[m]
                        if keep:
                            sig_ref[pl.ds(base + (m * VOX + at) * 8, 8), :] = sig[m]
                    if energy:
                        work = work + (
                            (sig[0] * eps[0] + sig[1] * eps[1])
                            + (sig[2] * eps[2] + sig[3] * eps[3])
                            + (sig[4] * eps[4] + sig[5] * eps[5])
                        )
                line = below
            return tuple(sums), work

        return lax.fori_loop(0, R, plane, ((zero,) * 6, zero))

    def force_pass(src, finish, dst):
        def plane(a, total):
            base = pl.multiple_of(a * 288, 8)
            behind = pl.multiple_of(jnp.where(a == 0, (R - 1) * 288, (a - 1) * 288), 8)
            for b in range(R):
                pb = (b + R - 1) % R
                last = [tile_at(sig_ref, base, PAIRS[2][i] * VOX + b * R + R - 1) for i in range(3)]
                for c in range(R):
                    at = b * R + c
                    own = [tile_at(sig_ref, base, m * VOX + at) for m in range(6)]
                    for i in range(3):
                        gone = (own[PAIRS[0][i]] + own[PAIRS[1][i]]) + own[PAIRS[2][i]]
                        come = (
                            tile_at(sig_ref, behind, PAIRS[0][i] * VOX + at)
                            + tile_at(sig_ref, base, PAIRS[1][i] * VOX + pb * R + c)
                        ) + last[i]
                        value = finish(come - gone, tile_at(src, base, i * VOX + at))
                        dst[pl.ds(base + (i * VOX + at) * 8, 8), :] = value
                        total = total + value * value
                    last = [own[PAIRS[2][i]] for i in range(3)]
            return total

        return lax.fori_loop(0, R, plane, zero)

    mean0, _ = stress_pass(w_ref, imposed, True, False)
    square0 = force_pass(w_ref, lambda div, w: -(div + STAB * w), p_ref)
    mean1, work1 = stress_pass(p_ref, None, True, True)
    step0 = square0 / (work1 + STAB * square0)
    square1 = force_pass(p_ref, lambda div, p: p - step0 * (div + STAB * p), q_ref)
    ratio = square1 / square0

    def direction(a, total):
        base = pl.multiple_of(a * 288, 8)
        for i in range(3):
            for at in range(36):
                value = tile_at(q_ref, base, i * VOX + at) + ratio * tile_at(
                    p_ref, base, i * VOX + at
                )
                q_ref[pl.ds(base + (i * VOX + at) * 8, 8), :] = value
                total = total + value * value
        return total

    length = lax.fori_loop(0, R, direction, zero)
    mean2, work2 = stress_pass(q_ref, None, False, True)
    step1 = square1 / (work2 + STAB * length)
    step_ref[0:8, :] = step0
    step_ref[8:16, :] = step1
    mean = [(mean0[m] + step0 * mean1[m] + step1 * mean2[m]) * (1.0 / VOX) for m in range(6)]

    shared = (slot_ref[...] >> 7).astype(jnp.float32)
    shared = jnp.broadcast_to(shared, (8, LANES))
    for m in range(6):
        shared = jnp.where(sub == m, mean[m][0:1], shared)
    terms = [mean[m][m + 1 : m + 2] for m in range(6)]
    for first, second in OFF_DIAGONAL:
        terms.append(mean[first][second + 1 : second + 2] + mean[second][first + 1 : first + 2])
    own = jnp.concatenate(terms + [jnp.zeros((1, LANES), jnp.float32)], axis=0)
    left = previous_row_lanes(own)
    stacked = jnp.concatenate(
        [jnp.zeros((64, LANES), jnp.float32), own, left, below_lanes(own), below_lanes(left)],
        axis=0,
    )
    special = stacked.T + node_row(load_ref, scratch, 0)
    for peer in range(DEV):
        ret_ref[8 * peer : 8 * peer + 8, :] = shared
    ret_ref[pl.ds(7, DEV, stride=8), :] = special


def update_kernel(w_ref, p_ref, q_ref, step_ref, out_ref):
    for case in range(CASES):
        first = step_ref[case : case + 1, :]
        second = step_ref[8 + case : 9 + case, :]
        for start in range(0, ROWS, 72):
            rows = pl.ds(start * 8 + case, 72, stride=8)
            out_ref[case * ROWS + start : case * ROWS + start + 72, :] = (
                w_ref[rows, :] + first * p_ref[rows, :] + second * q_ref[rows, :]
            )


def row_of(value, index):
    return jnp.sum(jnp.where(sublane_iota(DEV) == index, value, 0), axis=0, keepdims=True)


def node_tile(row):
    sub = sublane_iota()
    wide = jnp.broadcast_to(row, (8, LANES))
    tile = wide
    for r in range(1, 6):
        tile = jnp.where(sub == r, pltpu.roll(wide, LANES - 8 * r, 1), tile)
    return tile


def final_kernel(
    recv_ref,
    me_ref,
    disp_ref,
    force_ref,
    weight_ref,
    place_ref,
    new_disp_ref,
    res_ref,
    norm_ref,
    scratch,
):
    me = me_ref[0, 0]
    order = recv_ref[pl.ds(6, DEV, stride=8), :].astype(jnp.int32)
    special = recv_ref[pl.ds(7, DEV, stride=8), :]
    stress = [
        jnp.take_along_axis(recv_ref[pl.ds(m, DEV, stride=8), :].T, order, axis=1)
        for m in range(6)
    ]
    forces = lax.dot_general(
        jnp.concatenate(stress, axis=1),
        force_ref[...],
        (((1,), (0,)), ((), ())),
        precision=HIGHEST,
        preferred_element_type=jnp.float32,
    )
    home = sublane_iota(DEV)
    lifted = jnp.where(home < 4, 0.0, pltpu.roll(forces[:, LANES:], 4, 0))
    near = forces[:, :LANES] + lifted
    beside = jnp.where(home % 4 == 0, pltpu.roll(near, DEV - 3, 0), pltpu.roll(near, 1, 0))
    force = near + pltpu.roll(beside, LANES - NODES, 1)
    node = lane_iota(DEV) < NODES
    loads = jnp.where(node, special, 0.0)
    residual = jnp.where(node, special - force, 0.0)
    top = jnp.sum(jnp.sum(residual * residual, axis=0, keepdims=True), axis=1, keepdims=True)
    bottom = jnp.sum(jnp.sum(loads * loads, axis=0, keepdims=True), axis=1, keepdims=True)
    norm_ref[...] = jnp.sqrt(top / bottom)

    own_residual = row_of(residual, me)
    left = jnp.where(me % 4 == 0, me + 3, me - 1)
    under = jnp.where(me < 4, 0, 4)
    turned = special.T
    diagonal = jnp.zeros((24, LANES), jnp.float32)
    for k, source in enumerate((me, left, me - under, left - under)):
        picks = jnp.broadcast_to(row_of(order, source), (16, LANES))
        terms = jnp.take_along_axis(turned[64 + 16 * k : 80 + 16 * k], picks, axis=1)
        corner = []
        for i in range(3):
            total = jnp.zeros((8, LANES), jnp.float32)
            for n, (_, _, t) in enumerate(diagonal_terms(i)):
                at = (i * 6 + n) * 8
                total = total + weight_ref[at : at + 8, :] * terms[t : t + 1]
            corner.append(total)
        diagonal = diagonal + lax.dot_general(
            jnp.concatenate(corner, axis=0),
            place_ref[k],
            (((1,), (0,)), ((), ())),
            precision=HIGHEST,
            preferred_element_type=jnp.float32,
        )
    lane = lane_iota(8)
    same = lane // 16 == sublane_iota()
    row = jnp.zeros((1, LANES), jnp.float32)
    for i in range(3):
        part = jnp.sum(jnp.where(same, diagonal[8 * i : 8 * i + 8], 0.0), axis=0, keepdims=True)
        for shift in (64, 32, 16):
            part = part + pltpu.roll(part, shift, 1)
        row = jnp.where(lane_iota() // 16 == i, part, row)
    moved = node_row(disp_ref, scratch, 0) + own_residual / jnp.maximum(row, FLOOR)
    for value, ref in ((moved, new_disp_ref), (own_residual, res_ref)):
        tile = node_tile(value)
        for i in range(3):
            ref[i, 0] = tile[2 * i : 2 * i + 2, 0:8]


def exchange(value):
    return lax.all_to_all(value, AXES, split_axis=0, concat_axis=0, tiled=True)


def per_device(displacement, load, home_slot, micro_state, state_slot, phases, phase_moduli):
    force_table, weight_table, place_table = assembly_tables()
    f32 = jnp.float32
    home_row = home_slot.reshape(1, LANES)
    sent = pl.pallas_call(
        pack_kernel,
        out_shape=jax.ShapeDtypeStruct((DEV, 1, WIDE), f32),
        in_specs=[VMEM] * 4,
        out_specs=VMEM,
        scratch_shapes=[pltpu.VMEM((8, LANES), f32)],
        name="pack",
    )(
        micro_state.reshape(CASES * ROWS, LANES),
        state_slot.reshape(1, LANES),
        home_row,
        displacement,
    )
    received = exchange(sent)
    big = jax.ShapeDtypeStruct((ROWS * 8, LANES), f32)
    answer, w, p, q, steps = pl.pallas_call(
        solve_kernel,
        out_shape=(
            jax.ShapeDtypeStruct((DEV * 8, LANES), f32),
            big,
            big,
            big,
            jax.ShapeDtypeStruct((16, LANES), f32),
        ),
        in_specs=[VMEM, VMEM, SMEM, VMEM, VMEM],
        out_specs=[VMEM] * 5,
        scratch_shapes=[
            pltpu.VMEM((6 * VOX * 8, LANES), f32),
            pltpu.VMEM((VOX, LANES), f32),
            pltpu.VMEM((VOX, LANES), f32),
            pltpu.VMEM((VOX, LANES), f32),
            pltpu.VMEM((8, LANES), f32),
        ],
        name="solve",
    )(received, phases, phase_moduli, home_row, load)
    returned = exchange(answer.reshape(DEV, 8, LANES)).reshape(DEV * 8, LANES)
    new_state = pl.pallas_call(
        update_kernel,
        out_shape=jax.ShapeDtypeStruct((CASES * ROWS, LANES), f32),
        in_specs=[VMEM] * 4,
        out_specs=VMEM,
        cost_estimate=pl.CostEstimate(
            flops=20_000_000, bytes_accessed=10_000_000, transcendentals=0
        ),
        name="update",
    )(w, p, q, steps)
    me = lax.axis_index(AXES).astype(jnp.int32).reshape(1, 1)
    node_shape = jax.ShapeDtypeStruct(displacement.shape, f32)
    displaced, residual, rel_norm = pl.pallas_call(
        final_kernel,
        out_shape=(node_shape, node_shape, jax.ShapeDtypeStruct((1, 1), f32)),
        in_specs=[VMEM, SMEM, VMEM, VMEM, VMEM, VMEM],
        out_specs=[VMEM] * 3,
        scratch_shapes=[pltpu.VMEM((8, LANES), f32)],
        name="final",
    )(
        returned,
        me,
        displacement,
        jnp.asarray(force_table),
        jnp.asarray(weight_table),
        jnp.asarray(place_table),
    )
    return (
        new_state.reshape(micro_state.shape),
        displaced,
        residual,
        rel_norm.reshape(()),
    )


def solution(mesh):
    return jax.shard_map(
        per_device,
        mesh=mesh,
        in_specs=(
            P(None, "sub", "rve", None),
            P(None, "sub", "rve", None),
            P(AXES),
            P(None, None, None, AXES),
            P(AXES),
            P(None, AXES),
            P(),
        ),
        out_specs=(
            P(None, None, None, AXES),
            P(None, "sub", "rve", None),
            P(None, "sub", "rve", None),
            P(),
        ),
        check_vma=False,
    )
```

```python
import math

import jax
import jax.numpy as jnp
import numpy as np
from jax import lax
from jax.experimental import pallas as pl
from jax.experimental.pallas import tpu as pltpu
from jax.sharding import PartitionSpec as P

R = 6
VOX = R * R * R
ROWS = 3 * VOX
CASES = 7
DEV = 128
LANES = 128
CHUNKS = 36
WIDE = CHUNKS * LANES
TAIL = CASES * ROWS - (CHUNKS - 1) * LANES
NODES = 48
STAB = 0.1
FLOOR = 1.0
AXES = ("sub", "rve")
PAIRS = ((0, 5, 4), (5, 1, 3), (4, 3, 2))
STRAIN_OF = ((0, 4, 5), (5, 1, 3), (4, 3, 2))
OFF_DIAGONAL = ((0, 4), (0, 5), (4, 5), (1, 3), (1, 5), (3, 5), (2, 3), (2, 4), (3, 4))
LOW = 0.5 - 0.5 / math.sqrt(3.0)
HIGH = 0.5 + 0.5 / math.sqrt(3.0)
HIGHEST = lax.Precision.HIGHEST
VMEM = pl.BlockSpec(memory_space=pltpu.VMEM)
SMEM = pl.BlockSpec(memory_space=pltpu.SMEM)
HBM = pl.BlockSpec(memory_space=pltpu.HBM)
PARTS = 6
UPDATE = 72
PART_ROWS = CHUNKS // PARTS * LANES


def strain_table():
    places = (LOW, HIGH)
    table = np.zeros((8, 8, 3, 6))
    for gauss in range(8):
        at = (places[gauss % 2], places[gauss // 2 % 2], places[gauss // 4])
        for corner in range(8):
            bits = (corner % 2, corner // 2 % 2, corner // 4)
            weight = [at[k] if bits[k] else 1.0 - at[k] for k in range(3)]
            sign = [1.0 if bits[k] else -1.0 for k in range(3)]
            dx = sign[0] * weight[1] * weight[2]
            dy = weight[0] * sign[1] * weight[2]
            dz = weight[0] * weight[1] * sign[2]
            table[gauss, corner, 0, [0, 4, 5]] = (dx, dz, dy)
            table[gauss, corner, 1, [1, 3, 5]] = (dy, dz, dx)
            table[gauss, corner, 2, [2, 3, 4]] = (dz, dy, dx)
    return table


def term_index(first, second):
    if first == second:
        return first
    return 6 + OFF_DIAGONAL.index((min(first, second), max(first, second)))


def diagonal_terms(component):
    m = STRAIN_OF[component]
    pairs = [(m[0], m[0]), (m[1], m[1]), (m[2], m[2]), (m[0], m[1]), (m[0], m[2]), (m[1], m[2])]
    return [(a, b, term_index(a, b)) for a, b in pairs]


def assembly_tables():
    table = strain_table()
    force = np.zeros((6, LANES, 2 * LANES), np.float32)
    weights = np.zeros((3, 6, 8, LANES), np.float32)
    place = np.zeros((4, LANES, LANES), np.float32)
    for j in range(LANES):
        ly, ex, gauss = j // 64, j // 8 % 8, j % 8
        for corner in range(8):
            az, row, col = corner // 4, ly + corner // 2 % 2, (ex + corner % 2) % 8
            for i in range(3):
                lane = az * LANES + (NODES if row == 2 else 0) + i * 16 + row % 2 * 8 + col
                for m in STRAIN_OF[i]:
                    force[m, j, lane] += 0.125 * table[gauss, corner, i, m]
                for n, (first, second, _) in enumerate(diagonal_terms(i)):
                    weights[i, n, corner, j] = (
                        0.125 * table[gauss, corner, i, first] * table[gauss, corner, i, second]
                    )
            place[az * 2 + (1 if row == 2 else 0), j, corner * 16 + row % 2 * 8 + col] = 1.0
    return force.reshape(6 * LANES, 2 * LANES), weights.reshape(18 * 8, LANES), place


def lane_iota(rows=1):
    return lax.broadcasted_iota(jnp.int32, (rows, LANES), 1)


def sublane_iota(rows=8):
    return lax.broadcasted_iota(jnp.int32, (rows, LANES), 0)


def node_row(ref, scratch, offset):
    scratch[...] = jnp.zeros((8, LANES), jnp.float32)
    for i in range(3):
        scratch[2 * i : 2 * i + 2, 0:8] = ref[i, 0]
    tile = scratch[...]
    total = jnp.zeros((1, LANES), jnp.float32)
    for row in range(6):
        total = total + pltpu.roll(tile[row : row + 1], offset + 8 * row, 1)
    return total


def previous_row_lanes(value):
    lane = lane_iota(value.shape[0])
    return jnp.where(lane % 4 == 0, pltpu.roll(value, LANES - 3, 1), pltpu.roll(value, 1, 1))


def next_row_lanes(value):
    lane = lane_iota(value.shape[0])
    return jnp.where(lane % 4 == 3, pltpu.roll(value, 3, 1), pltpu.roll(value, LANES - 1, 1))


def below_lanes(value):
    return jnp.where(lane_iota(value.shape[0]) < 4, 0.0, pltpu.roll(value, 4, 1))


def above_lanes(value):
    return jnp.where(lane_iota(value.shape[0]) >= 124, 0.0, pltpu.roll(value, LANES - 4, 1))


def part_copy(src, dst, sems, part):
    rows = pl.ds(part * PART_ROWS, min(PART_ROWS, CASES * ROWS - part * PART_ROWS))
    return pltpu.make_async_copy(src.at[rows], dst.at[rows], sems.at[part])


def split_bf16(value):
    high = value.astype(jnp.bfloat16)
    rest = value - high.astype(jnp.float32)
    middle = rest.astype(jnp.bfloat16)
    low = (rest - middle.astype(jnp.float32)).astype(jnp.bfloat16)
    return high, middle, low


def turn(choose, block):
    high, middle, low = (
        lax.dot_general(
            choose, part, (((1,), (1,)), ((), ())), preferred_element_type=jnp.float32
        )
        for part in split_bf16(block)
    )
    return (high + middle) + low


def pack_kernel(
    state_ref, state_slot_ref, home_slot_ref, disp_ref, out_ref, held_ref, scratch, sems
):
    for part in range(PARTS):
        part_copy(state_ref, held_ref, sems, part).start()
    owner = sublane_iota(DEV)
    lane = lane_iota(DEV)
    choose = ((state_slot_ref[...] >> 7) == owner).astype(jnp.float32).astype(jnp.bfloat16)
    home = (home_slot_ref[...] >> 7) == owner
    local = jnp.sum(jnp.where(home, lane, 0).astype(jnp.float32), axis=1, keepdims=True)
    extra = node_row(disp_ref, scratch, TAIL) + jnp.where(lane == TAIL + NODES, local, 0.0)
    held_ref[CASES * ROWS :, :] = jnp.zeros((WIDE - CASES * ROWS, LANES), jnp.float32)
    for part in range(PARTS):
        part_copy(state_ref, held_ref, sems, part).wait()
        for k in range(part * CHUNKS // PARTS, (part + 1) * CHUNKS // PARTS):
            turned = turn(choose, held_ref[k * LANES : (k + 1) * LANES, :])
            if k == CHUNKS - 1:
                turned = turned + extra
            out_ref[:, 0, k * LANES : (k + 1) * LANES] = turned


def macro_strain_rows(tail):
    local = tail[TAIL + NODES : TAIL + NODES + 1].astype(jnp.int32)
    upper = (local >> 6) == 1
    ex = (local >> 3) & 7
    point = [jnp.where(((local >> k) & 1) == 1, HIGH, LOW) for k in range(3)]
    shape = [(1.0 - point[k], point[k]) for k in range(3)]
    sub = sublane_iota()
    hits = (sub == ex, sub == ((ex + 1) & 7))
    slopes = []
    for i in range(3):
        own = [tail[TAIL + 16 * i + 8 * y : TAIL + 16 * i + 8 * y + 8] for y in range(2)]
        rows = [own[0], own[1], next_row_lanes(own[0])]
        planes = [rows, [above_lanes(row) for row in rows]]
        at = {}
        for az in range(2):
            for ay in range(2):
                chosen = jnp.where(upper, planes[az][ay + 1], planes[az][ay])
                for ax in range(2):
                    at[az, ay, ax] = jnp.sum(
                        jnp.where(hits[ax], chosen, 0.0), axis=0, keepdims=True
                    )
        sx, sy, sz = shape
        slope = [0.0, 0.0, 0.0]
        for first in range(2):
            for second in range(2):
                slope[0] = slope[0] + sz[first] * sy[second] * (
                    at[first, second, 1] - at[first, second, 0]
                )
                slope[1] = slope[1] + sz[first] * sx[second] * (
                    at[first, 1, second] - at[first, 0, second]
                )
                slope[2] = slope[2] + sy[first] * sx[second] * (
                    at[1, first, second] - at[0, first, second]
                )
        slopes.append(slope)
    return [
        slopes[0][0],
        slopes[1][1],
        slopes[2][2],
        slopes[1][2] + slopes[2][1],
        slopes[0][2] + slopes[2][0],
        slopes[0][1] + slopes[1][0],
    ]


def tile_at(ref, base, row):
    return ref[pl.ds(base + row * 8, 8), :]


def solve_kernel(
    recv_ref,
    phase_ref,
    moduli_ref,
    slot_ref,
    load_ref,
    ret_ref,
    w_out,
    p_out,
    q_out,
    step_ref,
    w_ref,
    p_ref,
    q_ref,
    sig_ref,
    lam_ref,
    mu_ref,
    mu2_ref,
    scratch,
    sems,
):
    saves = [
        pltpu.make_async_copy(src, dst, sems.at[k])
        for k, (src, dst) in enumerate(((w_ref, w_out), (p_ref, p_out), (q_ref, q_out)))
    ]
    zero = jnp.zeros((8, LANES), jnp.float32)
    phase = phase_ref[...]
    mu = jnp.where(
        phase == 0, moduli_ref[1, 0], jnp.where(phase == 1, moduli_ref[1, 1], moduli_ref[1, 2])
    )
    lam_ref[...] = jnp.where(
        phase == 0, moduli_ref[0, 0], jnp.where(phase == 1, moduli_ref[0, 1], moduli_ref[0, 2])
    )
    mu_ref[...] = mu
    mu2_ref[...] = mu + mu
    w_ref[pl.ds(7, ROWS, stride=8), :] = jnp.zeros((ROWS, LANES), jnp.float32)
    tail = None
    for k in range(CHUNKS):
        turned = recv_ref[:, 0, k * LANES : (k + 1) * LANES].T
        start, stop = k * LANES, min((k + 1) * LANES, CASES * ROWS)
        while start < stop:
            case = start // ROWS
            end = min(stop, (case + 1) * ROWS)
            w_ref[pl.ds((start - case * ROWS) * 8 + case, end - start, stride=8), :] = turned[
                start - k * LANES : end - k * LANES
            ]
            start = end
        tail = turned
    saves[0].start()
    macro = macro_strain_rows(tail)
    sub = sublane_iota()
    imposed = [
        jnp.where(sub == 0, macro[m], jnp.where(sub == m + 1, 1.0, 0.0)) for m in range(6)
    ]

    def stress_pass(src, strain, keep, energy):
        def plane(a, carry):
            sums, work = list(carry[0]), carry[1]
            base = pl.multiple_of(a * 288, 8)
            ahead = pl.multiple_of(jnp.where(a == R - 1, 0, (a + 1) * 288), 8)
            voxel = a * 36
            line = [[tile_at(src, base, i * VOX + c) for c in range(R)] for i in range(3)]
            for b in range(R):
                nb = (b + 1) % R
                below = [
                    [tile_at(src, base, i * VOX + nb * R + c) for c in range(R)] for i in range(3)
                ]
                for c in range(R):
                    at = b * R + c
                    here = [line[i][c] for i in range(3)]
                    grad = [
                        [
                            tile_at(src, ahead, i * VOX + at) - here[i],
                            below[i][c] - here[i],
                            line[i][(c + 1) % R] - here[i],
                        ]
                        for i in range(3)
                    ]
                    eps = [
                        grad[0][0],
                        grad[1][1],
                        grad[2][2],
                        grad[1][2] + grad[2][1],
                        grad[0][2] + grad[2][0],
                        grad[0][1] + grad[1][0],
                    ]
                    if strain is not None:
                        eps = [eps[m] + strain[m] for m in range(6)]
                    lam = lam_ref[pl.ds(voxel + at, 8, stride=0), :]
                    mu1 = mu_ref[pl.ds(voxel + at, 8, stride=0), :]
                    mu2 = mu2_ref[pl.ds(voxel + at, 8, stride=0), :]
                    bulk = lam * (eps[0] + eps[1] + eps[2])
                    sig = [bulk + mu2 * eps[m] for m in range(3)]
                    sig += [mu1 * eps[m] for m in range(3, 6)]
                    for m in range(6):
                        sums[m] = sums[m] + sig[m]
                        if keep:
                            sig_ref[pl.ds(base + (m * VOX + at) * 8, 8), :] = sig[m]
                    if energy:
                        work = work + (
                            (sig[0] * eps[0] + sig[1] * eps[1])
                            + (sig[2] * eps[2] + sig[3] * eps[3])
                            + (sig[4] * eps[4] + sig[5] * eps[5])
                        )
                line = below
            return tuple(sums), work

        return lax.fori_loop(0, R, plane, ((zero,) * 6, zero))

    def force_pass(src, finish, dst):
        def plane(a, total):
            base = pl.multiple_of(a * 288, 8)
            behind = pl.multiple_of(jnp.where(a == 0, (R - 1) * 288, (a - 1) * 288), 8)
            for b in range(R):
                pb = (b + R - 1) % R
                last = [tile_at(sig_ref, base, PAIRS[2][i] * VOX + b * R + R - 1) for i in range(3)]
                for c in range(R):
                    at = b * R + c
                    own = [tile_at(sig_ref, base, m * VOX + at) for m in range(6)]
                    for i in range(3):
                        gone = (own[PAIRS[0][i]] + own[PAIRS[1][i]]) + own[PAIRS[2][i]]
                        come = (
                            tile_at(sig_ref, behind, PAIRS[0][i] * VOX + at)
                            + tile_at(sig_ref, base, PAIRS[1][i] * VOX + pb * R + c)
                        ) + last[i]
                        value = finish(come - gone, tile_at(src, base, i * VOX + at))
                        dst[pl.ds(base + (i * VOX + at) * 8, 8), :] = value
                        total = total + value * value
                    last = [own[PAIRS[2][i]] for i in range(3)]
            return total

        return lax.fori_loop(0, R, plane, zero)

    mean0, _ = stress_pass(w_ref, imposed, True, False)
    square0 = force_pass(w_ref, lambda div, w: -(div + STAB * w), p_ref)
    saves[1].start()
    mean1, work1 = stress_pass(p_ref, None, True, True)
    step0 = square0 / (work1 + STAB * square0)
    square1 = force_pass(p_ref, lambda div, p: p - step0 * (div + STAB * p), q_ref)
    ratio = square1 / square0

    def direction(a, total):
        base = pl.multiple_of(a * 288, 8)
        for i in range(3):
            for at in range(36):
                value = tile_at(q_ref, base, i * VOX + at) + ratio * tile_at(
                    p_ref, base, i * VOX + at
                )
                q_ref[pl.ds(base + (i * VOX + at) * 8, 8), :] = value
                total = total + value * value
        return total

    length = lax.fori_loop(0, R, direction, zero)
    saves[2].start()
    mean2, work2 = stress_pass(q_ref, None, False, True)
    step1 = square1 / (work2 + STAB * length)
    step_ref[0:8, :] = step0
    step_ref[8:16, :] = step1
    mean = [(mean0[m] + step0 * mean1[m] + step1 * mean2[m]) * (1.0 / VOX) for m in range(6)]

    shared = (slot_ref[...] >> 7).astype(jnp.float32)
    shared = jnp.broadcast_to(shared, (8, LANES))
    for m in range(6):
        shared = jnp.where(sub == m, mean[m][0:1], shared)
    terms = [mean[m][m + 1 : m + 2] for m in range(6)]
    for first, second in OFF_DIAGONAL:
        terms.append(mean[first][second + 1 : second + 2] + mean[second][first + 1 : first + 2])
    own = jnp.concatenate(terms + [jnp.zeros((1, LANES), jnp.float32)], axis=0)
    left = previous_row_lanes(own)
    stacked = jnp.concatenate(
        [jnp.zeros((64, LANES), jnp.float32), own, left, below_lanes(own), below_lanes(left)],
        axis=0,
    )
    special = stacked.T + node_row(load_ref, scratch, 0)
    for peer in range(DEV):
        ret_ref[8 * peer : 8 * peer + 8, :] = shared
    ret_ref[pl.ds(7, DEV, stride=8), :] = special
    for save in saves:
        save.wait()


def update_kernel(w_ref, p_ref, q_ref, step_ref, out_ref):
    for case in range(CASES):
        first = step_ref[case : case + 1, :]
        second = step_ref[8 + case : 9 + case, :]
        rows = pl.ds(case, UPDATE, stride=8)
        out_ref[case] = w_ref[rows, :] + first * p_ref[rows, :] + second * q_ref[rows, :]


def row_of(value, index):
    return jnp.sum(jnp.where(sublane_iota(DEV) == index, value, 0), axis=0, keepdims=True)


def node_tile(row):
    sub = sublane_iota()
    wide = jnp.broadcast_to(row, (8, LANES))
    tile = wide
    for r in range(1, 6):
        tile = jnp.where(sub == r, pltpu.roll(wide, LANES - 8 * r, 1), tile)
    return tile


def final_kernel(
    recv_ref,
    me_ref,
    disp_ref,
    force_ref,
    weight_ref,
    place_ref,
    new_disp_ref,
    res_ref,
    norm_ref,
    scratch,
):
    me = me_ref[0, 0]
    order = recv_ref[pl.ds(6, DEV, stride=8), :].astype(jnp.int32)
    special = recv_ref[pl.ds(7, DEV, stride=8), :]
    stress = [
        jnp.take_along_axis(recv_ref[pl.ds(m, DEV, stride=8), :].T, order, axis=1)
        for m in range(6)
    ]
    forces = lax.dot_general(
        jnp.concatenate(stress, axis=1),
        force_ref[...],
        (((1,), (0,)), ((), ())),
        precision=HIGHEST,
        preferred_element_type=jnp.float32,
    )
    home = sublane_iota(DEV)
    lifted = jnp.where(home < 4, 0.0, pltpu.roll(forces[:, LANES:], 4, 0))
    near = forces[:, :LANES] + lifted
    beside = jnp.where(home % 4 == 0, pltpu.roll(near, DEV - 3, 0), pltpu.roll(near, 1, 0))
    force = near + pltpu.roll(beside, LANES - NODES, 1)
    node = lane_iota(DEV) < NODES
    loads = jnp.where(node, special, 0.0)
    residual = jnp.where(node, special - force, 0.0)
    top = jnp.sum(jnp.sum(residual * residual, axis=0, keepdims=True), axis=1, keepdims=True)
    bottom = jnp.sum(jnp.sum(loads * loads, axis=0, keepdims=True), axis=1, keepdims=True)
    norm_ref[...] = jnp.sqrt(top / bottom)

    own_residual = row_of(residual, me)
    left = jnp.where(me % 4 == 0, me + 3, me - 1)
    under = jnp.where(me < 4, 0, 4)
    turned = special.T
    diagonal = jnp.zeros((24, LANES), jnp.float32)
    for k, source in enumerate((me, left, me - under, left - under)):
        picks = jnp.broadcast_to(row_of(order, source), (16, LANES))
        terms = jnp.take_along_axis(turned[64 + 16 * k : 80 + 16 * k], picks, axis=1)
        corner = []
        for i in range(3):
            total = jnp.zeros((8, LANES), jnp.float32)
            for n, (_, _, t) in enumerate(diagonal_terms(i)):
                at = (i * 6 + n) * 8
                total = total + weight_ref[at : at + 8, :] * terms[t : t + 1]
            corner.append(total)
        diagonal = diagonal + lax.dot_general(
            jnp.concatenate(corner, axis=0),
            place_ref[k],
            (((1,), (0,)), ((), ())),
            precision=HIGHEST,
            preferred_element_type=jnp.float32,
        )
    lane = lane_iota(8)
    same = lane // 16 == sublane_iota()
    row = jnp.zeros((1, LANES), jnp.float32)
    for i in range(3):
        part = jnp.sum(jnp.where(same, diagonal[8 * i : 8 * i + 8], 0.0), axis=0, keepdims=True)
        for shift in (64, 32, 16):
            part = part + pltpu.roll(part, shift, 1)
        row = jnp.where(lane_iota() // 16 == i, part, row)
    moved = node_row(disp_ref, scratch, 0) + own_residual / jnp.maximum(row, FLOOR)
    for value, ref in ((moved, new_disp_ref), (own_residual, res_ref)):
        tile = node_tile(value)
        for i in range(3):
            ref[i, 0] = tile[2 * i : 2 * i + 2, 0:8]


def exchange(value):
    return lax.all_to_all(value, AXES, split_axis=0, concat_axis=0, tiled=True)


def per_device(displacement, load, home_slot, micro_state, state_slot, phases, phase_moduli):
    force_table, weight_table, place_table = assembly_tables()
    f32 = jnp.float32
    home_row = home_slot.reshape(1, LANES)
    sent = pl.pallas_call(
        pack_kernel,
        out_shape=jax.ShapeDtypeStruct((DEV, 1, WIDE), f32),
        in_specs=[HBM] + [VMEM] * 3,
        out_specs=VMEM,
        scratch_shapes=[
            pltpu.VMEM((WIDE, LANES), f32),
            pltpu.VMEM((8, LANES), f32),
            pltpu.SemaphoreType.DMA((PARTS,)),
        ],
        compiler_params=pltpu.CompilerParams(vmem_limit_bytes=12 << 20),
        name="pack",
    )(
        pltpu.with_memory_space_constraint(
            micro_state.reshape(CASES * ROWS, LANES), pltpu.HBM
        ),
        state_slot.reshape(1, LANES),
        home_row,
        displacement,
    )
    received = exchange(sent)
    big = pltpu.HBM((ROWS * 8, LANES), f32)
    answer, w, p, q, steps = pl.pallas_call(
        solve_kernel,
        out_shape=(
            jax.ShapeDtypeStruct((DEV * 8, LANES), f32),
            big,
            big,
            big,
            jax.ShapeDtypeStruct((16, LANES), f32),
        ),
        in_specs=[VMEM, VMEM, SMEM, VMEM, VMEM],
        out_specs=[VMEM, HBM, HBM, HBM, VMEM],
        scratch_shapes=[
            pltpu.VMEM((ROWS * 8, LANES), f32),
            pltpu.VMEM((ROWS * 8, LANES), f32),
            pltpu.VMEM((ROWS * 8, LANES), f32),
            pltpu.VMEM((6 * VOX * 8, LANES), f32),
            pltpu.VMEM((VOX, LANES), f32),
            pltpu.VMEM((VOX, LANES), f32),
            pltpu.VMEM((VOX, LANES), f32),
            pltpu.VMEM((8, LANES), f32),
            pltpu.SemaphoreType.DMA((3,)),
        ],
        compiler_params=pltpu.CompilerParams(vmem_limit_bytes=32 << 20),
        name="solve",
    )(received, phases, phase_moduli, home_row, load)
    returned = exchange(answer.reshape(DEV, 8, LANES)).reshape(DEV * 8, LANES)
    new_state = pl.pallas_call(
        update_kernel,
        out_shape=jax.ShapeDtypeStruct((CASES, ROWS, LANES), f32),
        grid=(ROWS // UPDATE,),
        in_specs=[pl.BlockSpec((UPDATE * 8, LANES), lambda k: (k, 0))] * 3
        + [pl.BlockSpec((16, LANES), lambda k: (0, 0))],
        out_specs=pl.BlockSpec((CASES, UPDATE, LANES), lambda k: (0, k, 0)),
        compiler_params=pltpu.CompilerParams(vmem_limit_bytes=8 << 20),
        cost_estimate=pl.CostEstimate(
            flops=20_000_000, bytes_accessed=10_000_000, transcendentals=0
        ),
        name="update",
    )(w, p, q, steps)
    me = lax.axis_index(AXES).astype(jnp.int32).reshape(1, 1)
    node_shape = jax.ShapeDtypeStruct(displacement.shape, f32)
    displaced, residual, rel_norm = pl.pallas_call(
        final_kernel,
        out_shape=(node_shape, node_shape, jax.ShapeDtypeStruct((1, 1), f32)),
        in_specs=[VMEM, SMEM, VMEM, VMEM, VMEM, VMEM],
        out_specs=[VMEM] * 3,
        scratch_shapes=[pltpu.VMEM((8, LANES), f32)],
        compiler_params=pltpu.CompilerParams(vmem_limit_bytes=12 << 20),
        name="final",
    )(
        returned,
        me,
        displacement,
        jnp.asarray(force_table),
        jnp.asarray(weight_table),
        jnp.asarray(place_table),
    )
    return (
        new_state.reshape(micro_state.shape),
        displaced,
        residual,
        rel_norm.reshape(()),
    )


def solution(mesh):
    return jax.shard_map(
        per_device,
        mesh=mesh,
        in_specs=(
            P(None, "sub", "rve", None),
            P(None, "sub", "rve", None),
            P(AXES),
            P(None, None, None, AXES),
            P(AXES),
            P(None, AXES),
            P(),
        ),
        out_specs=(
            P(None, None, None, AXES),
            P(None, "sub", "rve", None),
            P(None, "sub", "rve", None),
            P(),
        ),
        check_vma=False,
    )
```

```python
import math

import jax
import jax.numpy as jnp
import numpy as np
from jax import lax
from jax.experimental import pallas as pl
from jax.experimental.pallas import tpu as pltpu
from jax.sharding import Mesh
from jax.sharding import PartitionSpec as P

R = 6
VOX = R * R * R
ROWS = 3 * VOX
CASES = 7
DEV = 128
LANES = 128
CHUNKS = 36
WIDE = CHUNKS * LANES
TAIL = CASES * ROWS - (CHUNKS - 1) * LANES
NODES = 48
STAB = 0.1
FLOOR = 1.0
SPLIT = ("far", "core", "rve")
AXES = ("core", "far", "rve")
SUB = ("far", "core")
PAIRS = ((0, 5, 4), (5, 1, 3), (4, 3, 2))
STRAIN_OF = ((0, 4, 5), (5, 1, 3), (4, 3, 2))
OFF_DIAGONAL = ((0, 4), (0, 5), (4, 5), (1, 3), (1, 5), (3, 5), (2, 3), (2, 4), (3, 4))
LOW = 0.5 - 0.5 / math.sqrt(3.0)
HIGH = 0.5 + 0.5 / math.sqrt(3.0)
HIGHEST = lax.Precision.HIGHEST
VMEM = pl.BlockSpec(memory_space=pltpu.VMEM)
SMEM = pl.BlockSpec(memory_space=pltpu.SMEM)
HBM = pl.BlockSpec(memory_space=pltpu.HBM)
PARTS = 6
UPDATE = 72
PART_ROWS = CHUNKS // PARTS * LANES


def strain_table():
    places = (LOW, HIGH)
    table = np.zeros((8, 8, 3, 6))
    for gauss in range(8):
        at = (places[gauss % 2], places[gauss // 2 % 2], places[gauss // 4])
        for corner in range(8):
            bits = (corner % 2, corner // 2 % 2, corner // 4)
            weight = [at[k] if bits[k] else 1.0 - at[k] for k in range(3)]
            sign = [1.0 if bits[k] else -1.0 for k in range(3)]
            dx = sign[0] * weight[1] * weight[2]
            dy = weight[0] * sign[1] * weight[2]
            dz = weight[0] * weight[1] * sign[2]
            table[gauss, corner, 0, [0, 4, 5]] = (dx, dz, dy)
            table[gauss, corner, 1, [1, 3, 5]] = (dy, dz, dx)
            table[gauss, corner, 2, [2, 3, 4]] = (dz, dy, dx)
    return table


def term_index(first, second):
    if first == second:
        return first
    return 6 + OFF_DIAGONAL.index((min(first, second), max(first, second)))


def diagonal_terms(component):
    m = STRAIN_OF[component]
    pairs = [(m[0], m[0]), (m[1], m[1]), (m[2], m[2]), (m[0], m[1]), (m[0], m[2]), (m[1], m[2])]
    return [(a, b, term_index(a, b)) for a, b in pairs]


def assembly_tables():
    table = strain_table()
    force = np.zeros((6, LANES, 2 * LANES), np.float32)
    weights = np.zeros((3, 6, 8, LANES), np.float32)
    place = np.zeros((4, LANES, LANES), np.float32)
    for j in range(LANES):
        ly, ex, gauss = j // 64, j // 8 % 8, j % 8
        for corner in range(8):
            az, row, col = corner // 4, ly + corner // 2 % 2, (ex + corner % 2) % 8
            for i in range(3):
                lane = az * LANES + (NODES if row == 2 else 0) + i * 16 + row % 2 * 8 + col
                for m in STRAIN_OF[i]:
                    force[m, j, lane] += 0.125 * table[gauss, corner, i, m]
                for n, (first, second, _) in enumerate(diagonal_terms(i)):
                    weights[i, n, corner, j] = (
                        0.125 * table[gauss, corner, i, first] * table[gauss, corner, i, second]
                    )
            place[az * 2 + (1 if row == 2 else 0), j, corner * 16 + row % 2 * 8 + col] = 1.0
    return force.reshape(6 * LANES, 2 * LANES), weights.reshape(18 * 8, LANES), place


def lane_iota(rows=1):
    return lax.broadcasted_iota(jnp.int32, (rows, LANES), 1)


def sublane_iota(rows=8):
    return lax.broadcasted_iota(jnp.int32, (rows, LANES), 0)


def node_row(ref, scratch, offset):
    scratch[...] = jnp.zeros((8, LANES), jnp.float32)
    for i in range(3):
        scratch[2 * i : 2 * i + 2, 0:8] = ref[i, 0]
    tile = scratch[...]
    total = jnp.zeros((1, LANES), jnp.float32)
    for row in range(6):
        total = total + pltpu.roll(tile[row : row + 1], offset + 8 * row, 1)
    return total


def previous_row_lanes(value):
    lane = lane_iota(value.shape[0])
    return jnp.where(lane % 4 == 0, pltpu.roll(value, LANES - 3, 1), pltpu.roll(value, 1, 1))


def next_row_lanes(value):
    lane = lane_iota(value.shape[0])
    return jnp.where(lane % 4 == 3, pltpu.roll(value, 3, 1), pltpu.roll(value, LANES - 1, 1))


def below_lanes(value):
    lane = lane_iota(value.shape[0])
    moved = jnp.where(lane < 64, pltpu.roll(value, 68, 1), pltpu.roll(value, 64, 1))
    return jnp.where(lane < 4, 0.0, moved)


def above_lanes(value):
    lane = lane_iota(value.shape[0])
    moved = jnp.where(lane < 64, pltpu.roll(value, 64, 1), pltpu.roll(value, 60, 1))
    return jnp.where(lane >= 124, 0.0, moved)


def device_at(place):
    return ((place >> 2) & 15) * 8 + (place >> 6) * 4 + (place & 3)


def place_of(device):
    return ((device >> 2) & 1) * 64 + (device >> 3) * 4 + (device & 3)


def part_copy(src, dst, sems, part):
    rows = pl.ds(part * PART_ROWS, min(PART_ROWS, CASES * ROWS - part * PART_ROWS))
    return pltpu.make_async_copy(src.at[rows], dst.at[rows], sems.at[part])


def split_bf16(value):
    high = value.astype(jnp.bfloat16)
    rest = value - high.astype(jnp.float32)
    middle = rest.astype(jnp.bfloat16)
    low = (rest - middle.astype(jnp.float32)).astype(jnp.bfloat16)
    return high, middle, low


def turn(choose, block):
    high, middle, low = (
        lax.dot_general(
            choose, part, (((1,), (1,)), ((), ())), preferred_element_type=jnp.float32
        )
        for part in split_bf16(block)
    )
    return (high + middle) + low


def pack_kernel(
    state_ref,
    state_slot_hbm,
    home_slot_hbm,
    disp_hbm,
    out_ref,
    held_ref,
    state_slot_ref,
    home_slot_ref,
    disp_ref,
    scratch,
    sems,
):
    small = [
        pltpu.make_async_copy(src, dst, sems.at[PARTS + k])
        for k, (src, dst) in enumerate(
            (
                (state_slot_hbm, state_slot_ref),
                (home_slot_hbm, home_slot_ref),
                (disp_hbm, disp_ref),
            )
        )
    ]
    for copy in small:
        copy.start()
    for part in range(PARTS):
        part_copy(state_ref, held_ref, sems, part).start()
    owner = device_at(sublane_iota(DEV))
    lane = lane_iota(DEV)
    for copy in small:
        copy.wait()
    choose = ((state_slot_ref[...] >> 7) == owner).astype(jnp.float32).astype(jnp.bfloat16)
    home = (home_slot_ref[...] >> 7) == owner
    local = jnp.sum(jnp.where(home, lane, 0).astype(jnp.float32), axis=1, keepdims=True)
    extra = node_row(disp_ref, scratch, TAIL) + jnp.where(lane == TAIL + NODES, local, 0.0)
    held_ref[CASES * ROWS :, :] = jnp.zeros((WIDE - CASES * ROWS, LANES), jnp.float32)
    for part in range(PARTS):
        part_copy(state_ref, held_ref, sems, part).wait()
        for k in range(part * CHUNKS // PARTS, (part + 1) * CHUNKS // PARTS):
            turned = turn(choose, held_ref[k * LANES : (k + 1) * LANES, :])
            if k == CHUNKS - 1:
                turned = turned + extra
            out_ref[pl.ds(k, DEV, stride=CHUNKS), :] = turned


def macro_strain_rows(tail):
    local = tail[TAIL + NODES : TAIL + NODES + 1].astype(jnp.int32)
    upper = (local >> 6) == 1
    ex = (local >> 3) & 7
    point = [jnp.where(((local >> k) & 1) == 1, HIGH, LOW) for k in range(3)]
    shape = [(1.0 - point[k], point[k]) for k in range(3)]
    sub = sublane_iota()
    hits = (sub == ex, sub == ((ex + 1) & 7))
    slopes = []
    for i in range(3):
        own = [tail[TAIL + 16 * i + 8 * y : TAIL + 16 * i + 8 * y + 8] for y in range(2)]
        rows = [own[0], own[1], next_row_lanes(own[0])]
        planes = [rows, [above_lanes(row) for row in rows]]
        at = {}
        for az in range(2):
            for ay in range(2):
                chosen = jnp.where(upper, planes[az][ay + 1], planes[az][ay])
                for ax in range(2):
                    at[az, ay, ax] = jnp.sum(
                        jnp.where(hits[ax], chosen, 0.0), axis=0, keepdims=True
                    )
        sx, sy, sz = shape
        slope = [0.0, 0.0, 0.0]
        for first in range(2):
            for second in range(2):
                slope[0] = slope[0] + sz[first] * sy[second] * (
                    at[first, second, 1] - at[first, second, 0]
                )
                slope[1] = slope[1] + sz[first] * sx[second] * (
                    at[first, 1, second] - at[first, 0, second]
                )
                slope[2] = slope[2] + sy[first] * sx[second] * (
                    at[1, first, second] - at[0, first, second]
                )
        slopes.append(slope)
    return [
        slopes[0][0],
        slopes[1][1],
        slopes[2][2],
        slopes[1][2] + slopes[2][1],
        slopes[0][2] + slopes[2][0],
        slopes[0][1] + slopes[1][0],
    ]


def tile_at(ref, base, row):
    return ref[pl.ds(base + row * 8, 8), :]


def solve_kernel(
    recv_ref,
    phase_ref,
    moduli_ref,
    slot_ref,
    load_ref,
    ret_ref,
    w_out,
    p_out,
    q_out,
    step_ref,
    w_ref,
    p_ref,
    q_ref,
    sig_ref,
    lam_ref,
    mu_ref,
    mu2_ref,
    scratch,
    sems,
):
    saves = [
        pltpu.make_async_copy(src, dst, sems.at[k])
        for k, (src, dst) in enumerate(((w_ref, w_out), (p_ref, p_out), (q_ref, q_out)))
    ]

    def save_plane(base):
        for i in range(3):
            rows = pl.ds(base + i * VOX * 8, 288)
            pltpu.make_async_copy(q_ref.at[rows], q_out.at[rows], sems.at[2]).start()

    zero = jnp.zeros((8, LANES), jnp.float32)
    phase = jnp.take_along_axis(phase_ref[...], device_at(lane_iota(VOX)), axis=1)
    mu = jnp.where(
        phase == 0, moduli_ref[1, 0], jnp.where(phase == 1, moduli_ref[1, 1], moduli_ref[1, 2])
    )
    lam_ref[...] = jnp.where(
        phase == 0, moduli_ref[0, 0], jnp.where(phase == 1, moduli_ref[0, 1], moduli_ref[0, 2])
    )
    mu_ref[...] = mu
    mu2_ref[...] = mu + mu
    w_ref[pl.ds(7, ROWS, stride=8), :] = jnp.zeros((ROWS, LANES), jnp.float32)
    tail = None
    for k in range(CHUNKS):
        turned = recv_ref[pl.ds(k, DEV, stride=CHUNKS), :].T
        start, stop = k * LANES, min((k + 1) * LANES, CASES * ROWS)
        while start < stop:
            case = start // ROWS
            end = min(stop, (case + 1) * ROWS)
            w_ref[pl.ds((start - case * ROWS) * 8 + case, end - start, stride=8), :] = turned[
                start - k * LANES : end - k * LANES
            ]
            start = end
        tail = turned
    saves[0].start()
    macro = macro_strain_rows(tail)
    sub = sublane_iota()
    imposed = [
        jnp.where(sub == 0, macro[m], jnp.where(sub == m + 1, 1.0, 0.0)) for m in range(6)
    ]

    def stress_pass(src, strain, keep, energy):
        def plane(a, carry):
            sums, work = list(carry[0]), carry[1]
            base = pl.multiple_of(a * 288, 8)
            ahead = pl.multiple_of(jnp.where(a == R - 1, 0, (a + 1) * 288), 8)
            voxel = a * 36
            line = [[tile_at(src, base, i * VOX + c) for c in range(R)] for i in range(3)]
            for b in range(R):
                nb = (b + 1) % R
                below = [
                    [tile_at(src, base, i * VOX + nb * R + c) for c in range(R)] for i in range(3)
                ]
                for c in range(R):
                    at = b * R + c
                    here = [line[i][c] for i in range(3)]
                    grad = [
                        [
                            tile_at(src, ahead, i * VOX + at) - here[i],
                            below[i][c] - here[i],
                            line[i][(c + 1) % R] - here[i],
                        ]
                        for i in range(3)
                    ]
                    eps = [
                        grad[0][0],
                        grad[1][1],
                        grad[2][2],
                        grad[1][2] + grad[2][1],
                        grad[0][2] + grad[2][0],
                        grad[0][1] + grad[1][0],
                    ]
                    if strain is not None:
                        eps = [eps[m] + strain[m] for m in range(6)]
                    lam = lam_ref[pl.ds(voxel + at, 8, stride=0), :]
                    mu1 = mu_ref[pl.ds(voxel + at, 8, stride=0), :]
                    mu2 = mu2_ref[pl.ds(voxel + at, 8, stride=0), :]
                    bulk = lam * (eps[0] + eps[1] + eps[2])
                    sig = [bulk + mu2 * eps[m] for m in range(3)]
                    sig += [mu1 * eps[m] for m in range(3, 6)]
                    for m in range(6):
                        sums[m] = sums[m] + sig[m]
                        if keep:
                            sig_ref[pl.ds(base + (m * VOX + at) * 8, 8), :] = sig[m]
                    if energy:
                        work = work + (
                            (sig[0] * eps[0] + sig[1] * eps[1])
                            + (sig[2] * eps[2] + sig[3] * eps[3])
                            + (sig[4] * eps[4] + sig[5] * eps[5])
                        )
                line = below
            return tuple(sums), work

        return lax.fori_loop(0, R, plane, ((zero,) * 6, zero))

    def force_pass(src, finish, dst):
        def plane(a, carry):
            totals = list(carry)
            base = pl.multiple_of(a * 288, 8)
            behind = pl.multiple_of(jnp.where(a == 0, (R - 1) * 288, (a - 1) * 288), 8)
            for b in range(R):
                pb = (b + R - 1) % R
                last = [tile_at(sig_ref, base, PAIRS[2][i] * VOX + b * R + R - 1) for i in range(3)]
                for c in range(R):
                    at = b * R + c
                    own = [tile_at(sig_ref, base, m * VOX + at) for m in range(6)]
                    for i in range(3):
                        gone = (own[PAIRS[0][i]] + own[PAIRS[1][i]]) + own[PAIRS[2][i]]
                        come = (
                            tile_at(sig_ref, behind, PAIRS[0][i] * VOX + at)
                            + tile_at(sig_ref, base, PAIRS[1][i] * VOX + pb * R + c)
                        ) + last[i]
                        value = finish(come - gone, tile_at(src, base, i * VOX + at))
                        dst[pl.ds(base + (i * VOX + at) * 8, 8), :] = value
                        totals[i] = totals[i] + value * value
                    last = [own[PAIRS[2][i]] for i in range(3)]
            return tuple(totals)

        totals = lax.fori_loop(0, R, plane, (zero,) * 3)
        return (totals[0] + totals[1]) + totals[2]

    mean0, _ = stress_pass(w_ref, imposed, True, False)
    square0 = force_pass(w_ref, lambda div, w: -(div + STAB * w), p_ref)
    saves[1].start()
    mean1, work1 = stress_pass(p_ref, None, True, True)
    step0 = square0 / (work1 + STAB * square0)
    square1 = force_pass(p_ref, lambda div, p: p - step0 * (div + STAB * p), q_ref)
    ratio = square1 / square0

    def direction(a, carry):
        totals = list(carry)
        base = pl.multiple_of(a * 288, 8)
        for at in range(36):
            for i in range(3):
                value = tile_at(q_ref, base, i * VOX + at) + ratio * tile_at(
                    p_ref, base, i * VOX + at
                )
                q_ref[pl.ds(base + (i * VOX + at) * 8, 8), :] = value
                totals[i] = totals[i] + value * value
        save_plane(base)
        return tuple(totals)

    totals = lax.fori_loop(0, R, direction, (zero,) * 3)
    length = (totals[0] + totals[1]) + totals[2]
    mean2, work2 = stress_pass(q_ref, None, False, True)
    step1 = square1 / (work2 + STAB * length)
    step_ref[0:8, :] = step0
    step_ref[8:16, :] = step1
    mean = [(mean0[m] + step0 * mean1[m] + step1 * mean2[m]) * (1.0 / VOX) for m in range(6)]

    shared = place_of(slot_ref[...] >> 7).astype(jnp.float32)
    shared = jnp.broadcast_to(shared, (8, LANES))
    for m in range(6):
        shared = jnp.where(sub == m, mean[m][0:1], shared)
    terms = [mean[m][m + 1 : m + 2] for m in range(6)]
    for first, second in OFF_DIAGONAL:
        terms.append(mean[first][second + 1 : second + 2] + mean[second][first + 1 : first + 2])
    own = jnp.concatenate(terms + [jnp.zeros((1, LANES), jnp.float32)], axis=0)
    left = previous_row_lanes(own)
    stacked = jnp.concatenate(
        [jnp.zeros((64, LANES), jnp.float32), own, left, below_lanes(own), below_lanes(left)],
        axis=0,
    )
    special = stacked.T + node_row(load_ref, scratch, 0)
    for peer in range(DEV):
        ret_ref[8 * peer : 8 * peer + 8, :] = shared
    ret_ref[pl.ds(7, DEV, stride=8), :] = special
    for save in saves:
        save.wait()


def update_kernel(w_ref, p_ref, q_ref, step_ref, out_ref):
    place = place_of(lane_iota(UPDATE))
    for case in range(CASES):
        first = step_ref[case : case + 1, :]
        second = step_ref[8 + case : 9 + case, :]
        rows = pl.ds(case, UPDATE, stride=8)
        value = w_ref[rows, :] + first * p_ref[rows, :] + second * q_ref[rows, :]
        out_ref[case] = jnp.take_along_axis(value, place, axis=1)


def row_of(value, index):
    return jnp.sum(jnp.where(sublane_iota(DEV) == index, value, 0), axis=0, keepdims=True)


def node_tile(row):
    sub = sublane_iota()
    wide = jnp.broadcast_to(row, (8, LANES))
    tile = wide
    for r in range(1, 6):
        tile = jnp.where(sub == r, pltpu.roll(wide, LANES - 8 * r, 1), tile)
    return tile


def final_kernel(
    recv_ref,
    me_ref,
    disp_ref,
    force_ref,
    weight_ref,
    place_ref,
    new_disp_ref,
    res_ref,
    norm_ref,
    scratch,
):
    me = me_ref[0, 0]
    order = recv_ref[pl.ds(6, DEV, stride=8), :].astype(jnp.int32)
    special = recv_ref[pl.ds(7, DEV, stride=8), :]
    stress = [
        jnp.take_along_axis(recv_ref[pl.ds(m, DEV, stride=8), :].T, order, axis=1)
        for m in range(6)
    ]
    forces = lax.dot_general(
        jnp.concatenate(stress, axis=1),
        force_ref[...],
        (((1,), (0,)), ((), ())),
        precision=HIGHEST,
        preferred_element_type=jnp.float32,
    )
    home = sublane_iota(DEV)
    upper = forces[:, LANES:]
    lifted = jnp.where(home < 64, pltpu.roll(upper, 68, 0), pltpu.roll(upper, 64, 0))
    lifted = jnp.where(home < 4, 0.0, lifted)
    near = forces[:, :LANES] + lifted
    beside = jnp.where(home % 4 == 0, pltpu.roll(near, DEV - 3, 0), pltpu.roll(near, 1, 0))
    force = near + pltpu.roll(beside, LANES - NODES, 1)
    node = lane_iota(DEV) < NODES
    loads = jnp.where(node, special, 0.0)
    residual = jnp.where(node, special - force, 0.0)
    top = jnp.sum(jnp.sum(residual * residual, axis=0, keepdims=True), axis=1, keepdims=True)
    bottom = jnp.sum(jnp.sum(loads * loads, axis=0, keepdims=True), axis=1, keepdims=True)
    norm_ref[...] = jnp.sqrt(top / bottom)

    own_residual = row_of(residual, me)
    left = jnp.where(me % 4 == 0, me + 3, me - 1)
    under = jnp.where(me >= 64, 64, jnp.where(me < 4, 0, -60))
    turned = special.T
    diagonal = jnp.zeros((24, LANES), jnp.float32)
    for k, source in enumerate((me, left, me - under, left - under)):
        picks = jnp.broadcast_to(row_of(order, source), (16, LANES))
        terms = jnp.take_along_axis(turned[64 + 16 * k : 80 + 16 * k], picks, axis=1)
        corner = []
        for i in range(3):
            total = jnp.zeros((8, LANES), jnp.float32)
            for n, (_, _, t) in enumerate(diagonal_terms(i)):
                at = (i * 6 + n) * 8
                total = total + weight_ref[at : at + 8, :] * terms[t : t + 1]
            corner.append(total)
        diagonal = diagonal + lax.dot_general(
            jnp.concatenate(corner, axis=0),
            place_ref[k],
            (((1,), (0,)), ((), ())),
            precision=HIGHEST,
            preferred_element_type=jnp.float32,
        )
    lane = lane_iota(8)
    same = lane // 16 == sublane_iota()
    row = jnp.zeros((1, LANES), jnp.float32)
    for i in range(3):
        part = jnp.sum(jnp.where(same, diagonal[8 * i : 8 * i + 8], 0.0), axis=0, keepdims=True)
        for shift in (64, 32, 16):
            part = part + pltpu.roll(part, shift, 1)
        row = jnp.where(lane_iota() // 16 == i, part, row)
    moved = node_row(disp_ref, scratch, 0) + own_residual / jnp.maximum(row, FLOOR)
    for value, ref in ((moved, new_disp_ref), (own_residual, res_ref)):
        tile = node_tile(value)
        for i in range(3):
            ref[i, 0] = tile[2 * i : 2 * i + 2, 0:8]


def in_hbm(value):
    return pltpu.with_memory_space_constraint(value, pltpu.HBM)


def exchange(value):
    return lax.all_to_all(value, AXES, split_axis=0, concat_axis=0, tiled=True)


def per_device(displacement, load, home_slot, micro_state, state_slot, phases, phase_moduli):
    force_table, weight_table, place_table = assembly_tables()
    f32 = jnp.float32
    home_row = home_slot.reshape(1, LANES)
    sent = pl.pallas_call(
        pack_kernel,
        out_shape=jax.ShapeDtypeStruct((DEV * CHUNKS, LANES), f32),
        in_specs=[HBM] * 4,
        out_specs=VMEM,
        scratch_shapes=[
            pltpu.VMEM((WIDE, LANES), f32),
            pltpu.VMEM((1, LANES), jnp.int32),
            pltpu.VMEM((1, LANES), jnp.int32),
            pltpu.VMEM(displacement.shape, f32),
            pltpu.VMEM((8, LANES), f32),
            pltpu.SemaphoreType.DMA((PARTS + 3,)),
        ],
        compiler_params=pltpu.CompilerParams(vmem_limit_bytes=12 << 20),
        name="pack",
    )(
        in_hbm(micro_state.reshape(CASES * ROWS, LANES)),
        in_hbm(state_slot.reshape(1, LANES)),
        in_hbm(home_row),
        in_hbm(displacement),
    )
    received = exchange(sent.reshape(DEV, 1, WIDE)).reshape(DEV * CHUNKS, LANES)
    big = pltpu.HBM((ROWS * 8, LANES), f32)
    answer, w, p, q, steps = pl.pallas_call(
        solve_kernel,
        out_shape=(
            jax.ShapeDtypeStruct((DEV * 8, LANES), f32),
            big,
            big,
            big,
            jax.ShapeDtypeStruct((16, LANES), f32),
        ),
        in_specs=[VMEM, VMEM, SMEM, VMEM, VMEM],
        out_specs=[VMEM, HBM, HBM, HBM, VMEM],
        scratch_shapes=[
            pltpu.VMEM((ROWS * 8, LANES), f32),
            pltpu.VMEM((ROWS * 8, LANES), f32),
            pltpu.VMEM((ROWS * 8, LANES), f32),
            pltpu.VMEM((6 * VOX * 8, LANES), f32),
            pltpu.VMEM((VOX, LANES), f32),
            pltpu.VMEM((VOX, LANES), f32),
            pltpu.VMEM((VOX, LANES), f32),
            pltpu.VMEM((8, LANES), f32),
            pltpu.SemaphoreType.DMA((3,)),
        ],
        compiler_params=pltpu.CompilerParams(vmem_limit_bytes=32 << 20),
        name="solve",
    )(received, phases, phase_moduli, home_row, load)
    returned = exchange(answer.reshape(DEV, 8, LANES)).reshape(DEV * 8, LANES)
    new_state = pl.pallas_call(
        update_kernel,
        out_shape=jax.ShapeDtypeStruct((CASES, ROWS, LANES), f32),
        grid=(ROWS // UPDATE,),
        in_specs=[pl.BlockSpec((UPDATE * 8, LANES), lambda k: (k, 0))] * 3
        + [pl.BlockSpec((16, LANES), lambda k: (0, 0))],
        out_specs=pl.BlockSpec((CASES, UPDATE, LANES), lambda k: (0, k, 0)),
        compiler_params=pltpu.CompilerParams(vmem_limit_bytes=8 << 20),
        cost_estimate=pl.CostEstimate(
            flops=20_000_000, bytes_accessed=10_000_000, transcendentals=0
        ),
        name="update",
    )(in_hbm(w), in_hbm(p), in_hbm(q), steps)
    me = lax.axis_index(AXES).astype(jnp.int32).reshape(1, 1)
    node_shape = jax.ShapeDtypeStruct(displacement.shape, f32)
    displaced, residual, rel_norm = pl.pallas_call(
        final_kernel,
        out_shape=(node_shape, node_shape, jax.ShapeDtypeStruct((1, 1), f32)),
        in_specs=[VMEM, SMEM, VMEM, VMEM, VMEM, VMEM],
        out_specs=[VMEM] * 3,
        scratch_shapes=[pltpu.VMEM((8, LANES), f32)],
        compiler_params=pltpu.CompilerParams(vmem_limit_bytes=12 << 20),
        name="final",
    )(
        returned,
        me,
        displacement,
        jnp.asarray(force_table),
        jnp.asarray(weight_table),
        jnp.asarray(place_table),
    )
    return (
        new_state.reshape(micro_state.shape),
        displaced,
        residual,
        rel_norm.reshape(()),
    )


def solution(mesh):
    split = Mesh(mesh.devices.reshape(-1, 2, mesh.shape["rve"]), SPLIT)
    return jax.shard_map(
        per_device,
        mesh=split,
        in_specs=(
            P(None, SUB, "rve", None),
            P(None, SUB, "rve", None),
            P(SPLIT),
            P(None, None, None, SPLIT),
            P(SPLIT),
            P(None, SPLIT),
            P(),
        ),
        out_specs=(
            P(None, None, None, SPLIT),
            P(None, SUB, "rve", None),
            P(None, SUB, "rve", None),
            P(),
        ),
        check_vma=False,
    )
```

```python
import math

import jax
import jax.numpy as jnp
import numpy as np
from jax import lax
from jax.experimental import pallas as pl
from jax.experimental.pallas import tpu as pltpu
from jax.sharding import Mesh
from jax.sharding import PartitionSpec as P

R = 6
VOX = R * R * R
ROWS = 3 * VOX
CASES = 7
DEV = 128
LANES = 128
CHUNKS = 36
WIDE = CHUNKS * LANES
TAIL = CASES * ROWS - (CHUNKS - 1) * LANES
NODES = 48
STAB = 0.1
FLOOR = 1.0
SPLIT = ("far", "core", "rve")
AXES = ("core", "far", "rve")
SUB = ("far", "core")
PAIRS = ((0, 5, 4), (5, 1, 3), (4, 3, 2))
STRAIN_OF = ((0, 4, 5), (5, 1, 3), (4, 3, 2))
OFF_DIAGONAL = ((0, 4), (0, 5), (4, 5), (1, 3), (1, 5), (3, 5), (2, 3), (2, 4), (3, 4))
LOW = 0.5 - 0.5 / math.sqrt(3.0)
HIGH = 0.5 + 0.5 / math.sqrt(3.0)
HIGHEST = lax.Precision.HIGHEST
VMEM = pl.BlockSpec(memory_space=pltpu.VMEM)
SMEM = pl.BlockSpec(memory_space=pltpu.SMEM)
HBM = pl.BlockSpec(memory_space=pltpu.HBM)
CUTS = (0, 18, 30, 36)
PARTS = len(CUTS) - 1
STEP = 6
UPDATE = 72


def strain_table():
    places = (LOW, HIGH)
    table = np.zeros((8, 8, 3, 6))
    for gauss in range(8):
        at = (places[gauss % 2], places[gauss // 2 % 2], places[gauss // 4])
        for corner in range(8):
            bits = (corner % 2, corner // 2 % 2, corner // 4)
            weight = [at[k] if bits[k] else 1.0 - at[k] for k in range(3)]
            sign = [1.0 if bits[k] else -1.0 for k in range(3)]
            dx = sign[0] * weight[1] * weight[2]
            dy = weight[0] * sign[1] * weight[2]
            dz = weight[0] * weight[1] * sign[2]
            table[gauss, corner, 0, [0, 4, 5]] = (dx, dz, dy)
            table[gauss, corner, 1, [1, 3, 5]] = (dy, dz, dx)
            table[gauss, corner, 2, [2, 3, 4]] = (dz, dy, dx)
    return table


def term_index(first, second):
    if first == second:
        return first
    return 6 + OFF_DIAGONAL.index((min(first, second), max(first, second)))


def diagonal_terms(component):
    m = STRAIN_OF[component]
    pairs = [(m[0], m[0]), (m[1], m[1]), (m[2], m[2]), (m[0], m[1]), (m[0], m[2]), (m[1], m[2])]
    return [(a, b, term_index(a, b)) for a, b in pairs]


def assembly_tables():
    table = strain_table()
    force = np.zeros((6, LANES, 2 * LANES), np.float32)
    weights = np.zeros((3, 6, 8, LANES), np.float32)
    place = np.zeros((4, LANES, LANES), np.float32)
    for j in range(LANES):
        ly, ex, gauss = j // 64, j // 8 % 8, j % 8
        for corner in range(8):
            az, row, col = corner // 4, ly + corner // 2 % 2, (ex + corner % 2) % 8
            for i in range(3):
                lane = az * LANES + (NODES if row == 2 else 0) + i * 16 + row % 2 * 8 + col
                for m in STRAIN_OF[i]:
                    force[m, j, lane] += 0.125 * table[gauss, corner, i, m]
                for n, (first, second, _) in enumerate(diagonal_terms(i)):
                    weights[i, n, corner, j] = (
                        0.125 * table[gauss, corner, i, first] * table[gauss, corner, i, second]
                    )
            place[az * 2 + (1 if row == 2 else 0), j, corner * 16 + row % 2 * 8 + col] = 1.0
    return force.reshape(6 * LANES, 2 * LANES), weights.reshape(18 * 8, LANES), place


def lane_iota(rows=1):
    return lax.broadcasted_iota(jnp.int32, (rows, LANES), 1)


def sublane_iota(rows=8):
    return lax.broadcasted_iota(jnp.int32, (rows, LANES), 0)


def node_row(ref, scratch, offset):
    scratch[...] = jnp.zeros((8, LANES), jnp.float32)
    for i in range(3):
        scratch[2 * i : 2 * i + 2, 0:8] = ref[i, 0]
    tile = scratch[...]
    total = jnp.zeros((1, LANES), jnp.float32)
    for row in range(6):
        total = total + pltpu.roll(tile[row : row + 1], offset + 8 * row, 1)
    return total


def previous_row_lanes(value):
    lane = lane_iota(value.shape[0])
    return jnp.where(lane % 4 == 0, pltpu.roll(value, LANES - 3, 1), pltpu.roll(value, 1, 1))


def next_row_lanes(value):
    lane = lane_iota(value.shape[0])
    return jnp.where(lane % 4 == 3, pltpu.roll(value, 3, 1), pltpu.roll(value, LANES - 1, 1))


def below_lanes(value):
    lane = lane_iota(value.shape[0])
    moved = jnp.where(lane < 64, pltpu.roll(value, 68, 1), pltpu.roll(value, 64, 1))
    return jnp.where(lane < 4, 0.0, moved)


def above_lanes(value):
    lane = lane_iota(value.shape[0])
    moved = jnp.where(lane < 64, pltpu.roll(value, 64, 1), pltpu.roll(value, 60, 1))
    return jnp.where(lane >= 124, 0.0, moved)


def device_at(place):
    return ((place >> 2) & 15) * 8 + (place >> 6) * 4 + (place & 3)


def place_of(device):
    return ((device >> 2) & 1) * 64 + (device >> 3) * 4 + (device & 3)


def part_copy(src, dst, sems, part):
    start, stop = CUTS[part] * LANES, min(CUTS[part + 1] * LANES, CASES * ROWS)
    rows = pl.ds(start, stop - start)
    return pltpu.make_async_copy(src.at[rows], dst.at[rows], sems.at[part])


def split_bf16(value):
    high = value.astype(jnp.bfloat16)
    rest = value - high.astype(jnp.float32)
    middle = rest.astype(jnp.bfloat16)
    low = (rest - middle.astype(jnp.float32)).astype(jnp.bfloat16)
    return high, middle, low


def pack_kernel(
    state_ref,
    state_slot_hbm,
    home_slot_hbm,
    disp_hbm,
    out_ref,
    held_ref,
    state_slot_ref,
    home_slot_ref,
    disp_ref,
    scratch,
    sems,
):
    small = [
        pltpu.make_async_copy(src, dst, sems.at[PARTS + k])
        for k, (src, dst) in enumerate(
            (
                (state_slot_hbm, state_slot_ref),
                (home_slot_hbm, home_slot_ref),
                (disp_hbm, disp_ref),
            )
        )
    ]
    for copy in small:
        copy.start()
    for part in range(PARTS):
        part_copy(state_ref, held_ref, sems, part).start()
    owner = device_at(sublane_iota(DEV))
    lane = lane_iota(DEV)
    for copy in small:
        copy.wait()
    choose = ((state_slot_ref[...] >> 7) == owner).astype(jnp.float32).astype(jnp.bfloat16)
    twice = jnp.concatenate([choose, choose], axis=1)
    home = (home_slot_ref[...] >> 7) == owner
    local = jnp.sum(jnp.where(home, lane, 0).astype(jnp.float32), axis=1, keepdims=True)
    extra = node_row(disp_ref, scratch, TAIL) + jnp.where(lane == TAIL + NODES, local, 0.0)
    held_ref[CASES * ROWS :, :] = jnp.zeros((WIDE - CASES * ROWS, LANES), jnp.float32)
    for part in range(PARTS):
        part_copy(state_ref, held_ref, sems, part).wait()
        for first in range(CUTS[part], CUTS[part + 1], STEP):
            high, middle, low = split_bf16(held_ref[first * LANES : (first + STEP) * LANES, :])
            picked = lax.dot_general(
                jnp.concatenate([high, middle], axis=1),
                twice,
                (((1,), (1,)), ((), ())),
                preferred_element_type=jnp.float32,
            )
            picked = picked + lax.dot_general(
                low, choose, (((1,), (1,)), ((), ())), preferred_element_type=jnp.float32
            )
            for k in range(first, first + STEP):
                turned = picked[(k - first) * LANES : (k - first + 1) * LANES].T
                if k == CHUNKS - 1:
                    turned = turned + extra
                out_ref[pl.ds(k, DEV, stride=CHUNKS), :] = turned


def macro_strain_rows(tail):
    local = tail[TAIL + NODES : TAIL + NODES + 1].astype(jnp.int32)
    upper = (local >> 6) == 1
    ex = (local >> 3) & 7
    point = [jnp.where(((local >> k) & 1) == 1, HIGH, LOW) for k in range(3)]
    shape = [(1.0 - point[k], point[k]) for k in range(3)]
    sub = sublane_iota()
    hits = (sub == ex, sub == ((ex + 1) & 7))
    slopes = []
    for i in range(3):
        own = [tail[TAIL + 16 * i + 8 * y : TAIL + 16 * i + 8 * y + 8] for y in range(2)]
        rows = [own[0], own[1], next_row_lanes(own[0])]
        planes = [rows, [above_lanes(row) for row in rows]]
        at = {}
        for az in range(2):
            for ay in range(2):
                chosen = jnp.where(upper, planes[az][ay + 1], planes[az][ay])
                for ax in range(2):
                    at[az, ay, ax] = jnp.sum(
                        jnp.where(hits[ax], chosen, 0.0), axis=0, keepdims=True
                    )
        sx, sy, sz = shape
        slope = [0.0, 0.0, 0.0]
        for first in range(2):
            for second in range(2):
                slope[0] = slope[0] + sz[first] * sy[second] * (
                    at[first, second, 1] - at[first, second, 0]
                )
                slope[1] = slope[1] + sz[first] * sx[second] * (
                    at[first, 1, second] - at[first, 0, second]
                )
                slope[2] = slope[2] + sy[first] * sx[second] * (
                    at[1, first, second] - at[0, first, second]
                )
        slopes.append(slope)
    return [
        slopes[0][0],
        slopes[1][1],
        slopes[2][2],
        slopes[1][2] + slopes[2][1],
        slopes[0][2] + slopes[2][0],
        slopes[0][1] + slopes[1][0],
    ]


def tile_at(ref, base, row):
    return ref[pl.ds(base + row * 8, 8), :]


def solve_kernel(
    recv_ref,
    phase_ref,
    moduli_ref,
    slot_ref,
    load_ref,
    ret_ref,
    w_out,
    p_out,
    q_out,
    step_ref,
    w_ref,
    p_ref,
    q_ref,
    sig_ref,
    lam_ref,
    mu_ref,
    mu2_ref,
    scratch,
    sems,
):
    saves = [
        pltpu.make_async_copy(src, dst, sems.at[k])
        for k, (src, dst) in enumerate(((w_ref, w_out), (p_ref, p_out), (q_ref, q_out)))
    ]

    def save_plane(base):
        for i in range(3):
            rows = pl.ds(base + i * VOX * 8, 288)
            pltpu.make_async_copy(q_ref.at[rows], q_out.at[rows], sems.at[2]).start()

    zero = jnp.zeros((8, LANES), jnp.float32)
    phase = jnp.take_along_axis(phase_ref[...], device_at(lane_iota(VOX)), axis=1)
    mu = jnp.where(
        phase == 0, moduli_ref[1, 0], jnp.where(phase == 1, moduli_ref[1, 1], moduli_ref[1, 2])
    )
    lam_ref[...] = jnp.where(
        phase == 0, moduli_ref[0, 0], jnp.where(phase == 1, moduli_ref[0, 1], moduli_ref[0, 2])
    )
    mu_ref[...] = mu
    mu2_ref[...] = mu + mu
    w_ref[pl.ds(7, ROWS, stride=8), :] = jnp.zeros((ROWS, LANES), jnp.float32)
    tail = None
    for k in range(CHUNKS):
        turned = recv_ref[pl.ds(k, DEV, stride=CHUNKS), :].T
        start, stop = k * LANES, min((k + 1) * LANES, CASES * ROWS)
        while start < stop:
            case = start // ROWS
            end = min(stop, (case + 1) * ROWS)
            w_ref[pl.ds((start - case * ROWS) * 8 + case, end - start, stride=8), :] = turned[
                start - k * LANES : end - k * LANES
            ]
            start = end
        tail = turned
    saves[0].start()
    macro = macro_strain_rows(tail)
    sub = sublane_iota()
    imposed = [
        jnp.where(sub == 0, macro[m], jnp.where(sub == m + 1, 1.0, 0.0)) for m in range(6)
    ]

    def stress_pass(src, strain, keep, energy):
        def plane(a, carry):
            sums, work = list(carry[0]), carry[1]
            base = pl.multiple_of(a * 288, 8)
            ahead = pl.multiple_of(jnp.where(a == R - 1, 0, (a + 1) * 288), 8)
            voxel = a * 36
            line = [[tile_at(src, base, i * VOX + c) for c in range(R)] for i in range(3)]
            for b in range(R):
                nb = (b + 1) % R
                below = [
                    [tile_at(src, base, i * VOX + nb * R + c) for c in range(R)] for i in range(3)
                ]
                for c in range(R):
                    at = b * R + c
                    here = [line[i][c] for i in range(3)]
                    grad = [
                        [
                            tile_at(src, ahead, i * VOX + at) - here[i],
                            below[i][c] - here[i],
                            line[i][(c + 1) % R] - here[i],
                        ]
                        for i in range(3)
                    ]
                    eps = [
                        grad[0][0],
                        grad[1][1],
                        grad[2][2],
                        grad[1][2] + grad[2][1],
                        grad[0][2] + grad[2][0],
                        grad[0][1] + grad[1][0],
                    ]
                    if strain is not None:
                        eps = [eps[m] + strain[m] for m in range(6)]
                    lam = lam_ref[pl.ds(voxel + at, 8, stride=0), :]
                    mu1 = mu_ref[pl.ds(voxel + at, 8, stride=0), :]
                    mu2 = mu2_ref[pl.ds(voxel + at, 8, stride=0), :]
                    bulk = lam * (eps[0] + eps[1] + eps[2])
                    sig = [bulk + mu2 * eps[m] for m in range(3)]
                    sig += [mu1 * eps[m] for m in range(3, 6)]
                    for m in range(6):
                        sums[m] = sums[m] + sig[m]
                        if keep:
                            sig_ref[pl.ds(base + (m * VOX + at) * 8, 8), :] = sig[m]
                    if energy:
                        work = work + (
                            (sig[0] * eps[0] + sig[1] * eps[1])
                            + (sig[2] * eps[2] + sig[3] * eps[3])
                            + (sig[4] * eps[4] + sig[5] * eps[5])
                        )
                line = below
            return tuple(sums), work

        return lax.fori_loop(0, R, plane, ((zero,) * 6, zero), unroll=2)

    def force_pass(src, finish, dst):
        def plane(a, carry):
            totals = list(carry)
            base = pl.multiple_of(a * 288, 8)
            behind = pl.multiple_of(jnp.where(a == 0, (R - 1) * 288, (a - 1) * 288), 8)
            for b in range(R):
                pb = (b + R - 1) % R
                last = [tile_at(sig_ref, base, PAIRS[2][i] * VOX + b * R + R - 1) for i in range(3)]
                for c in range(R):
                    at = b * R + c
                    own = [tile_at(sig_ref, base, m * VOX + at) for m in range(6)]
                    for i in range(3):
                        gone = (own[PAIRS[0][i]] + own[PAIRS[1][i]]) + own[PAIRS[2][i]]
                        come = (
                            tile_at(sig_ref, behind, PAIRS[0][i] * VOX + at)
                            + tile_at(sig_ref, base, PAIRS[1][i] * VOX + pb * R + c)
                        ) + last[i]
                        value = finish(come, gone, tile_at(src, base, i * VOX + at))
                        dst[pl.ds(base + (i * VOX + at) * 8, 8), :] = value
                        totals[i] = totals[i] + value * value
                    last = [own[PAIRS[2][i]] for i in range(3)]
            return tuple(totals)

        totals = lax.fori_loop(0, R, plane, (zero,) * 3, unroll=2)
        return (totals[0] + totals[1]) + totals[2]

    mean0, _ = stress_pass(w_ref, imposed, True, False)
    square0 = force_pass(w_ref, lambda come, gone, w: (gone - come) - STAB * w, p_ref)
    saves[1].start()
    mean1, work1 = stress_pass(p_ref, None, True, True)
    step0 = square0 / (work1 + STAB * square0)
    kept = 1.0 - STAB * step0
    square1 = force_pass(p_ref, lambda come, gone, p: kept * p - step0 * (come - gone), q_ref)
    ratio = square1 / square0

    def direction(a, carry):
        base = pl.multiple_of(a * 288, 8)
        for at in range(36):
            for i in range(3):
                q_ref[pl.ds(base + (i * VOX + at) * 8, 8), :] = tile_at(
                    q_ref, base, i * VOX + at
                ) + ratio * tile_at(p_ref, base, i * VOX + at)
        save_plane(base)
        return carry

    lax.fori_loop(0, R, direction, 0)
    length = square1 + ratio * square1
    mean2, work2 = stress_pass(q_ref, None, False, True)
    step1 = square1 / (work2 + STAB * length)
    step_ref[0:8, :] = step0
    step_ref[8:16, :] = step1
    mean = [(mean0[m] + step0 * mean1[m] + step1 * mean2[m]) * (1.0 / VOX) for m in range(6)]

    shared = place_of(slot_ref[...] >> 7).astype(jnp.float32)
    shared = jnp.broadcast_to(shared, (8, LANES))
    for m in range(6):
        shared = jnp.where(sub == m, mean[m][0:1], shared)
    terms = [mean[m][m + 1 : m + 2] for m in range(6)]
    for first, second in OFF_DIAGONAL:
        terms.append(mean[first][second + 1 : second + 2] + mean[second][first + 1 : first + 2])
    own = jnp.concatenate(terms + [jnp.zeros((1, LANES), jnp.float32)], axis=0)
    left = previous_row_lanes(own)
    stacked = jnp.concatenate(
        [jnp.zeros((64, LANES), jnp.float32), own, left, below_lanes(own), below_lanes(left)],
        axis=0,
    )
    special = stacked.T + node_row(load_ref, scratch, 0)
    for peer in range(DEV):
        ret_ref[8 * peer : 8 * peer + 8, :] = shared
    ret_ref[pl.ds(7, DEV, stride=8), :] = special
    for save in saves:
        save.wait()


def update_kernel(w_ref, p_ref, q_ref, step_ref, out_ref):
    place = place_of(lane_iota(UPDATE))
    for case in range(CASES):
        first = step_ref[case : case + 1, :]
        second = step_ref[8 + case : 9 + case, :]
        rows = pl.ds(case, UPDATE, stride=8)
        value = w_ref[rows, :] + first * p_ref[rows, :] + second * q_ref[rows, :]
        out_ref[case] = jnp.take_along_axis(value, place, axis=1)


def row_of(value, index):
    return jnp.sum(jnp.where(sublane_iota(DEV) == index, value, 0), axis=0, keepdims=True)


def node_tile(row):
    sub = sublane_iota()
    wide = jnp.broadcast_to(row, (8, LANES))
    tile = wide
    for r in range(1, 6):
        tile = jnp.where(sub == r, pltpu.roll(wide, LANES - 8 * r, 1), tile)
    return tile


def final_kernel(
    recv_ref,
    me_ref,
    disp_ref,
    force_ref,
    weight_ref,
    place_ref,
    new_disp_ref,
    res_ref,
    norm_ref,
    scratch,
):
    me = me_ref[0, 0]
    order = recv_ref[pl.ds(6, DEV, stride=8), :].astype(jnp.int32)
    special = recv_ref[pl.ds(7, DEV, stride=8), :]
    stress = [
        jnp.take_along_axis(recv_ref[pl.ds(m, DEV, stride=8), :].T, order, axis=1)
        for m in range(6)
    ]
    forces = lax.dot_general(
        jnp.concatenate(stress, axis=1),
        force_ref[...],
        (((1,), (0,)), ((), ())),
        precision=HIGHEST,
        preferred_element_type=jnp.float32,
    )
    home = sublane_iota(DEV)
    upper = forces[:, LANES:]
    lifted = jnp.where(home < 64, pltpu.roll(upper, 68, 0), pltpu.roll(upper, 64, 0))
    lifted = jnp.where(home < 4, 0.0, lifted)
    near = forces[:, :LANES] + lifted
    beside = jnp.where(home % 4 == 0, pltpu.roll(near, DEV - 3, 0), pltpu.roll(near, 1, 0))
    force = near + pltpu.roll(beside, LANES - NODES, 1)
    node = lane_iota(DEV) < NODES
    loads = jnp.where(node, special, 0.0)
    residual = jnp.where(node, special - force, 0.0)
    top = jnp.sum(jnp.sum(residual * residual, axis=0, keepdims=True), axis=1, keepdims=True)
    bottom = jnp.sum(jnp.sum(loads * loads, axis=0, keepdims=True), axis=1, keepdims=True)
    norm_ref[...] = jnp.sqrt(top / bottom)

    own_residual = row_of(residual, me)
    left = jnp.where(me % 4 == 0, me + 3, me - 1)
    under = jnp.where(me >= 64, 64, jnp.where(me < 4, 0, -60))
    turned = special.T
    diagonal = jnp.zeros((24, LANES), jnp.float32)
    for k, source in enumerate((me, left, me - under, left - under)):
        picks = jnp.broadcast_to(row_of(order, source), (16, LANES))
        terms = jnp.take_along_axis(turned[64 + 16 * k : 80 + 16 * k], picks, axis=1)
        corner = []
        for i in range(3):
            total = jnp.zeros((8, LANES), jnp.float32)
            for n, (_, _, t) in enumerate(diagonal_terms(i)):
                at = (i * 6 + n) * 8
                total = total + weight_ref[at : at + 8, :] * terms[t : t + 1]
            corner.append(total)
        diagonal = diagonal + lax.dot_general(
            jnp.concatenate(corner, axis=0),
            place_ref[k],
            (((1,), (0,)), ((), ())),
            precision=HIGHEST,
            preferred_element_type=jnp.float32,
        )
    lane = lane_iota(8)
    same = lane // 16 == sublane_iota()
    row = jnp.zeros((1, LANES), jnp.float32)
    for i in range(3):
        part = jnp.sum(jnp.where(same, diagonal[8 * i : 8 * i + 8], 0.0), axis=0, keepdims=True)
        for shift in (64, 32, 16):
            part = part + pltpu.roll(part, shift, 1)
        row = jnp.where(lane_iota() // 16 == i, part, row)
    moved = node_row(disp_ref, scratch, 0) + own_residual / jnp.maximum(row, FLOOR)
    for value, ref in ((moved, new_disp_ref), (own_residual, res_ref)):
        tile = node_tile(value)
        for i in range(3):
            ref[i, 0] = tile[2 * i : 2 * i + 2, 0:8]


def in_hbm(value):
    return pltpu.with_memory_space_constraint(value, pltpu.HBM)


def exchange(value):
    return lax.all_to_all(value, AXES, split_axis=0, concat_axis=0, tiled=True)


def run_pack(micro_state, state_slot, home_slot, displacement):
    return pl.pallas_call(
        pack_kernel,
        out_shape=jax.ShapeDtypeStruct((DEV * CHUNKS, LANES), jnp.float32),
        in_specs=[HBM] * 4,
        out_specs=VMEM,
        scratch_shapes=[
            pltpu.VMEM((WIDE, LANES), jnp.float32),
            pltpu.VMEM((1, LANES), jnp.int32),
            pltpu.VMEM((1, LANES), jnp.int32),
            pltpu.VMEM(displacement.shape, jnp.float32),
            pltpu.VMEM((8, LANES), jnp.float32),
            pltpu.SemaphoreType.DMA((PARTS + 3,)),
        ],
        compiler_params=pltpu.CompilerParams(vmem_limit_bytes=12 << 20),
        name="pack",
    )(
        in_hbm(micro_state.reshape(CASES * ROWS, LANES)),
        in_hbm(state_slot.reshape(1, LANES)),
        in_hbm(home_slot.reshape(1, LANES)),
        in_hbm(displacement),
    )


def run_solve(received, phases, phase_moduli, home_slot, load):
    f32 = jnp.float32
    big = pltpu.HBM((ROWS * 8, LANES), f32)
    return pl.pallas_call(
        solve_kernel,
        out_shape=(
            jax.ShapeDtypeStruct((DEV * 8, LANES), f32),
            big,
            big,
            big,
            jax.ShapeDtypeStruct((16, LANES), f32),
        ),
        in_specs=[VMEM, VMEM, SMEM, VMEM, VMEM],
        out_specs=[VMEM, HBM, HBM, HBM, VMEM],
        scratch_shapes=[
            pltpu.VMEM((ROWS * 8, LANES), f32),
            pltpu.VMEM((ROWS * 8, LANES), f32),
            pltpu.VMEM((ROWS * 8, LANES), f32),
            pltpu.VMEM((6 * VOX * 8, LANES), f32),
            pltpu.VMEM((VOX, LANES), f32),
            pltpu.VMEM((VOX, LANES), f32),
            pltpu.VMEM((VOX, LANES), f32),
            pltpu.VMEM((8, LANES), f32),
            pltpu.SemaphoreType.DMA((3,)),
        ],
        compiler_params=pltpu.CompilerParams(vmem_limit_bytes=32 << 20),
        name="solve",
    )(received, phases, phase_moduli, home_slot.reshape(1, LANES), load)


def run_update(w, p, q, steps):
    return pl.pallas_call(
        update_kernel,
        out_shape=jax.ShapeDtypeStruct((CASES, ROWS, LANES), jnp.float32),
        grid=(ROWS // UPDATE,),
        in_specs=[pl.BlockSpec((UPDATE * 8, LANES), lambda k: (k, 0))] * 3
        + [pl.BlockSpec((16, LANES), lambda k: (0, 0))],
        out_specs=pl.BlockSpec((CASES, UPDATE, LANES), lambda k: (0, k, 0)),
        compiler_params=pltpu.CompilerParams(vmem_limit_bytes=8 << 20),
        cost_estimate=pl.CostEstimate(
            flops=20_000_000, bytes_accessed=10_000_000, transcendentals=0
        ),
        name="update",
    )(in_hbm(w), in_hbm(p), in_hbm(q), steps)


def run_final(returned, me, displacement):
    force_table, weight_table, place_table = assembly_tables()
    node_shape = jax.ShapeDtypeStruct(displacement.shape, jnp.float32)
    return pl.pallas_call(
        final_kernel,
        out_shape=(node_shape, node_shape, jax.ShapeDtypeStruct((1, 1), jnp.float32)),
        in_specs=[VMEM, SMEM, VMEM, VMEM, VMEM, VMEM],
        out_specs=[VMEM] * 3,
        scratch_shapes=[pltpu.VMEM((8, LANES), jnp.float32)],
        compiler_params=pltpu.CompilerParams(vmem_limit_bytes=12 << 20),
        name="final",
    )(
        returned,
        me,
        displacement,
        jnp.asarray(force_table),
        jnp.asarray(weight_table),
        jnp.asarray(place_table),
    )


def per_device(displacement, load, home_slot, micro_state, state_slot, phases, phase_moduli):
    sent = run_pack(micro_state, state_slot, home_slot, displacement)
    received = exchange(sent.reshape(DEV, 1, WIDE)).reshape(DEV * CHUNKS, LANES)
    answer, w, p, q, steps = run_solve(received, phases, phase_moduli, home_slot, load)
    returned = exchange(answer.reshape(DEV, 8, LANES)).reshape(DEV * 8, LANES)
    new_state = run_update(w, p, q, steps)
    me = lax.axis_index(AXES).astype(jnp.int32).reshape(1, 1)
    displaced, residual, rel_norm = run_final(returned, me, displacement)
    return (
        new_state.reshape(micro_state.shape),
        displaced,
        residual,
        rel_norm.reshape(()),
    )


def solution(mesh):
    split = Mesh(mesh.devices.reshape(-1, 2, mesh.shape["rve"]), SPLIT)
    return jax.shard_map(
        per_device,
        mesh=split,
        in_specs=(
            P(None, SUB, "rve", None),
            P(None, SUB, "rve", None),
            P(SPLIT),
            P(None, None, None, SPLIT),
            P(SPLIT),
            P(None, SPLIT),
            P(),
        ),
        out_specs=(
            P(None, None, None, SPLIT),
            P(None, SUB, "rve", None),
            P(None, SUB, "rve", None),
            P(),
        ),
        check_vma=False,
    )
```

```python
import math

import jax
import jax.numpy as jnp
import numpy as np
from jax import lax
from jax.experimental import pallas as pl
from jax.experimental.pallas import tpu as pltpu
from jax.sharding import Mesh
from jax.sharding import PartitionSpec as P

R = 6
VOX = R * R * R
ROWS = 3 * VOX
CASES = 7
DEV = 128
LANES = 128
CHUNKS = 36
WIDE = CHUNKS * LANES
TAIL = CASES * ROWS - (CHUNKS - 1) * LANES
NODES = 48
STAB = 0.1
FLOOR = 1.0
SPLIT = ("far", "core", "rve")
AXES = ("core", "far", "rve")
SUB = ("far", "core")
PAIRS = ((0, 5, 4), (5, 1, 3), (4, 3, 2))
STRAIN_OF = ((0, 4, 5), (5, 1, 3), (4, 3, 2))
OFF_DIAGONAL = ((0, 4), (0, 5), (4, 5), (1, 3), (1, 5), (3, 5), (2, 3), (2, 4), (3, 4))
LOW = 0.5 - 0.5 / math.sqrt(3.0)
HIGH = 0.5 + 0.5 / math.sqrt(3.0)
HIGHEST = lax.Precision.HIGHEST
VMEM = pl.BlockSpec(memory_space=pltpu.VMEM)
SMEM = pl.BlockSpec(memory_space=pltpu.SMEM)
HBM = pl.BlockSpec(memory_space=pltpu.HBM)
CUTS = (0, 6, 36)
PARTS = len(CUTS) - 1
STEP = 6
UPDATE = 72


def strain_table():
    places = (LOW, HIGH)
    table = np.zeros((8, 8, 3, 6))
    for gauss in range(8):
        at = (places[gauss % 2], places[gauss // 2 % 2], places[gauss // 4])
        for corner in range(8):
            bits = (corner % 2, corner // 2 % 2, corner // 4)
            weight = [at[k] if bits[k] else 1.0 - at[k] for k in range(3)]
            sign = [1.0 if bits[k] else -1.0 for k in range(3)]
            dx = sign[0] * weight[1] * weight[2]
            dy = weight[0] * sign[1] * weight[2]
            dz = weight[0] * weight[1] * sign[2]
            table[gauss, corner, 0, [0, 4, 5]] = (dx, dz, dy)
            table[gauss, corner, 1, [1, 3, 5]] = (dy, dz, dx)
            table[gauss, corner, 2, [2, 3, 4]] = (dz, dy, dx)
    return table


def term_index(first, second):
    if first == second:
        return first
    return 6 + OFF_DIAGONAL.index((min(first, second), max(first, second)))


def diagonal_terms(component):
    m = STRAIN_OF[component]
    pairs = [(m[0], m[0]), (m[1], m[1]), (m[2], m[2]), (m[0], m[1]), (m[0], m[2]), (m[1], m[2])]
    return [(a, b, term_index(a, b)) for a, b in pairs]


def assembly_tables():
    table = strain_table()
    force = np.zeros((6, LANES, 2 * LANES), np.float32)
    weights = np.zeros((3, 6, 8, LANES), np.float32)
    place = np.zeros((4, LANES, LANES), np.float32)
    for j in range(LANES):
        ly, ex, gauss = j // 64, j // 8 % 8, j % 8
        for corner in range(8):
            az, row, col = corner // 4, ly + corner // 2 % 2, (ex + corner % 2) % 8
            for i in range(3):
                lane = az * LANES + (NODES if row == 2 else 0) + i * 16 + row % 2 * 8 + col
                for m in STRAIN_OF[i]:
                    force[m, j, lane] += 0.125 * table[gauss, corner, i, m]
                for n, (first, second, _) in enumerate(diagonal_terms(i)):
                    weights[i, n, corner, j] = (
                        0.125 * table[gauss, corner, i, first] * table[gauss, corner, i, second]
                    )
            place[az * 2 + (1 if row == 2 else 0), j, corner * 16 + row % 2 * 8 + col] = 1.0
    return force.reshape(6 * LANES, 2 * LANES), weights.reshape(18 * 8, LANES), place


def lane_iota(rows=1):
    return lax.broadcasted_iota(jnp.int32, (rows, LANES), 1)


def sublane_iota(rows=8):
    return lax.broadcasted_iota(jnp.int32, (rows, LANES), 0)


def node_row(ref, scratch, offset):
    scratch[...] = jnp.zeros((8, LANES), jnp.float32)
    for i in range(3):
        scratch[2 * i : 2 * i + 2, 0:8] = ref[i, 0]
    tile = scratch[...]
    total = jnp.zeros((1, LANES), jnp.float32)
    for row in range(6):
        total = total + pltpu.roll(tile[row : row + 1], offset + 8 * row, 1)
    return total


def previous_row_lanes(value):
    lane = lane_iota(value.shape[0])
    return jnp.where(lane % 4 == 0, pltpu.roll(value, LANES - 3, 1), pltpu.roll(value, 1, 1))


def next_row_lanes(value):
    lane = lane_iota(value.shape[0])
    return jnp.where(lane % 4 == 3, pltpu.roll(value, 3, 1), pltpu.roll(value, LANES - 1, 1))


def below_lanes(value):
    lane = lane_iota(value.shape[0])
    moved = jnp.where(lane < 64, pltpu.roll(value, 68, 1), pltpu.roll(value, 64, 1))
    return jnp.where(lane < 4, 0.0, moved)


def above_lanes(value):
    lane = lane_iota(value.shape[0])
    moved = jnp.where(lane < 64, pltpu.roll(value, 64, 1), pltpu.roll(value, 60, 1))
    return jnp.where(lane >= 124, 0.0, moved)


def device_at(place):
    return ((place >> 2) & 15) * 8 + (place >> 6) * 4 + (place & 3)


def place_of(device):
    return ((device >> 2) & 1) * 64 + (device >> 3) * 4 + (device & 3)


def part_copy(src, dst, sems, part):
    start, stop = CUTS[part] * LANES, min(CUTS[part + 1] * LANES, CASES * ROWS)
    rows = pl.ds(start, stop - start)
    return pltpu.make_async_copy(src.at[rows], dst.at[rows], sems.at[part])


def split_bf16(value):
    high = value.astype(jnp.bfloat16)
    rest = value - high.astype(jnp.float32)
    middle = rest.astype(jnp.bfloat16)
    low = (rest - middle.astype(jnp.float32)).astype(jnp.bfloat16)
    return high, middle, low


def flip(same, block):
    high, middle, low = (
        lax.dot_general(
            same, part, (((1,), (1,)), ((), ())), preferred_element_type=jnp.float32
        )
        for part in split_bf16(block)
    )
    return (high + middle) + low


def pack_kernel(
    state_ref,
    state_slot_hbm,
    home_slot_hbm,
    disp_hbm,
    out_ref,
    held_ref,
    state_slot_ref,
    home_slot_ref,
    disp_ref,
    scratch,
    sems,
):
    small = [
        pltpu.make_async_copy(src, dst, sems.at[PARTS + k])
        for k, (src, dst) in enumerate(
            (
                (state_slot_hbm, state_slot_ref),
                (home_slot_hbm, home_slot_ref),
                (disp_hbm, disp_ref),
            )
        )
    ]
    for copy in small:
        copy.start()
    for part in range(PARTS):
        part_copy(state_ref, held_ref, sems, part).start()
    owner = device_at(sublane_iota(DEV))
    lane = lane_iota(DEV)
    for copy in small:
        copy.wait()
    choose = ((state_slot_ref[...] >> 7) == owner).astype(jnp.float32).astype(jnp.bfloat16)
    twice = jnp.concatenate([choose, choose], axis=1)
    home = (home_slot_ref[...] >> 7) == owner
    local = jnp.sum(jnp.where(home, lane, 0).astype(jnp.float32), axis=1, keepdims=True)
    extra = node_row(disp_ref, scratch, TAIL) + jnp.where(lane == TAIL + NODES, local, 0.0)
    held_ref[CASES * ROWS :, :] = jnp.zeros((WIDE - CASES * ROWS, LANES), jnp.float32)
    for part in range(PARTS):
        part_copy(state_ref, held_ref, sems, part).wait()
        for first in range(CUTS[part], CUTS[part + 1], STEP):
            high, middle, low = split_bf16(held_ref[first * LANES : (first + STEP) * LANES, :])
            picked = lax.dot_general(
                jnp.concatenate([high, middle], axis=1),
                twice,
                (((1,), (1,)), ((), ())),
                preferred_element_type=jnp.float32,
            )
            picked = picked + lax.dot_general(
                low, choose, (((1,), (1,)), ((), ())), preferred_element_type=jnp.float32
            )
            for k in range(first, first + STEP):
                turned = picked[(k - first) * LANES : (k - first + 1) * LANES].T
                if k == CHUNKS - 1:
                    turned = turned + extra
                out_ref[pl.ds(k, DEV, stride=CHUNKS), :] = turned


def macro_strain_rows(tail):
    local = tail[TAIL + NODES : TAIL + NODES + 1].astype(jnp.int32)
    upper = (local >> 6) == 1
    ex = (local >> 3) & 7
    point = [jnp.where(((local >> k) & 1) == 1, HIGH, LOW) for k in range(3)]
    shape = [(1.0 - point[k], point[k]) for k in range(3)]
    sub = sublane_iota()
    hits = (sub == ex, sub == ((ex + 1) & 7))
    slopes = []
    for i in range(3):
        own = [tail[TAIL + 16 * i + 8 * y : TAIL + 16 * i + 8 * y + 8] for y in range(2)]
        rows = [own[0], own[1], next_row_lanes(own[0])]
        planes = [rows, [above_lanes(row) for row in rows]]
        at = {}
        for az in range(2):
            for ay in range(2):
                chosen = jnp.where(upper, planes[az][ay + 1], planes[az][ay])
                for ax in range(2):
                    at[az, ay, ax] = jnp.sum(
                        jnp.where(hits[ax], chosen, 0.0), axis=0, keepdims=True
                    )
        sx, sy, sz = shape
        slope = [0.0, 0.0, 0.0]
        for first in range(2):
            for second in range(2):
                slope[0] = slope[0] + sz[first] * sy[second] * (
                    at[first, second, 1] - at[first, second, 0]
                )
                slope[1] = slope[1] + sz[first] * sx[second] * (
                    at[first, 1, second] - at[first, 0, second]
                )
                slope[2] = slope[2] + sy[first] * sx[second] * (
                    at[1, first, second] - at[0, first, second]
                )
        slopes.append(slope)
    return [
        slopes[0][0],
        slopes[1][1],
        slopes[2][2],
        slopes[1][2] + slopes[2][1],
        slopes[0][2] + slopes[2][0],
        slopes[0][1] + slopes[1][0],
    ]


def tile_at(ref, base, row):
    return ref[pl.ds(base + row * 8, 8), :]


def solve_kernel(
    recv_ref,
    phase_ref,
    moduli_ref,
    slot_ref,
    load_ref,
    ret_ref,
    w_out,
    p_out,
    q_out,
    step_ref,
    w_ref,
    p_ref,
    q_ref,
    sig_ref,
    lam_ref,
    mu_ref,
    mu2_ref,
    scratch,
    sems,
):
    saves = [
        pltpu.make_async_copy(src, dst, sems.at[k])
        for k, (src, dst) in enumerate(((w_ref, w_out), (p_ref, p_out), (q_ref, q_out)))
    ]

    def save_plane(base):
        for i in range(3):
            rows = pl.ds(base + i * VOX * 8, 288)
            pltpu.make_async_copy(q_ref.at[rows], q_out.at[rows], sems.at[2]).start()

    zero = jnp.zeros((8, LANES), jnp.float32)
    phase = jnp.take_along_axis(phase_ref[...], device_at(lane_iota(VOX)), axis=1)
    mu = jnp.where(
        phase == 0, moduli_ref[1:2, 0:1], jnp.where(phase == 1, moduli_ref[1:2, 1:2], moduli_ref[1:2, 2:3])
    )
    lam_ref[...] = jnp.where(
        phase == 0, moduli_ref[0:1, 0:1], jnp.where(phase == 1, moduli_ref[0:1, 1:2], moduli_ref[0:1, 2:3])
    )
    mu_ref[...] = mu
    mu2_ref[...] = mu + mu
    w_ref[pl.ds(7, ROWS, stride=8), :] = jnp.zeros((ROWS, LANES), jnp.float32)
    tail = None
    same = (sublane_iota(DEV) == lane_iota(DEV)).astype(jnp.float32).astype(jnp.bfloat16)
    for k in range(CHUNKS):
        block = recv_ref[pl.ds(k, DEV, stride=CHUNKS), :]
        turned = flip(same, block) if k % 3 == 1 else block.T
        start, stop = k * LANES, min((k + 1) * LANES, CASES * ROWS)
        while start < stop:
            case = start // ROWS
            end = min(stop, (case + 1) * ROWS)
            w_ref[pl.ds((start - case * ROWS) * 8 + case, end - start, stride=8), :] = turned[
                start - k * LANES : end - k * LANES
            ]
            start = end
        tail = turned
    saves[0].start()
    macro = macro_strain_rows(tail)
    sub = sublane_iota()
    imposed = [
        jnp.where(sub == 0, macro[m], jnp.where(sub == m + 1, 1.0, 0.0)) for m in range(6)
    ]

    def stress_pass(src, strain, keep, energy):
        def plane(a, carry):
            sums, work = list(carry[0]), carry[1]
            base = pl.multiple_of(a * 288, 8)
            ahead = pl.multiple_of(jnp.where(a == R - 1, 0, (a + 1) * 288), 8)
            voxel = a * 36
            line = [[tile_at(src, base, i * VOX + c) for c in range(R)] for i in range(3)]
            for b in range(R):
                nb = (b + 1) % R
                below = [
                    [tile_at(src, base, i * VOX + nb * R + c) for c in range(R)] for i in range(3)
                ]
                for c in range(R):
                    at = b * R + c
                    here = [line[i][c] for i in range(3)]
                    grad = [
                        [
                            tile_at(src, ahead, i * VOX + at) - here[i],
                            below[i][c] - here[i],
                            line[i][(c + 1) % R] - here[i],
                        ]
                        for i in range(3)
                    ]
                    eps = [
                        grad[0][0],
                        grad[1][1],
                        grad[2][2],
                        grad[1][2] + grad[2][1],
                        grad[0][2] + grad[2][0],
                        grad[0][1] + grad[1][0],
                    ]
                    if strain is not None:
                        eps = [eps[m] + strain[m] for m in range(6)]
                    lam = lam_ref[pl.ds(voxel + at, 8, stride=0), :]
                    mu1 = mu_ref[pl.ds(voxel + at, 8, stride=0), :]
                    mu2 = mu2_ref[pl.ds(voxel + at, 8, stride=0), :]
                    bulk = lam * (eps[0] + eps[1] + eps[2])
                    sig = [bulk + mu2 * eps[m] for m in range(3)]
                    sig += [mu1 * eps[m] for m in range(3, 6)]
                    for m in range(6):
                        sums[m] = sums[m] + sig[m]
                        if keep:
                            sig_ref[pl.ds(base + (m * VOX + at) * 8, 8), :] = sig[m]
                    if energy:
                        work = work + (
                            (sig[0] * eps[0] + sig[1] * eps[1])
                            + (sig[2] * eps[2] + sig[3] * eps[3])
                            + (sig[4] * eps[4] + sig[5] * eps[5])
                        )
                line = below
            return tuple(sums), work

        return lax.fori_loop(0, R, plane, ((zero,) * 6, zero), unroll=2)

    def force_pass(src, finish, dst):
        def plane(a, carry):
            totals = list(carry)
            base = pl.multiple_of(a * 288, 8)
            behind = pl.multiple_of(jnp.where(a == 0, (R - 1) * 288, (a - 1) * 288), 8)
            for b in range(R):
                pb = (b + R - 1) % R
                last = [tile_at(sig_ref, base, PAIRS[2][i] * VOX + b * R + R - 1) for i in range(3)]
                for c in range(R):
                    at = b * R + c
                    own = [tile_at(sig_ref, base, m * VOX + at) for m in range(6)]
                    for i in range(3):
                        gone = (own[PAIRS[0][i]] + own[PAIRS[1][i]]) + own[PAIRS[2][i]]
                        come = (
                            tile_at(sig_ref, behind, PAIRS[0][i] * VOX + at)
                            + tile_at(sig_ref, base, PAIRS[1][i] * VOX + pb * R + c)
                        ) + last[i]
                        value = finish(come, gone, tile_at(src, base, i * VOX + at))
                        dst[pl.ds(base + (i * VOX + at) * 8, 8), :] = value
                        totals[i] = totals[i] + value * value
                    last = [own[PAIRS[2][i]] for i in range(3)]
            return tuple(totals)

        totals = lax.fori_loop(0, R, plane, (zero,) * 3, unroll=2)
        return (totals[0] + totals[1]) + totals[2]

    mean0, _ = stress_pass(w_ref, imposed, True, False)
    square0 = force_pass(w_ref, lambda come, gone, w: (gone - come) - STAB * w, p_ref)
    saves[1].start()
    mean1, work1 = stress_pass(p_ref, None, True, True)
    step0 = square0 / (work1 + STAB * square0)
    kept = 1.0 - STAB * step0
    square1 = force_pass(p_ref, lambda come, gone, p: kept * p - step0 * (come - gone), q_ref)
    ratio = square1 / square0

    def direction(a, carry):
        base = pl.multiple_of(a * 288, 8)
        for at in range(36):
            for i in range(3):
                q_ref[pl.ds(base + (i * VOX + at) * 8, 8), :] = tile_at(
                    q_ref, base, i * VOX + at
                ) + ratio * tile_at(p_ref, base, i * VOX + at)
        save_plane(base)
        return carry

    lax.fori_loop(0, R, direction, 0)
    length = square1 + ratio * square1
    mean2, work2 = stress_pass(q_ref, None, False, True)
    step1 = square1 / (work2 + STAB * length)
    step_ref[0:8, :] = step0
    step_ref[8:16, :] = step1
    mean = [(mean0[m] + step0 * mean1[m] + step1 * mean2[m]) * (1.0 / VOX) for m in range(6)]

    shared = place_of(slot_ref[...] >> 7).astype(jnp.float32)
    shared = jnp.broadcast_to(shared, (8, LANES))
    for m in range(6):
        shared = jnp.where(sub == m, mean[m][0:1], shared)
    terms = [mean[m][m + 1 : m + 2] for m in range(6)]
    for first, second in OFF_DIAGONAL:
        terms.append(mean[first][second + 1 : second + 2] + mean[second][first + 1 : first + 2])
    own = jnp.concatenate(terms + [jnp.zeros((1, LANES), jnp.float32)], axis=0)
    left = previous_row_lanes(own)
    stacked = jnp.concatenate(
        [jnp.zeros((64, LANES), jnp.float32), own, left, below_lanes(own), below_lanes(left)],
        axis=0,
    )
    special = stacked.T + node_row(load_ref, scratch, 0)
    for peer in range(DEV):
        ret_ref[8 * peer : 8 * peer + 8, :] = shared
    ret_ref[pl.ds(7, DEV, stride=8), :] = special
    for save in saves:
        save.wait()


def update_kernel(w_ref, p_ref, q_ref, step_ref, out_ref):
    place = place_of(lane_iota(UPDATE))
    for case in range(CASES):
        first = step_ref[case : case + 1, :]
        second = step_ref[8 + case : 9 + case, :]
        rows = pl.ds(case, UPDATE, stride=8)
        value = w_ref[rows, :] + first * p_ref[rows, :] + second * q_ref[rows, :]
        out_ref[case] = jnp.take_along_axis(value, place, axis=1)


def row_of(value, index):
    return jnp.sum(jnp.where(sublane_iota(DEV) == index, value, 0), axis=0, keepdims=True)


def node_tile(row):
    sub = sublane_iota()
    wide = jnp.broadcast_to(row, (8, LANES))
    tile = wide
    for r in range(1, 6):
        tile = jnp.where(sub == r, pltpu.roll(wide, LANES - 8 * r, 1), tile)
    return tile


def final_kernel(
    recv_ref,
    me_ref,
    disp_ref,
    force_ref,
    weight_ref,
    place_ref,
    new_disp_ref,
    res_ref,
    norm_ref,
    scratch,
):
    me = me_ref[...]
    order = recv_ref[pl.ds(6, DEV, stride=8), :].astype(jnp.int32)
    special = recv_ref[pl.ds(7, DEV, stride=8), :]
    stress = [
        jnp.take_along_axis(recv_ref[pl.ds(m, DEV, stride=8), :].T, order, axis=1)
        for m in range(6)
    ]
    forces = lax.dot_general(
        jnp.concatenate(stress, axis=1),
        force_ref[...],
        (((1,), (0,)), ((), ())),
        precision=HIGHEST,
        preferred_element_type=jnp.float32,
    )
    home = sublane_iota(DEV)
    upper = forces[:, LANES:]
    lifted = jnp.where(home < 64, pltpu.roll(upper, 68, 0), pltpu.roll(upper, 64, 0))
    lifted = jnp.where(home < 4, 0.0, lifted)
    near = forces[:, :LANES] + lifted
    beside = jnp.where(home % 4 == 0, pltpu.roll(near, DEV - 3, 0), pltpu.roll(near, 1, 0))
    force = near + pltpu.roll(beside, LANES - NODES, 1)
    node = lane_iota(DEV) < NODES
    loads = jnp.where(node, special, 0.0)
    residual = jnp.where(node, special - force, 0.0)
    top = jnp.sum(jnp.sum(residual * residual, axis=0, keepdims=True), axis=1, keepdims=True)
    bottom = jnp.sum(jnp.sum(loads * loads, axis=0, keepdims=True), axis=1, keepdims=True)
    norm_ref[...] = jnp.sqrt(top / bottom)

    own_residual = row_of(residual, me)
    left = jnp.where(me % 4 == 0, me + 3, me - 1)
    under = jnp.where(me >= 64, 64, jnp.where(me < 4, 0, -60))
    turned = special.T
    diagonal = jnp.zeros((24, LANES), jnp.float32)
    for k, source in enumerate((me, left, me - under, left - under)):
        picks = jnp.broadcast_to(row_of(order, source), (16, LANES))
        terms = jnp.take_along_axis(turned[64 + 16 * k : 80 + 16 * k], picks, axis=1)
        corner = []
        for i in range(3):
            total = jnp.zeros((8, LANES), jnp.float32)
            for n, (_, _, t) in enumerate(diagonal_terms(i)):
                at = (i * 6 + n) * 8
                total = total + weight_ref[at : at + 8, :] * terms[t : t + 1]
            corner.append(total)
        diagonal = diagonal + lax.dot_general(
            jnp.concatenate(corner, axis=0),
            place_ref[k],
            (((1,), (0,)), ((), ())),
            precision=HIGHEST,
            preferred_element_type=jnp.float32,
        )
    lane = lane_iota(8)
    same = lane // 16 == sublane_iota()
    row = jnp.zeros((1, LANES), jnp.float32)
    for i in range(3):
        part = jnp.sum(jnp.where(same, diagonal[8 * i : 8 * i + 8], 0.0), axis=0, keepdims=True)
        for shift in (64, 32, 16):
            part = part + pltpu.roll(part, shift, 1)
        row = jnp.where(lane_iota() // 16 == i, part, row)
    moved = node_row(disp_ref, scratch, 0) + own_residual / jnp.maximum(row, FLOOR)
    for value, ref in ((moved, new_disp_ref), (own_residual, res_ref)):
        tile = node_tile(value)
        for i in range(3):
            ref[i, 0] = tile[2 * i : 2 * i + 2, 0:8]


def in_hbm(value):
    return pltpu.with_memory_space_constraint(value, pltpu.HBM)


def exchange(value):
    return lax.all_to_all(value, AXES, split_axis=0, concat_axis=0, tiled=True)


def run_pack(micro_state, state_slot, home_slot, displacement):
    return pl.pallas_call(
        pack_kernel,
        out_shape=jax.ShapeDtypeStruct((DEV * CHUNKS, LANES), jnp.float32),
        in_specs=[HBM] * 4,
        out_specs=VMEM,
        scratch_shapes=[
            pltpu.VMEM((WIDE, LANES), jnp.float32),
            pltpu.VMEM((1, LANES), jnp.int32),
            pltpu.VMEM((1, LANES), jnp.int32),
            pltpu.VMEM(displacement.shape, jnp.float32),
            pltpu.VMEM((8, LANES), jnp.float32),
            pltpu.SemaphoreType.DMA((PARTS + 3,)),
        ],
        compiler_params=pltpu.CompilerParams(vmem_limit_bytes=12 << 20),
        name="pack",
    )(
        in_hbm(micro_state.reshape(CASES * ROWS, LANES)),
        in_hbm(state_slot.reshape(1, LANES)),
        in_hbm(home_slot.reshape(1, LANES)),
        in_hbm(displacement),
    )


def run_solve(received, phases, phase_moduli, home_slot, load):
    f32 = jnp.float32
    big = pltpu.HBM((ROWS * 8, LANES), f32)
    return pl.pallas_call(
        solve_kernel,
        out_shape=(
            jax.ShapeDtypeStruct((DEV * 8, LANES), f32),
            big,
            big,
            big,
            jax.ShapeDtypeStruct((16, LANES), f32),
        ),
        in_specs=[VMEM, VMEM, VMEM, VMEM, VMEM],
        out_specs=[VMEM, HBM, HBM, HBM, VMEM],
        scratch_shapes=[
            pltpu.VMEM((ROWS * 8, LANES), f32),
            pltpu.VMEM((ROWS * 8, LANES), f32),
            pltpu.VMEM((ROWS * 8, LANES), f32),
            pltpu.VMEM((6 * VOX * 8, LANES), f32),
            pltpu.VMEM((VOX, LANES), f32),
            pltpu.VMEM((VOX, LANES), f32),
            pltpu.VMEM((VOX, LANES), f32),
            pltpu.VMEM((8, LANES), f32),
            pltpu.SemaphoreType.DMA((3,)),
        ],
        compiler_params=pltpu.CompilerParams(vmem_limit_bytes=32 << 20),
        name="solve",
    )(received, phases, phase_moduli, home_slot.reshape(1, LANES), load)


def run_update(w, p, q, steps):
    return pl.pallas_call(
        update_kernel,
        out_shape=jax.ShapeDtypeStruct((CASES, ROWS, LANES), jnp.float32),
        grid=(ROWS // UPDATE,),
        in_specs=[pl.BlockSpec((UPDATE * 8, LANES), lambda k: (k, 0))] * 3
        + [pl.BlockSpec((16, LANES), lambda k: (0, 0))],
        out_specs=pl.BlockSpec((CASES, UPDATE, LANES), lambda k: (0, k, 0)),
        compiler_params=pltpu.CompilerParams(vmem_limit_bytes=8 << 20),
        cost_estimate=pl.CostEstimate(
            flops=20_000_000, bytes_accessed=10_000_000, transcendentals=0
        ),
        name="update",
    )(in_hbm(w), in_hbm(p), in_hbm(q), steps)


def run_final(returned, me, displacement):
    force_table, weight_table, place_table = assembly_tables()
    node_shape = jax.ShapeDtypeStruct(displacement.shape, jnp.float32)
    return pl.pallas_call(
        final_kernel,
        out_shape=(node_shape, node_shape, jax.ShapeDtypeStruct((1, 1), jnp.float32)),
        in_specs=[VMEM] * 6,
        out_specs=[VMEM] * 3,
        scratch_shapes=[pltpu.VMEM((8, LANES), jnp.float32)],
        compiler_params=pltpu.CompilerParams(vmem_limit_bytes=12 << 20),
        name="final",
    )(
        returned,
        me,
        displacement,
        jnp.asarray(force_table),
        jnp.asarray(weight_table),
        jnp.asarray(place_table),
    )


def per_device(displacement, load, home_slot, micro_state, state_slot, phases, phase_moduli):
    sent = run_pack(micro_state, state_slot, home_slot, displacement)
    received = exchange(sent.reshape(DEV, 1, WIDE)).reshape(DEV * CHUNKS, LANES)
    answer, w, p, q, steps = run_solve(received, phases, phase_moduli, home_slot, load)
    returned = exchange(answer.reshape(DEV, 8, LANES)).reshape(DEV * 8, LANES)
    new_state = run_update(w, p, q, steps)
    me = jnp.full((1, LANES), lax.axis_index(AXES), jnp.int32)
    displaced, residual, rel_norm = run_final(returned, me, displacement)
    return (
        new_state.reshape(micro_state.shape),
        displaced,
        residual,
        rel_norm.reshape(()),
    )


def solution(mesh):
    split = Mesh(mesh.devices.reshape(-1, 2, mesh.shape["rve"]), SPLIT)
    return jax.shard_map(
        per_device,
        mesh=split,
        in_specs=(
            P(None, SUB, "rve", None),
            P(None, SUB, "rve", None),
            P(SPLIT),
            P(None, None, None, SPLIT),
            P(SPLIT),
            P(None, SPLIT),
            P(),
        ),
        out_specs=(
            P(None, None, None, SPLIT),
            P(None, SUB, "rve", None),
            P(None, SUB, "rve", None),
            P(),
        ),
        check_vma=False,
    )
```

```python
import math

import jax
import jax.numpy as jnp
import numpy as np
from jax import lax
from jax.experimental import pallas as pl
from jax.experimental.pallas import tpu as pltpu
from jax.sharding import Mesh
from jax.sharding import PartitionSpec as P

R = 6
VOX = R * R * R
ROWS = 3 * VOX
CASES = 7
DEV = 128
LANES = 128
CHUNKS = 36
WIDE = CHUNKS * LANES
TAIL = CASES * ROWS - (CHUNKS - 1) * LANES
NODES = 48
STAB = 0.1
FLOOR = 1.0
SPLIT = ("far", "core", "rve")
AXES = ("core", "far", "rve")
SUB = ("far", "core")
PAIRS = ((0, 5, 4), (5, 1, 3), (4, 3, 2))
STRAIN_OF = ((0, 4, 5), (5, 1, 3), (4, 3, 2))
OFF_DIAGONAL = ((0, 4), (0, 5), (4, 5), (1, 3), (1, 5), (3, 5), (2, 3), (2, 4), (3, 4))
LOW = 0.5 - 0.5 / math.sqrt(3.0)
HIGH = 0.5 + 0.5 / math.sqrt(3.0)
HIGHEST = lax.Precision.HIGHEST
VMEM = pl.BlockSpec(memory_space=pltpu.VMEM)
SMEM = pl.BlockSpec(memory_space=pltpu.SMEM)
HBM = pl.BlockSpec(memory_space=pltpu.HBM)
CUTS = (0, 6, 36)
PARTS = len(CUTS) - 1
STEP = 6
PITCH = ROWS + 1


def strain_table():
    places = (LOW, HIGH)
    table = np.zeros((8, 8, 3, 6))
    for gauss in range(8):
        at = (places[gauss % 2], places[gauss // 2 % 2], places[gauss // 4])
        for corner in range(8):
            bits = (corner % 2, corner // 2 % 2, corner // 4)
            weight = [at[k] if bits[k] else 1.0 - at[k] for k in range(3)]
            sign = [1.0 if bits[k] else -1.0 for k in range(3)]
            dx = sign[0] * weight[1] * weight[2]
            dy = weight[0] * sign[1] * weight[2]
            dz = weight[0] * weight[1] * sign[2]
            table[gauss, corner, 0, [0, 4, 5]] = (dx, dz, dy)
            table[gauss, corner, 1, [1, 3, 5]] = (dy, dz, dx)
            table[gauss, corner, 2, [2, 3, 4]] = (dz, dy, dx)
    return table


def term_index(first, second):
    if first == second:
        return first
    return 6 + OFF_DIAGONAL.index((min(first, second), max(first, second)))


def diagonal_terms(component):
    m = STRAIN_OF[component]
    pairs = [(m[0], m[0]), (m[1], m[1]), (m[2], m[2]), (m[0], m[1]), (m[0], m[2]), (m[1], m[2])]
    return [(a, b, term_index(a, b)) for a, b in pairs]


def assembly_tables():
    table = strain_table()
    force = np.zeros((6, LANES, 2 * LANES), np.float32)
    weights = np.zeros((3, 6, 8, LANES), np.float32)
    place = np.zeros((4, LANES, LANES), np.float32)
    for j in range(LANES):
        ly, ex, gauss = j // 64, j // 8 % 8, j % 8
        for corner in range(8):
            az, row, col = corner // 4, ly + corner // 2 % 2, (ex + corner % 2) % 8
            for i in range(3):
                lane = az * LANES + (NODES if row == 2 else 0) + i * 16 + row % 2 * 8 + col
                for m in STRAIN_OF[i]:
                    force[m, j, lane] += 0.125 * table[gauss, corner, i, m]
                for n, (first, second, _) in enumerate(diagonal_terms(i)):
                    weights[i, n, corner, j] = (
                        0.125 * table[gauss, corner, i, first] * table[gauss, corner, i, second]
                    )
            place[az * 2 + (1 if row == 2 else 0), j, corner * 16 + row % 2 * 8 + col] = 1.0
    return force.reshape(6 * LANES, 2 * LANES), weights.reshape(18 * 8, LANES), place


def lane_iota(rows=1):
    return lax.broadcasted_iota(jnp.int32, (rows, LANES), 1)


def sublane_iota(rows=8):
    return lax.broadcasted_iota(jnp.int32, (rows, LANES), 0)


def node_row(ref, scratch, offset):
    scratch[...] = jnp.zeros((8, LANES), jnp.float32)
    for i in range(3):
        scratch[2 * i : 2 * i + 2, 0:8] = ref[i, 0]
    tile = scratch[...]
    total = jnp.zeros((1, LANES), jnp.float32)
    for row in range(6):
        total = total + pltpu.roll(tile[row : row + 1], offset + 8 * row, 1)
    return total


def previous_row_lanes(value):
    lane = lane_iota(value.shape[0])
    return jnp.where(lane % 4 == 0, pltpu.roll(value, LANES - 3, 1), pltpu.roll(value, 1, 1))


def next_row_lanes(value):
    lane = lane_iota(value.shape[0])
    return jnp.where(lane % 4 == 3, pltpu.roll(value, 3, 1), pltpu.roll(value, LANES - 1, 1))


def below_lanes(value):
    lane = lane_iota(value.shape[0])
    moved = jnp.where(lane < 64, pltpu.roll(value, 68, 1), pltpu.roll(value, 64, 1))
    return jnp.where(lane < 4, 0.0, moved)


def above_lanes(value):
    lane = lane_iota(value.shape[0])
    moved = jnp.where(lane < 64, pltpu.roll(value, 64, 1), pltpu.roll(value, 60, 1))
    return jnp.where(lane >= 124, 0.0, moved)


def device_at(place):
    return ((place >> 2) & 15) * 8 + (place >> 6) * 4 + (place & 3)


def place_of(device):
    return ((device >> 2) & 1) * 64 + (device >> 3) * 4 + (device & 3)


def part_copy(src, dst, sems, part):
    start, stop = CUTS[part] * LANES, min(CUTS[part + 1] * LANES, CASES * ROWS)
    rows = pl.ds(start, stop - start)
    return pltpu.make_async_copy(src.at[rows], dst.at[rows], sems.at[part])


def split_bf16(value):
    high = value.astype(jnp.bfloat16)
    rest = value - high.astype(jnp.float32)
    middle = rest.astype(jnp.bfloat16)
    low = (rest - middle.astype(jnp.float32)).astype(jnp.bfloat16)
    return high, middle, low


def flip(same, block):
    high, middle, low = (
        lax.dot_general(
            same, part, (((1,), (1,)), ((), ())), preferred_element_type=jnp.float32
        )
        for part in split_bf16(block)
    )
    return (high + middle) + low


def pack_kernel(
    state_ref,
    state_slot_hbm,
    home_slot_hbm,
    disp_hbm,
    out_ref,
    held_ref,
    state_slot_ref,
    home_slot_ref,
    disp_ref,
    scratch,
    sems,
):
    small = [
        pltpu.make_async_copy(src, dst, sems.at[PARTS + k])
        for k, (src, dst) in enumerate(
            (
                (state_slot_hbm, state_slot_ref),
                (home_slot_hbm, home_slot_ref),
                (disp_hbm, disp_ref),
            )
        )
    ]
    for copy in small:
        copy.start()
    for part in range(PARTS):
        part_copy(state_ref, held_ref, sems, part).start()
    owner = device_at(sublane_iota(DEV))
    lane = lane_iota(DEV)
    for copy in small:
        copy.wait()
    choose = ((state_slot_ref[...] >> 7) == owner).astype(jnp.float32).astype(jnp.bfloat16)
    twice = jnp.concatenate([choose, choose], axis=1)
    home = (home_slot_ref[...] >> 7) == owner
    local = jnp.sum(jnp.where(home, lane, 0).astype(jnp.float32), axis=1, keepdims=True)
    extra = node_row(disp_ref, scratch, TAIL) + jnp.where(lane == TAIL + NODES, local, 0.0)
    held_ref[CASES * ROWS :, :] = jnp.zeros((WIDE - CASES * ROWS, LANES), jnp.float32)
    for part in range(PARTS):
        part_copy(state_ref, held_ref, sems, part).wait()
        for first in range(CUTS[part], CUTS[part + 1], STEP):
            high, middle, low = split_bf16(held_ref[first * LANES : (first + STEP) * LANES, :])
            picked = lax.dot_general(
                jnp.concatenate([high, middle], axis=1),
                twice,
                (((1,), (1,)), ((), ())),
                preferred_element_type=jnp.float32,
            )
            picked = picked + lax.dot_general(
                low, choose, (((1,), (1,)), ((), ())), preferred_element_type=jnp.float32
            )
            for k in range(first, first + STEP):
                turned = picked[(k - first) * LANES : (k - first + 1) * LANES].T
                if k == CHUNKS - 1:
                    turned = turned + extra
                out_ref[pl.ds(k, DEV, stride=CHUNKS), :] = turned


def macro_strain_rows(tail):
    local = tail[TAIL + NODES : TAIL + NODES + 1].astype(jnp.int32)
    upper = (local >> 6) == 1
    ex = (local >> 3) & 7
    point = [jnp.where(((local >> k) & 1) == 1, HIGH, LOW) for k in range(3)]
    shape = [(1.0 - point[k], point[k]) for k in range(3)]
    sub = sublane_iota()
    hits = (sub == ex, sub == ((ex + 1) & 7))
    slopes = []
    for i in range(3):
        own = [tail[TAIL + 16 * i + 8 * y : TAIL + 16 * i + 8 * y + 8] for y in range(2)]
        rows = [own[0], own[1], next_row_lanes(own[0])]
        planes = [rows, [above_lanes(row) for row in rows]]
        at = {}
        for az in range(2):
            for ay in range(2):
                chosen = jnp.where(upper, planes[az][ay + 1], planes[az][ay])
                for ax in range(2):
                    at[az, ay, ax] = jnp.sum(
                        jnp.where(hits[ax], chosen, 0.0), axis=0, keepdims=True
                    )
        sx, sy, sz = shape
        slope = [0.0, 0.0, 0.0]
        for first in range(2):
            for second in range(2):
                slope[0] = slope[0] + sz[first] * sy[second] * (
                    at[first, second, 1] - at[first, second, 0]
                )
                slope[1] = slope[1] + sz[first] * sx[second] * (
                    at[first, 1, second] - at[first, 0, second]
                )
                slope[2] = slope[2] + sy[first] * sx[second] * (
                    at[1, first, second] - at[0, first, second]
                )
        slopes.append(slope)
    return [
        slopes[0][0],
        slopes[1][1],
        slopes[2][2],
        slopes[1][2] + slopes[2][1],
        slopes[0][2] + slopes[2][0],
        slopes[0][1] + slopes[1][0],
    ]


def tile_at(ref, base, row):
    return ref[pl.ds(base + row * 8, 8), :]


def solve_kernel(
    recv_ref,
    phase_ref,
    moduli_ref,
    slot_ref,
    load_ref,
    ret_ref,
    new_ref,
    w_ref,
    p_ref,
    q_ref,
    sig_ref,
    lam_ref,
    mu_ref,
    mu2_ref,
    scratch,
):
    zero = jnp.zeros((8, LANES), jnp.float32)
    phase = jnp.take_along_axis(phase_ref[...], device_at(lane_iota(VOX)), axis=1)
    mu = jnp.where(
        phase == 0, moduli_ref[1:2, 0:1], jnp.where(phase == 1, moduli_ref[1:2, 1:2], moduli_ref[1:2, 2:3])
    )
    lam_ref[...] = jnp.where(
        phase == 0, moduli_ref[0:1, 0:1], jnp.where(phase == 1, moduli_ref[0:1, 1:2], moduli_ref[0:1, 2:3])
    )
    mu_ref[...] = mu
    mu2_ref[...] = mu + mu
    w_ref[pl.ds(7, ROWS, stride=8), :] = jnp.zeros((ROWS, LANES), jnp.float32)
    tail = None
    same = (sublane_iota(DEV) == lane_iota(DEV)).astype(jnp.float32).astype(jnp.bfloat16)
    for k in range(CHUNKS):
        block = recv_ref[pl.ds(k, DEV, stride=CHUNKS), :]
        turned = flip(same, block) if k % 3 == 1 else block.T
        start, stop = k * LANES, min((k + 1) * LANES, CASES * ROWS)
        while start < stop:
            case = start // ROWS
            end = min(stop, (case + 1) * ROWS)
            w_ref[pl.ds((start - case * ROWS) * 8 + case, end - start, stride=8), :] = turned[
                start - k * LANES : end - k * LANES
            ]
            start = end
        tail = turned
    macro = macro_strain_rows(tail)
    sub = sublane_iota()
    imposed = [
        jnp.where(sub == 0, macro[m], jnp.where(sub == m + 1, 1.0, 0.0)) for m in range(6)
    ]

    def stress_pass(src, strain, keep, energy):
        def plane(a, carry):
            sums, work = list(carry[0]), carry[1]
            base = pl.multiple_of(a * 288, 8)
            ahead = pl.multiple_of(jnp.where(a == R - 1, 0, (a + 1) * 288), 8)
            voxel = a * 36
            line = [[tile_at(src, base, i * VOX + c) for c in range(R)] for i in range(3)]
            for b in range(R):
                nb = (b + 1) % R
                below = [
                    [tile_at(src, base, i * VOX + nb * R + c) for c in range(R)] for i in range(3)
                ]
                for c in range(R):
                    at = b * R + c
                    here = [line[i][c] for i in range(3)]
                    grad = [
                        [
                            tile_at(src, ahead, i * VOX + at) - here[i],
                            below[i][c] - here[i],
                            line[i][(c + 1) % R] - here[i],
                        ]
                        for i in range(3)
                    ]
                    eps = [
                        grad[0][0],
                        grad[1][1],
                        grad[2][2],
                        grad[1][2] + grad[2][1],
                        grad[0][2] + grad[2][0],
                        grad[0][1] + grad[1][0],
                    ]
                    if strain is not None:
                        eps = [eps[m] + strain[m] for m in range(6)]
                    lam = lam_ref[pl.ds(voxel + at, 8, stride=0), :]
                    mu1 = mu_ref[pl.ds(voxel + at, 8, stride=0), :]
                    mu2 = mu2_ref[pl.ds(voxel + at, 8, stride=0), :]
                    bulk = lam * (eps[0] + eps[1] + eps[2])
                    sig = [bulk + mu2 * eps[m] for m in range(3)]
                    sig += [mu1 * eps[m] for m in range(3, 6)]
                    for m in range(6):
                        sums[m] = sums[m] + sig[m]
                        if keep:
                            sig_ref[pl.ds(base + (m * VOX + at) * 8, 8), :] = sig[m]
                    if energy:
                        work = work + (
                            (sig[0] * eps[0] + sig[1] * eps[1])
                            + (sig[2] * eps[2] + sig[3] * eps[3])
                            + (sig[4] * eps[4] + sig[5] * eps[5])
                        )
                line = below
            return tuple(sums), work

        return lax.fori_loop(0, R, plane, ((zero,) * 6, zero), unroll=2)

    def force_pass(src, finish, dst):
        def plane(a, carry):
            totals = list(carry)
            base = pl.multiple_of(a * 288, 8)
            behind = pl.multiple_of(jnp.where(a == 0, (R - 1) * 288, (a - 1) * 288), 8)
            for b in range(R):
                pb = (b + R - 1) % R
                last = [tile_at(sig_ref, base, PAIRS[2][i] * VOX + b * R + R - 1) for i in range(3)]
                for c in range(R):
                    at = b * R + c
                    own = [tile_at(sig_ref, base, m * VOX + at) for m in range(6)]
                    for i in range(3):
                        gone = (own[PAIRS[0][i]] + own[PAIRS[1][i]]) + own[PAIRS[2][i]]
                        come = (
                            tile_at(sig_ref, behind, PAIRS[0][i] * VOX + at)
                            + tile_at(sig_ref, base, PAIRS[1][i] * VOX + pb * R + c)
                        ) + last[i]
                        value = finish(come, gone, tile_at(src, base, i * VOX + at))
                        dst[pl.ds(base + (i * VOX + at) * 8, 8), :] = value
                        totals[i] = totals[i] + value * value
                    last = [own[PAIRS[2][i]] for i in range(3)]
            return tuple(totals)

        totals = lax.fori_loop(0, R, plane, (zero,) * 3, unroll=2)
        return (totals[0] + totals[1]) + totals[2]

    mean0, _ = stress_pass(w_ref, imposed, True, False)
    square0 = force_pass(w_ref, lambda come, gone, w: (gone - come) - STAB * w, p_ref)
    mean1, work1 = stress_pass(p_ref, None, True, True)
    step0 = square0 / (work1 + STAB * square0)
    kept = 1.0 - STAB * step0
    square1 = force_pass(p_ref, lambda come, gone, p: kept * p - step0 * (come - gone), q_ref)
    ratio = square1 / square0

    def direction(a, carry):
        base = pl.multiple_of(a * 288, 8)
        for at in range(36):
            for i in range(3):
                q_ref[pl.ds(base + (i * VOX + at) * 8, 8), :] = tile_at(
                    q_ref, base, i * VOX + at
                ) + ratio * tile_at(p_ref, base, i * VOX + at)
        return carry

    lax.fori_loop(0, R, direction, 0)
    length = square1 + ratio * square1
    mean2, work2 = stress_pass(q_ref, None, False, True)
    step1 = square1 / (work2 + STAB * length)
    place = place_of(lane_iota(8))

    def update(a, carry):
        base = pl.multiple_of(a * 288, 8)
        for i in range(3):
            for at in range(36):
                value = (
                    tile_at(w_ref, base, i * VOX + at)
                    + step0 * tile_at(p_ref, base, i * VOX + at)
                    + step1 * tile_at(q_ref, base, i * VOX + at)
                )
                new_ref[pl.ds(a * 36 + i * VOX + at, 8, stride=PITCH), :] = jnp.take_along_axis(
                    value, place, axis=1
                )
        return carry

    lax.fori_loop(0, R, update, 0)
    mean = [(mean0[m] + step0 * mean1[m] + step1 * mean2[m]) * (1.0 / VOX) for m in range(6)]

    shared = place_of(slot_ref[...] >> 7).astype(jnp.float32)
    shared = jnp.broadcast_to(shared, (8, LANES))
    for m in range(6):
        shared = jnp.where(sub == m, mean[m][0:1], shared)
    terms = [mean[m][m + 1 : m + 2] for m in range(6)]
    for first, second in OFF_DIAGONAL:
        terms.append(mean[first][second + 1 : second + 2] + mean[second][first + 1 : first + 2])
    own = jnp.concatenate(terms + [jnp.zeros((1, LANES), jnp.float32)], axis=0)
    left = previous_row_lanes(own)
    stacked = jnp.concatenate(
        [jnp.zeros((64, LANES), jnp.float32), own, left, below_lanes(own), below_lanes(left)],
        axis=0,
    )
    special = stacked.T + node_row(load_ref, scratch, 0)
    for peer in range(DEV):
        ret_ref[8 * peer : 8 * peer + 8, :] = shared
    ret_ref[pl.ds(7, DEV, stride=8), :] = special


def row_of(value, index):
    return jnp.sum(jnp.where(sublane_iota(DEV) == index, value, 0), axis=0, keepdims=True)


def node_tile(row):
    sub = sublane_iota()
    wide = jnp.broadcast_to(row, (8, LANES))
    tile = wide
    for r in range(1, 6):
        tile = jnp.where(sub == r, pltpu.roll(wide, LANES - 8 * r, 1), tile)
    return tile


def final_kernel(
    recv_ref,
    me_ref,
    disp_ref,
    force_ref,
    weight_ref,
    place_ref,
    state_ref,
    new_disp_ref,
    res_ref,
    norm_ref,
    state_out,
    scratch,
    sems,
):
    saves = [
        pltpu.make_async_copy(
            state_ref.at[pl.ds(case * PITCH, ROWS)], state_out.at[case], sems.at[case]
        )
        for case in range(CASES)
    ]
    for save in saves:
        save.start()
    me = me_ref[...]
    order = recv_ref[pl.ds(6, DEV, stride=8), :].astype(jnp.int32)
    special = recv_ref[pl.ds(7, DEV, stride=8), :]
    stress = [
        jnp.take_along_axis(recv_ref[pl.ds(m, DEV, stride=8), :].T, order, axis=1)
        for m in range(6)
    ]
    forces = lax.dot_general(
        jnp.concatenate(stress, axis=1),
        force_ref[...],
        (((1,), (0,)), ((), ())),
        precision=HIGHEST,
        preferred_element_type=jnp.float32,
    )
    home = sublane_iota(DEV)
    upper = forces[:, LANES:]
    lifted = jnp.where(home < 64, pltpu.roll(upper, 68, 0), pltpu.roll(upper, 64, 0))
    lifted = jnp.where(home < 4, 0.0, lifted)
    near = forces[:, :LANES] + lifted
    beside = jnp.where(home % 4 == 0, pltpu.roll(near, DEV - 3, 0), pltpu.roll(near, 1, 0))
    force = near + pltpu.roll(beside, LANES - NODES, 1)
    node = lane_iota(DEV) < NODES
    loads = jnp.where(node, special, 0.0)
    residual = jnp.where(node, special - force, 0.0)
    top = jnp.sum(jnp.sum(residual * residual, axis=0, keepdims=True), axis=1, keepdims=True)
    bottom = jnp.sum(jnp.sum(loads * loads, axis=0, keepdims=True), axis=1, keepdims=True)
    norm_ref[...] = jnp.sqrt(top / bottom)

    own_residual = row_of(residual, me)
    left = jnp.where(me % 4 == 0, me + 3, me - 1)
    under = jnp.where(me >= 64, 64, jnp.where(me < 4, 0, -60))
    turned = special.T
    diagonal = jnp.zeros((24, LANES), jnp.float32)
    for k, source in enumerate((me, left, me - under, left - under)):
        picks = jnp.broadcast_to(row_of(order, source), (16, LANES))
        terms = jnp.take_along_axis(turned[64 + 16 * k : 80 + 16 * k], picks, axis=1)
        corner = []
        for i in range(3):
            total = jnp.zeros((8, LANES), jnp.float32)
            for n, (_, _, t) in enumerate(diagonal_terms(i)):
                at = (i * 6 + n) * 8
                total = total + weight_ref[at : at + 8, :] * terms[t : t + 1]
            corner.append(total)
        diagonal = diagonal + lax.dot_general(
            jnp.concatenate(corner, axis=0),
            place_ref[k],
            (((1,), (0,)), ((), ())),
            precision=HIGHEST,
            preferred_element_type=jnp.float32,
        )
    lane = lane_iota(8)
    same = lane // 16 == sublane_iota()
    row = jnp.zeros((1, LANES), jnp.float32)
    for i in range(3):
        part = jnp.sum(jnp.where(same, diagonal[8 * i : 8 * i + 8], 0.0), axis=0, keepdims=True)
        for shift in (64, 32, 16):
            part = part + pltpu.roll(part, shift, 1)
        row = jnp.where(lane_iota() // 16 == i, part, row)
    moved = node_row(disp_ref, scratch, 0) + own_residual / jnp.maximum(row, FLOOR)
    for value, ref in ((moved, new_disp_ref), (own_residual, res_ref)):
        tile = node_tile(value)
        for i in range(3):
            ref[i, 0] = tile[2 * i : 2 * i + 2, 0:8]
    for save in saves:
        save.wait()


def in_hbm(value):
    return pltpu.with_memory_space_constraint(value, pltpu.HBM)


def exchange(value):
    return lax.all_to_all(value, AXES, split_axis=0, concat_axis=0, tiled=True)


def run_pack(micro_state, state_slot, home_slot, displacement):
    return pl.pallas_call(
        pack_kernel,
        out_shape=jax.ShapeDtypeStruct((DEV * CHUNKS, LANES), jnp.float32),
        in_specs=[HBM] * 4,
        out_specs=VMEM,
        scratch_shapes=[
            pltpu.VMEM((WIDE, LANES), jnp.float32),
            pltpu.VMEM((1, LANES), jnp.int32),
            pltpu.VMEM((1, LANES), jnp.int32),
            pltpu.VMEM(displacement.shape, jnp.float32),
            pltpu.VMEM((8, LANES), jnp.float32),
            pltpu.SemaphoreType.DMA((PARTS + 3,)),
        ],
        compiler_params=pltpu.CompilerParams(vmem_limit_bytes=12 << 20),
        name="pack",
    )(
        in_hbm(micro_state.reshape(CASES * ROWS, LANES)),
        in_hbm(state_slot.reshape(1, LANES)),
        in_hbm(home_slot.reshape(1, LANES)),
        in_hbm(displacement),
    )


def run_solve(received, phases, phase_moduli, home_slot, load):
    f32 = jnp.float32
    return pl.pallas_call(
        solve_kernel,
        out_shape=(
            jax.ShapeDtypeStruct((DEV * 8, LANES), f32),
            jax.ShapeDtypeStruct((8 * PITCH, LANES), f32),
        ),
        in_specs=[VMEM, VMEM, VMEM, VMEM, VMEM],
        out_specs=[VMEM] * 2,
        scratch_shapes=[
            pltpu.VMEM((ROWS * 8, LANES), f32),
            pltpu.VMEM((ROWS * 8, LANES), f32),
            pltpu.VMEM((ROWS * 8, LANES), f32),
            pltpu.VMEM((6 * VOX * 8, LANES), f32),
            pltpu.VMEM((VOX, LANES), f32),
            pltpu.VMEM((VOX, LANES), f32),
            pltpu.VMEM((VOX, LANES), f32),
            pltpu.VMEM((8, LANES), f32),
        ],
        compiler_params=pltpu.CompilerParams(vmem_limit_bytes=32 << 20),
        name="solve",
    )(received, phases, phase_moduli, home_slot.reshape(1, LANES), load)


def run_final(returned, me, displacement, state):
    force_table, weight_table, place_table = assembly_tables()
    node_shape = jax.ShapeDtypeStruct(displacement.shape, jnp.float32)
    return pl.pallas_call(
        final_kernel,
        out_shape=(
            node_shape,
            node_shape,
            jax.ShapeDtypeStruct((1, 1), jnp.float32),
            pltpu.HBM((CASES, ROWS, LANES), jnp.float32),
        ),
        in_specs=[VMEM] * 7,
        out_specs=[VMEM] * 3 + [HBM],
        scratch_shapes=[
            pltpu.VMEM((8, LANES), jnp.float32),
            pltpu.SemaphoreType.DMA((CASES,)),
        ],
        compiler_params=pltpu.CompilerParams(vmem_limit_bytes=12 << 20),
        name="final",
    )(
        returned,
        me,
        displacement,
        jnp.asarray(force_table),
        jnp.asarray(weight_table),
        jnp.asarray(place_table),
        state,
    )


def per_device(displacement, load, home_slot, micro_state, state_slot, phases, phase_moduli):
    sent = run_pack(micro_state, state_slot, home_slot, displacement)
    me = jnp.full((1, LANES), lax.axis_index(AXES), jnp.int32)
    sent, me = lax.optimization_barrier((sent, me))
    received = exchange(sent.reshape(DEV, 1, WIDE)).reshape(DEV * CHUNKS, LANES)
    answer, state = run_solve(received, phases, phase_moduli, home_slot, load)
    returned = exchange(answer.reshape(DEV, 8, LANES)).reshape(DEV * 8, LANES)
    displaced, residual, rel_norm, new_state = run_final(returned, me, displacement, state)
    return (
        new_state.reshape(micro_state.shape),
        displaced,
        residual,
        rel_norm.reshape(()),
    )


def solution(mesh):
    split = Mesh(mesh.devices.reshape(-1, 2, mesh.shape["rve"]), SPLIT)
    return jax.shard_map(
        per_device,
        mesh=split,
        in_specs=(
            P(None, SUB, "rve", None),
            P(None, SUB, "rve", None),
            P(SPLIT),
            P(None, None, None, SPLIT),
            P(SPLIT),
            P(None, SPLIT),
            P(),
        ),
        out_specs=(
            P(None, None, None, SPLIT),
            P(None, SUB, "rve", None),
            P(None, SUB, "rve", None),
            P(),
        ),
        check_vma=False,
    )
```

```python
import math

import jax
import jax.numpy as jnp
import numpy as np
from jax import lax
from jax.experimental import pallas as pl
from jax.experimental.pallas import tpu as pltpu
from jax.sharding import Mesh
from jax.sharding import PartitionSpec as P

R = 6
VOX = R * R * R
ROWS = 3 * VOX
CASES = 7
DEV = 128
LANES = 128
CHUNKS = 36
WIDE = CHUNKS * LANES
TAIL = CASES * ROWS - (CHUNKS - 1) * LANES
NODES = 48
STAB = 0.1
FLOOR = 1.0
SPLIT = ("far", "core", "rve")
AXES = ("core", "far", "rve")
SUB = ("far", "core")
PAIRS = ((0, 5, 4), (5, 1, 3), (4, 3, 2))
STRAIN_OF = ((0, 4, 5), (5, 1, 3), (4, 3, 2))
OFF_DIAGONAL = ((0, 4), (0, 5), (4, 5), (1, 3), (1, 5), (3, 5), (2, 3), (2, 4), (3, 4))
LOW = 0.5 - 0.5 / math.sqrt(3.0)
HIGH = 0.5 + 0.5 / math.sqrt(3.0)
HIGHEST = lax.Precision.HIGHEST
VMEM = pl.BlockSpec(memory_space=pltpu.VMEM)
SMEM = pl.BlockSpec(memory_space=pltpu.SMEM)
HBM = pl.BlockSpec(memory_space=pltpu.HBM)
CUTS = (0, 6, 36)
PARTS = len(CUTS) - 1
STEP = 6
UPDATE = 72


def strain_table():
    places = (LOW, HIGH)
    table = np.zeros((8, 8, 3, 6))
    for gauss in range(8):
        at = (places[gauss % 2], places[gauss // 2 % 2], places[gauss // 4])
        for corner in range(8):
            bits = (corner % 2, corner // 2 % 2, corner // 4)
            weight = [at[k] if bits[k] else 1.0 - at[k] for k in range(3)]
            sign = [1.0 if bits[k] else -1.0 for k in range(3)]
            dx = sign[0] * weight[1] * weight[2]
            dy = weight[0] * sign[1] * weight[2]
            dz = weight[0] * weight[1] * sign[2]
            table[gauss, corner, 0, [0, 4, 5]] = (dx, dz, dy)
            table[gauss, corner, 1, [1, 3, 5]] = (dy, dz, dx)
            table[gauss, corner, 2, [2, 3, 4]] = (dz, dy, dx)
    return table


def term_index(first, second):
    if first == second:
        return first
    return 6 + OFF_DIAGONAL.index((min(first, second), max(first, second)))


def diagonal_terms(component):
    m = STRAIN_OF[component]
    pairs = [(m[0], m[0]), (m[1], m[1]), (m[2], m[2]), (m[0], m[1]), (m[0], m[2]), (m[1], m[2])]
    return [(a, b, term_index(a, b)) for a, b in pairs]


def assembly_tables():
    table = strain_table()
    force = np.zeros((6, LANES, 2 * LANES), np.float32)
    weights = np.zeros((3, 6, 8, LANES), np.float32)
    place = np.zeros((4, LANES, LANES), np.float32)
    for j in range(LANES):
        ly, ex, gauss = j // 64, j // 8 % 8, j % 8
        for corner in range(8):
            az, row, col = corner // 4, ly + corner // 2 % 2, (ex + corner % 2) % 8
            for i in range(3):
                lane = az * LANES + (NODES if row == 2 else 0) + i * 16 + row % 2 * 8 + col
                for m in STRAIN_OF[i]:
                    force[m, j, lane] += 0.125 * table[gauss, corner, i, m]
                for n, (first, second, _) in enumerate(diagonal_terms(i)):
                    weights[i, n, corner, j] = (
                        0.125 * table[gauss, corner, i, first] * table[gauss, corner, i, second]
                    )
            place[az * 2 + (1 if row == 2 else 0), j, corner * 16 + row % 2 * 8 + col] = 1.0
    return force.reshape(6 * LANES, 2 * LANES), weights.reshape(18 * 8, LANES), place


def split_table(table):
    high = table.astype(jnp.bfloat16)
    rest = table - high.astype(np.float32)
    middle = rest.astype(jnp.bfloat16)
    return high, middle, (rest - middle.astype(np.float32)).astype(jnp.bfloat16)


def lane_iota(rows=1):
    return lax.broadcasted_iota(jnp.int32, (rows, LANES), 1)


def sublane_iota(rows=8):
    return lax.broadcasted_iota(jnp.int32, (rows, LANES), 0)


def node_row(ref, scratch, offset):
    scratch[...] = jnp.zeros((8, LANES), jnp.float32)
    for i in range(3):
        scratch[2 * i : 2 * i + 2, 0:8] = ref[i, 0]
    tile = scratch[...]
    total = jnp.zeros((1, LANES), jnp.float32)
    for row in range(6):
        total = total + pltpu.roll(tile[row : row + 1], offset + 8 * row, 1)
    return total


def previous_row_lanes(value):
    lane = lane_iota(value.shape[0])
    return jnp.where(lane % 4 == 0, pltpu.roll(value, LANES - 3, 1), pltpu.roll(value, 1, 1))


def next_row_lanes(value):
    lane = lane_iota(value.shape[0])
    return jnp.where(lane % 4 == 3, pltpu.roll(value, 3, 1), pltpu.roll(value, LANES - 1, 1))


def below_lanes(value):
    lane = lane_iota(value.shape[0])
    moved = jnp.where(lane < 64, pltpu.roll(value, 68, 1), pltpu.roll(value, 64, 1))
    return jnp.where(lane < 4, 0.0, moved)


def above_lanes(value):
    lane = lane_iota(value.shape[0])
    moved = jnp.where(lane < 64, pltpu.roll(value, 64, 1), pltpu.roll(value, 60, 1))
    return jnp.where(lane >= 124, 0.0, moved)


def device_at(place):
    return ((place >> 2) & 15) * 8 + (place >> 6) * 4 + (place & 3)


def place_of(device):
    return ((device >> 2) & 1) * 64 + (device >> 3) * 4 + (device & 3)


def part_copy(src, dst, sems, part):
    start, stop = CUTS[part] * LANES, min(CUTS[part + 1] * LANES, CASES * ROWS)
    rows = pl.ds(start, stop - start)
    return pltpu.make_async_copy(src.at[rows], dst.at[rows], sems.at[part])


def split_bf16(value):
    high = value.astype(jnp.bfloat16)
    rest = value - high.astype(jnp.float32)
    middle = rest.astype(jnp.bfloat16)
    low = (rest - middle.astype(jnp.float32)).astype(jnp.bfloat16)
    return high, middle, low


def flip(same, block):
    high, middle, low = (
        lax.dot_general(
            same, part, (((1,), (1,)), ((), ())), preferred_element_type=jnp.float32
        )
        for part in split_bf16(block)
    )
    return (high + middle) + low


def pack_kernel(
    state_ref,
    state_slot_hbm,
    home_slot_hbm,
    disp_hbm,
    out_ref,
    held_ref,
    state_slot_ref,
    home_slot_ref,
    disp_ref,
    scratch,
    sems,
):
    small = [
        pltpu.make_async_copy(src, dst, sems.at[PARTS + k])
        for k, (src, dst) in enumerate(
            (
                (state_slot_hbm, state_slot_ref),
                (home_slot_hbm, home_slot_ref),
                (disp_hbm, disp_ref),
            )
        )
    ]
    for copy in small:
        copy.start()
    for part in range(PARTS):
        part_copy(state_ref, held_ref, sems, part).start()
    owner = device_at(sublane_iota(DEV))
    lane = lane_iota(DEV)
    for copy in small:
        copy.wait()
    choose = ((state_slot_ref[...] >> 7) == owner).astype(jnp.float32).astype(jnp.bfloat16)
    twice = jnp.concatenate([choose, choose], axis=1)
    home = (home_slot_ref[...] >> 7) == owner
    local = jnp.sum(jnp.where(home, lane, 0).astype(jnp.float32), axis=1, keepdims=True)
    extra = node_row(disp_ref, scratch, TAIL) + jnp.where(lane == TAIL + NODES, local, 0.0)
    held_ref[CASES * ROWS :, :] = jnp.zeros((WIDE - CASES * ROWS, LANES), jnp.float32)
    for part in range(PARTS):
        part_copy(state_ref, held_ref, sems, part).wait()
        for first in range(CUTS[part], CUTS[part + 1], STEP):
            high, middle, low = split_bf16(held_ref[first * LANES : (first + STEP) * LANES, :])
            picked = lax.dot_general(
                jnp.concatenate([high, middle], axis=1),
                twice,
                (((1,), (1,)), ((), ())),
                preferred_element_type=jnp.float32,
            )
            picked = picked + lax.dot_general(
                low, choose, (((1,), (1,)), ((), ())), preferred_element_type=jnp.float32
            )
            for k in range(first, first + STEP):
                turned = picked[(k - first) * LANES : (k - first + 1) * LANES].T
                if k == CHUNKS - 1:
                    turned = turned + extra
                out_ref[pl.ds(k, DEV, stride=CHUNKS), :] = turned


def macro_strain_rows(tail):
    local = tail[TAIL + NODES : TAIL + NODES + 1].astype(jnp.int32)
    upper = (local >> 6) == 1
    ex = (local >> 3) & 7
    point = [jnp.where(((local >> k) & 1) == 1, HIGH, LOW) for k in range(3)]
    shape = [(1.0 - point[k], point[k]) for k in range(3)]
    sub = sublane_iota()
    hits = (sub == ex, sub == ((ex + 1) & 7))
    slopes = []
    for i in range(3):
        own = [tail[TAIL + 16 * i + 8 * y : TAIL + 16 * i + 8 * y + 8] for y in range(2)]
        rows = [own[0], own[1], next_row_lanes(own[0])]
        planes = [rows, [above_lanes(row) for row in rows]]
        at = {}
        for az in range(2):
            for ay in range(2):
                chosen = jnp.where(upper, planes[az][ay + 1], planes[az][ay])
                for ax in range(2):
                    at[az, ay, ax] = jnp.sum(
                        jnp.where(hits[ax], chosen, 0.0), axis=0, keepdims=True
                    )
        sx, sy, sz = shape
        slope = [0.0, 0.0, 0.0]
        for first in range(2):
            for second in range(2):
                slope[0] = slope[0] + sz[first] * sy[second] * (
                    at[first, second, 1] - at[first, second, 0]
                )
                slope[1] = slope[1] + sz[first] * sx[second] * (
                    at[first, 1, second] - at[first, 0, second]
                )
                slope[2] = slope[2] + sy[first] * sx[second] * (
                    at[1, first, second] - at[0, first, second]
                )
        slopes.append(slope)
    return [
        slopes[0][0],
        slopes[1][1],
        slopes[2][2],
        slopes[1][2] + slopes[2][1],
        slopes[0][2] + slopes[2][0],
        slopes[0][1] + slopes[1][0],
    ]


def tile_at(ref, base, row):
    return ref[pl.ds(base + row * 8, 8), :]


def solve_kernel(
    recv_ref,
    phase_ref,
    moduli_ref,
    slot_ref,
    load_ref,
    ret_ref,
    w_out,
    p_out,
    q_out,
    step_ref,
    w_ref,
    p_ref,
    q_ref,
    sig_ref,
    lam_ref,
    mu_ref,
    mu2_ref,
    scratch,
    sems,
):
    saves = [
        pltpu.make_async_copy(src, dst, sems.at[k])
        for k, (src, dst) in enumerate(((w_ref, w_out), (p_ref, p_out), (q_ref, q_out)))
    ]

    def save_plane(base):
        for i in range(3):
            rows = pl.ds(base + i * VOX * 8, 288)
            pltpu.make_async_copy(q_ref.at[rows], q_out.at[rows], sems.at[2]).start()

    zero = jnp.zeros((8, LANES), jnp.float32)
    phase = jnp.take_along_axis(phase_ref[...], device_at(lane_iota(VOX)), axis=1)
    mu = jnp.where(
        phase == 0, moduli_ref[1:2, 0:1], jnp.where(phase == 1, moduli_ref[1:2, 1:2], moduli_ref[1:2, 2:3])
    )
    lam_ref[...] = jnp.where(
        phase == 0, moduli_ref[0:1, 0:1], jnp.where(phase == 1, moduli_ref[0:1, 1:2], moduli_ref[0:1, 2:3])
    )
    mu_ref[...] = mu
    mu2_ref[...] = mu + mu
    same = (sublane_iota(DEV) == lane_iota(DEV)).astype(jnp.float32).astype(jnp.bfloat16)

    def unpack(k):
        block = recv_ref[pl.ds(k, DEV, stride=CHUNKS), :]
        turned = flip(same, block) if k % 4 == 1 else block.T
        start, stop = k * LANES, min((k + 1) * LANES, CASES * ROWS)
        while start < stop:
            case = start // ROWS
            end = min(stop, (case + 1) * ROWS)
            w_ref[pl.ds((start - case * ROWS) * 8 + case, end - start, stride=8), :] = turned[
                start - k * LANES : end - k * LANES
            ]
            start = end
        return turned

    macro = macro_strain_rows(unpack(CHUNKS - 1))
    for k in range(CHUNKS - 1):
        unpack(k)
    saves[0].start()
    sub = sublane_iota()
    imposed = [
        jnp.where(sub == 0, macro[m], jnp.where(sub == m + 1, 1.0, 0.0)) for m in range(6)
    ]

    def stress_pass(src, strain, keep, energy):
        def plane(a, carry):
            sums, work = list(carry[0]), carry[1]
            base = pl.multiple_of(a * 288, 8)
            ahead = pl.multiple_of(jnp.where(a == R - 1, 0, (a + 1) * 288), 8)
            voxel = a * 36
            line = [[tile_at(src, base, i * VOX + c) for c in range(R)] for i in range(3)]
            for b in range(R):
                nb = (b + 1) % R
                below = [
                    [tile_at(src, base, i * VOX + nb * R + c) for c in range(R)] for i in range(3)
                ]
                for c in range(R):
                    at = b * R + c
                    here = [line[i][c] for i in range(3)]
                    grad = [
                        [
                            tile_at(src, ahead, i * VOX + at) - here[i],
                            below[i][c] - here[i],
                            line[i][(c + 1) % R] - here[i],
                        ]
                        for i in range(3)
                    ]
                    eps = [
                        grad[0][0],
                        grad[1][1],
                        grad[2][2],
                        grad[1][2] + grad[2][1],
                        grad[0][2] + grad[2][0],
                        grad[0][1] + grad[1][0],
                    ]
                    if strain is not None:
                        eps = [eps[m] + strain[m] for m in range(6)]
                    lam = lam_ref[pl.ds(voxel + at, 8, stride=0), :]
                    mu1 = mu_ref[pl.ds(voxel + at, 8, stride=0), :]
                    mu2 = mu2_ref[pl.ds(voxel + at, 8, stride=0), :]
                    bulk = lam * (eps[0] + eps[1] + eps[2])
                    sig = [bulk + mu2 * eps[m] for m in range(3)]
                    sig += [mu1 * eps[m] for m in range(3, 6)]
                    for m in range(6):
                        sums[m] = sums[m] + sig[m]
                        if keep:
                            sig_ref[pl.ds(base + (m * VOX + at) * 8, 8), :] = sig[m]
                    if energy:
                        work = work + (
                            (sig[0] * eps[0] + sig[1] * eps[1])
                            + (sig[2] * eps[2] + sig[3] * eps[3])
                            + (sig[4] * eps[4] + sig[5] * eps[5])
                        )
                line = below
            return tuple(sums), work

        return lax.fori_loop(0, R, plane, ((zero,) * 6, zero), unroll=2)

    def force_pass(src, finish, dst):
        def plane(a, carry):
            totals = list(carry)
            base = pl.multiple_of(a * 288, 8)
            behind = pl.multiple_of(jnp.where(a == 0, (R - 1) * 288, (a - 1) * 288), 8)
            for b in range(R):
                pb = (b + R - 1) % R
                last = [tile_at(sig_ref, base, PAIRS[2][i] * VOX + b * R + R - 1) for i in range(3)]
                for c in range(R):
                    at = b * R + c
                    own = [tile_at(sig_ref, base, m * VOX + at) for m in range(6)]
                    for i in range(3):
                        gone = (own[PAIRS[0][i]] + own[PAIRS[1][i]]) + own[PAIRS[2][i]]
                        come = (
                            tile_at(sig_ref, behind, PAIRS[0][i] * VOX + at)
                            + tile_at(sig_ref, base, PAIRS[1][i] * VOX + pb * R + c)
                        ) + last[i]
                        value = finish(come, gone, tile_at(src, base, i * VOX + at))
                        dst[pl.ds(base + (i * VOX + at) * 8, 8), :] = value
                        totals[i] = totals[i] + value * value
                    last = [own[PAIRS[2][i]] for i in range(3)]
            return tuple(totals)

        totals = lax.fori_loop(0, R, plane, (zero,) * 3, unroll=2)
        return (totals[0] + totals[1]) + totals[2]

    mean0, _ = stress_pass(w_ref, imposed, True, False)
    square0 = force_pass(w_ref, lambda come, gone, w: (gone - come) - STAB * w, p_ref)
    saves[1].start()
    mean1, work1 = stress_pass(p_ref, None, True, True)
    step0 = square0 / (work1 + STAB * square0)
    kept = 1.0 - STAB * step0
    square1 = force_pass(p_ref, lambda come, gone, p: kept * p - step0 * (come - gone), q_ref)
    ratio = square1 / square0

    def direction(a, carry):
        base = pl.multiple_of(a * 288, 8)
        for at in range(36):
            for i in range(3):
                q_ref[pl.ds(base + (i * VOX + at) * 8, 8), :] = tile_at(
                    q_ref, base, i * VOX + at
                ) + ratio * tile_at(p_ref, base, i * VOX + at)
        save_plane(base)
        return carry

    lax.fori_loop(0, R, direction, 0)
    length = square1 + ratio * square1
    mean2, work2 = stress_pass(q_ref, None, False, True)
    step1 = square1 / (work2 + STAB * length)
    step_ref[0:8, :] = step0
    step_ref[8:16, :] = step1
    mean = [(mean0[m] + step0 * mean1[m] + step1 * mean2[m]) * (1.0 / VOX) for m in range(6)]

    shared = place_of(slot_ref[...] >> 7).astype(jnp.float32)
    shared = jnp.broadcast_to(shared, (8, LANES))
    for m in range(6):
        shared = jnp.where(sub == m, mean[m][0:1], shared)
    terms = [mean[m][m + 1 : m + 2] for m in range(6)]
    for first, second in OFF_DIAGONAL:
        terms.append(mean[first][second + 1 : second + 2] + mean[second][first + 1 : first + 2])
    own = jnp.concatenate(terms + [jnp.zeros((1, LANES), jnp.float32)], axis=0)
    left = previous_row_lanes(own)
    stacked = jnp.concatenate(
        [jnp.zeros((64, LANES), jnp.float32), own, left, below_lanes(own), below_lanes(left)],
        axis=0,
    )
    special = stacked.T + node_row(load_ref, scratch, 0)
    for peer in range(DEV):
        ret_ref[8 * peer : 8 * peer + 8, :] = shared
    ret_ref[pl.ds(7, DEV, stride=8), :] = special
    for save in saves:
        save.wait()


def update_kernel(w_ref, p_ref, q_ref, step_ref, out_ref):
    place = place_of(lane_iota(UPDATE))
    for case in range(CASES):
        first = step_ref[case : case + 1, :]
        second = step_ref[8 + case : 9 + case, :]
        rows = pl.ds(case, UPDATE, stride=8)
        value = w_ref[rows, :] + first * p_ref[rows, :] + second * q_ref[rows, :]
        out_ref[case] = jnp.take_along_axis(value, place, axis=1)


def row_of(value, index):
    return jnp.sum(jnp.where(sublane_iota(DEV) == index, value, 0), axis=0, keepdims=True)


def node_tile(row):
    sub = sublane_iota()
    wide = jnp.broadcast_to(row, (8, LANES))
    tile = wide
    for r in range(1, 6):
        tile = jnp.where(sub == r, pltpu.roll(wide, LANES - 8 * r, 1), tile)
    return tile


def final_kernel(
    recv_ref,
    me_ref,
    disp_ref,
    force_ref,
    weight_ref,
    place_ref,
    new_disp_ref,
    res_ref,
    norm_ref,
    scratch,
):
    me = me_ref[...]
    order = recv_ref[pl.ds(6, DEV, stride=8), :].astype(jnp.int32)
    special = recv_ref[pl.ds(7, DEV, stride=8), :]
    stress = [
        jnp.take_along_axis(recv_ref[pl.ds(m, DEV, stride=8), :].T, order, axis=1)
        for m in range(6)
    ]
    parts = split_bf16(jnp.concatenate(stress, axis=1))
    forces = None
    for order_sum in (2, 1, 0):
        for first in range(order_sum + 1):
            product = lax.dot_general(
                parts[first],
                force_ref[order_sum - first],
                (((1,), (0,)), ((), ())),
                preferred_element_type=jnp.float32,
            )
            forces = product if forces is None else forces + product
    home = sublane_iota(DEV)
    upper = forces[:, LANES:]
    lifted = jnp.where(home < 64, pltpu.roll(upper, 68, 0), pltpu.roll(upper, 64, 0))
    lifted = jnp.where(home < 4, 0.0, lifted)
    near = forces[:, :LANES] + lifted
    beside = jnp.where(home % 4 == 0, pltpu.roll(near, DEV - 3, 0), pltpu.roll(near, 1, 0))
    force = near + pltpu.roll(beside, LANES - NODES, 1)
    node = lane_iota(DEV) < NODES
    loads = jnp.where(node, special, 0.0)
    residual = jnp.where(node, special - force, 0.0)
    top = jnp.sum(jnp.sum(residual * residual, axis=0, keepdims=True), axis=1, keepdims=True)
    bottom = jnp.sum(jnp.sum(loads * loads, axis=0, keepdims=True), axis=1, keepdims=True)
    norm_ref[...] = jnp.sqrt(top / bottom)

    own_residual = row_of(residual, me)
    left = jnp.where(me % 4 == 0, me + 3, me - 1)
    under = jnp.where(me >= 64, 64, jnp.where(me < 4, 0, -60))
    turned = special.T
    corners = []
    for k, source in enumerate((me, left, me - under, left - under)):
        picks = jnp.broadcast_to(row_of(order, source), (16, LANES))
        terms = jnp.take_along_axis(turned[64 + 16 * k : 80 + 16 * k], picks, axis=1)
        corner = []
        for i in range(3):
            total = jnp.zeros((8, LANES), jnp.float32)
            for n, (_, _, t) in enumerate(diagonal_terms(i)):
                at = (i * 6 + n) * 8
                total = total + weight_ref[at : at + 8, :] * terms[t : t + 1]
            corner.append(total)
        corners.append(jnp.concatenate(corner, axis=0))
    pieces = split_bf16(jnp.concatenate(corners, axis=1))
    diagonal = jnp.zeros((24, LANES), jnp.float32)
    for piece in pieces:
        diagonal = diagonal + lax.dot_general(
            piece, place_ref[...], (((1,), (0,)), ((), ())), preferred_element_type=jnp.float32
        )
    lane = lane_iota(8)
    same = lane // 16 == sublane_iota()
    row = jnp.zeros((1, LANES), jnp.float32)
    for i in range(3):
        part = jnp.sum(jnp.where(same, diagonal[8 * i : 8 * i + 8], 0.0), axis=0, keepdims=True)
        for shift in (64, 32, 16):
            part = part + pltpu.roll(part, shift, 1)
        row = jnp.where(lane_iota() // 16 == i, part, row)
    moved = node_row(disp_ref, scratch, 0) + own_residual / jnp.maximum(row, FLOOR)
    for value, ref in ((moved, new_disp_ref), (own_residual, res_ref)):
        tile = node_tile(value)
        for i in range(3):
            ref[i, 0] = tile[2 * i : 2 * i + 2, 0:8]


def in_hbm(value):
    return pltpu.with_memory_space_constraint(value, pltpu.HBM)


def exchange(value):
    return lax.all_to_all(value, AXES, split_axis=0, concat_axis=0, tiled=True)


def run_pack(micro_state, state_slot, home_slot, displacement):
    return pl.pallas_call(
        pack_kernel,
        out_shape=jax.ShapeDtypeStruct((DEV * CHUNKS, LANES), jnp.float32),
        in_specs=[HBM] * 4,
        out_specs=VMEM,
        scratch_shapes=[
            pltpu.VMEM((WIDE, LANES), jnp.float32),
            pltpu.VMEM((1, LANES), jnp.int32),
            pltpu.VMEM((1, LANES), jnp.int32),
            pltpu.VMEM(displacement.shape, jnp.float32),
            pltpu.VMEM((8, LANES), jnp.float32),
            pltpu.SemaphoreType.DMA((PARTS + 3,)),
        ],
        compiler_params=pltpu.CompilerParams(vmem_limit_bytes=12 << 20),
        name="pack",
    )(
        in_hbm(micro_state.reshape(CASES * ROWS, LANES)),
        in_hbm(state_slot.reshape(1, LANES)),
        in_hbm(home_slot.reshape(1, LANES)),
        in_hbm(displacement),
    )


def run_solve(received, phases, phase_moduli, home_slot, load):
    f32 = jnp.float32
    big = pltpu.HBM((ROWS * 8, LANES), f32)
    return pl.pallas_call(
        solve_kernel,
        out_shape=(
            jax.ShapeDtypeStruct((DEV * 8, LANES), f32),
            big,
            big,
            big,
            jax.ShapeDtypeStruct((16, LANES), f32),
        ),
        in_specs=[VMEM, VMEM, VMEM, VMEM, VMEM],
        out_specs=[VMEM, HBM, HBM, HBM, VMEM],
        scratch_shapes=[
            pltpu.VMEM((ROWS * 8, LANES), f32),
            pltpu.VMEM((ROWS * 8, LANES), f32),
            pltpu.VMEM((ROWS * 8, LANES), f32),
            pltpu.VMEM((6 * VOX * 8, LANES), f32),
            pltpu.VMEM((VOX, LANES), f32),
            pltpu.VMEM((VOX, LANES), f32),
            pltpu.VMEM((VOX, LANES), f32),
            pltpu.VMEM((8, LANES), f32),
            pltpu.SemaphoreType.DMA((3,)),
        ],
        compiler_params=pltpu.CompilerParams(vmem_limit_bytes=32 << 20),
        name="solve",
    )(received, phases, phase_moduli, home_slot.reshape(1, LANES), load)


def run_update(w, p, q, steps):
    return pl.pallas_call(
        update_kernel,
        out_shape=jax.ShapeDtypeStruct((CASES, ROWS, LANES), jnp.float32),
        grid=(ROWS // UPDATE,),
        in_specs=[pl.BlockSpec((UPDATE * 8, LANES), lambda k: (k, 0))] * 3
        + [pl.BlockSpec((16, LANES), lambda k: (0, 0))],
        out_specs=pl.BlockSpec((CASES, UPDATE, LANES), lambda k: (0, k, 0)),
        compiler_params=pltpu.CompilerParams(vmem_limit_bytes=8 << 20),
        cost_estimate=pl.CostEstimate(
            flops=20_000_000, bytes_accessed=10_000_000, transcendentals=0
        ),
        name="update",
    )(in_hbm(w), in_hbm(p), in_hbm(q), steps)


def run_final(returned, me, displacement):
    force_table, weight_table, place_table = assembly_tables()
    node_shape = jax.ShapeDtypeStruct(displacement.shape, jnp.float32)
    return pl.pallas_call(
        final_kernel,
        out_shape=(node_shape, node_shape, jax.ShapeDtypeStruct((1, 1), jnp.float32)),
        in_specs=[VMEM] * 6,
        out_specs=[VMEM] * 3,
        scratch_shapes=[pltpu.VMEM((8, LANES), jnp.float32)],
        compiler_params=pltpu.CompilerParams(vmem_limit_bytes=12 << 20),
        name="final",
    )(
        returned,
        me,
        displacement,
        jnp.asarray(np.stack(split_table(force_table))),
        jnp.asarray(weight_table),
        jnp.asarray(place_table.reshape(4 * LANES, LANES), jnp.bfloat16),
    )


def per_device(displacement, load, home_slot, micro_state, state_slot, phases, phase_moduli):
    sent = run_pack(micro_state, state_slot, home_slot, displacement)
    received = exchange(sent.reshape(DEV, 1, WIDE)).reshape(DEV * CHUNKS, LANES)
    answer, w, p, q, steps = run_solve(received, phases, phase_moduli, home_slot, load)
    returned = exchange(answer.reshape(DEV, 8, LANES)).reshape(DEV * 8, LANES)
    new_state = run_update(w, p, q, steps)
    me = jnp.full((1, LANES), lax.axis_index(AXES), jnp.int32)
    displaced, residual, rel_norm = run_final(returned, me, displacement)
    return (
        new_state.reshape(micro_state.shape),
        displaced,
        residual,
        rel_norm.reshape(()),
    )


def solution(mesh):
    split = Mesh(mesh.devices.reshape(-1, 2, mesh.shape["rve"]), SPLIT)
    return jax.shard_map(
        per_device,
        mesh=split,
        in_specs=(
            P(None, SUB, "rve", None),
            P(None, SUB, "rve", None),
            P(SPLIT),
            P(None, None, None, SPLIT),
            P(SPLIT),
            P(None, SPLIT),
            P(),
        ),
        out_specs=(
            P(None, None, None, SPLIT),
            P(None, SUB, "rve", None),
            P(None, SUB, "rve", None),
            P(),
        ),
        check_vma=False,
    )
```

```python
import math

import jax
import jax.numpy as jnp
import numpy as np
from jax import lax
from jax.experimental import pallas as pl
from jax.experimental.pallas import tpu as pltpu
from jax.sharding import Mesh
from jax.sharding import PartitionSpec as P

R = 6
VOX = R * R * R
ROWS = 3 * VOX
CASES = 7
DEV = 128
LANES = 128
CHUNKS = 36
WIDE = CHUNKS * LANES
TAIL = CASES * ROWS - (CHUNKS - 1) * LANES
NODES = 48
STAB = 0.1
FLOOR = 1.0
SPLIT = ("far", "core", "rve")
AXES = ("core", "far", "rve")
SUB = ("far", "core")
PAIRS = ((0, 5, 4), (5, 1, 3), (4, 3, 2))
STRAIN_OF = ((0, 4, 5), (5, 1, 3), (4, 3, 2))
OFF_DIAGONAL = ((0, 4), (0, 5), (4, 5), (1, 3), (1, 5), (3, 5), (2, 3), (2, 4), (3, 4))
LOW = 0.5 - 0.5 / math.sqrt(3.0)
HIGH = 0.5 + 0.5 / math.sqrt(3.0)
HIGHEST = lax.Precision.HIGHEST
VMEM = pl.BlockSpec(memory_space=pltpu.VMEM)
SMEM = pl.BlockSpec(memory_space=pltpu.SMEM)
HBM = pl.BlockSpec(memory_space=pltpu.HBM)
CUTS = (0, 4, 36)
PARTS = len(CUTS) - 1
STEP = 4
UPDATE = 72


def strain_table():
    places = (LOW, HIGH)
    table = np.zeros((8, 8, 3, 6))
    for gauss in range(8):
        at = (places[gauss % 2], places[gauss // 2 % 2], places[gauss // 4])
        for corner in range(8):
            bits = (corner % 2, corner // 2 % 2, corner // 4)
            weight = [at[k] if bits[k] else 1.0 - at[k] for k in range(3)]
            sign = [1.0 if bits[k] else -1.0 for k in range(3)]
            dx = sign[0] * weight[1] * weight[2]
            dy = weight[0] * sign[1] * weight[2]
            dz = weight[0] * weight[1] * sign[2]
            table[gauss, corner, 0, [0, 4, 5]] = (dx, dz, dy)
            table[gauss, corner, 1, [1, 3, 5]] = (dy, dz, dx)
            table[gauss, corner, 2, [2, 3, 4]] = (dz, dy, dx)
    return table


def term_index(first, second):
    if first == second:
        return first
    return 6 + OFF_DIAGONAL.index((min(first, second), max(first, second)))


def diagonal_terms(component):
    m = STRAIN_OF[component]
    pairs = [(m[0], m[0]), (m[1], m[1]), (m[2], m[2]), (m[0], m[1]), (m[0], m[2]), (m[1], m[2])]
    return [(a, b, term_index(a, b)) for a, b in pairs]


def assembly_tables():
    table = strain_table()
    force = np.zeros((6, LANES, 2 * LANES), np.float32)
    weights = np.zeros((3, 6, 8, LANES), np.float32)
    place = np.zeros((4, LANES, LANES), np.float32)
    for j in range(LANES):
        ly, ex, gauss = j // 64, j // 8 % 8, j % 8
        for corner in range(8):
            az, row, col = corner // 4, ly + corner // 2 % 2, (ex + corner % 2) % 8
            for i in range(3):
                lane = az * LANES + (NODES if row == 2 else 0) + i * 16 + row % 2 * 8 + col
                for m in STRAIN_OF[i]:
                    force[m, j, lane] += 0.125 * table[gauss, corner, i, m]
                for n, (first, second, _) in enumerate(diagonal_terms(i)):
                    weights[i, n, corner, j] = (
                        0.125 * table[gauss, corner, i, first] * table[gauss, corner, i, second]
                    )
            place[az * 2 + (1 if row == 2 else 0), j, corner * 16 + row % 2 * 8 + col] = 1.0
    return force.reshape(6 * LANES, 2 * LANES), weights.reshape(18 * 8, LANES), place


def split_table(table):
    high = table.astype(jnp.bfloat16)
    rest = table - high.astype(np.float32)
    middle = rest.astype(jnp.bfloat16)
    return high, middle, (rest - middle.astype(np.float32)).astype(jnp.bfloat16)


def lane_iota(rows=1):
    return lax.broadcasted_iota(jnp.int32, (rows, LANES), 1)


def sublane_iota(rows=8):
    return lax.broadcasted_iota(jnp.int32, (rows, LANES), 0)


def node_row(ref, scratch, offset):
    scratch[...] = jnp.zeros((8, LANES), jnp.float32)
    for i in range(3):
        scratch[2 * i : 2 * i + 2, 0:8] = ref[i, 0]
    tile = scratch[...]
    total = jnp.zeros((1, LANES), jnp.float32)
    for row in range(6):
        total = total + pltpu.roll(tile[row : row + 1], offset + 8 * row, 1)
    return total


def previous_row_lanes(value):
    lane = lane_iota(value.shape[0])
    return jnp.where(lane % 4 == 0, pltpu.roll(value, LANES - 3, 1), pltpu.roll(value, 1, 1))


def next_row_lanes(value):
    lane = lane_iota(value.shape[0])
    return jnp.where(lane % 4 == 3, pltpu.roll(value, 3, 1), pltpu.roll(value, LANES - 1, 1))


def below_lanes(value):
    lane = lane_iota(value.shape[0])
    moved = jnp.where(lane < 64, pltpu.roll(value, 68, 1), pltpu.roll(value, 64, 1))
    return jnp.where(lane < 4, 0.0, moved)


def above_lanes(value):
    lane = lane_iota(value.shape[0])
    moved = jnp.where(lane < 64, pltpu.roll(value, 64, 1), pltpu.roll(value, 60, 1))
    return jnp.where(lane >= 124, 0.0, moved)


def device_at(place):
    return ((place >> 2) & 15) * 8 + (place >> 6) * 4 + (place & 3)


def place_of(device):
    return ((device >> 2) & 1) * 64 + (device >> 3) * 4 + (device & 3)


def part_copy(src, dst, sems, part):
    start, stop = CUTS[part] * LANES, min(CUTS[part + 1] * LANES, CASES * ROWS)
    rows = pl.ds(start, stop - start)
    return pltpu.make_async_copy(src.at[rows], dst.at[rows], sems.at[part])


def split_bf16(value):
    high = value.astype(jnp.bfloat16)
    rest = value - high.astype(jnp.float32)
    middle = rest.astype(jnp.bfloat16)
    low = (rest - middle.astype(jnp.float32)).astype(jnp.bfloat16)
    return high, middle, low


def flip(same, block):
    high, middle, low = (
        lax.dot_general(
            same, part, (((1,), (1,)), ((), ())), preferred_element_type=jnp.float32
        )
        for part in split_bf16(block)
    )
    return (high + middle) + low


def pack_kernel(
    state_ref,
    state_slot_hbm,
    home_slot_hbm,
    disp_hbm,
    out_ref,
    held_ref,
    state_slot_ref,
    home_slot_ref,
    disp_ref,
    scratch,
    sems,
):
    small = [
        pltpu.make_async_copy(src, dst, sems.at[PARTS + k])
        for k, (src, dst) in enumerate(
            (
                (state_slot_hbm, state_slot_ref),
                (home_slot_hbm, home_slot_ref),
                (disp_hbm, disp_ref),
            )
        )
    ]
    for copy in small:
        copy.start()
    for part in range(PARTS):
        part_copy(state_ref, held_ref, sems, part).start()
    owner = device_at(sublane_iota(DEV))
    lane = lane_iota(DEV)
    for copy in small:
        copy.wait()
    choose = ((state_slot_ref[...] >> 7) == owner).astype(jnp.float32).astype(jnp.bfloat16)
    twice = jnp.concatenate([choose, choose], axis=1)
    home = (home_slot_ref[...] >> 7) == owner
    local = jnp.sum(jnp.where(home, lane, 0).astype(jnp.float32), axis=1, keepdims=True)
    extra = node_row(disp_ref, scratch, TAIL) + jnp.where(lane == TAIL + NODES, local, 0.0)
    held_ref[CASES * ROWS :, :] = jnp.zeros((WIDE - CASES * ROWS, LANES), jnp.float32)
    for part in range(PARTS):
        part_copy(state_ref, held_ref, sems, part).wait()
        for first in range(CUTS[part], CUTS[part + 1], STEP):
            high, middle, low = split_bf16(held_ref[first * LANES : (first + STEP) * LANES, :])
            picked = lax.dot_general(
                jnp.concatenate([high, middle], axis=1),
                twice,
                (((1,), (1,)), ((), ())),
                preferred_element_type=jnp.float32,
            )
            picked = picked + lax.dot_general(
                low, choose, (((1,), (1,)), ((), ())), preferred_element_type=jnp.float32
            )
            for k in range(first, first + STEP):
                turned = picked[(k - first) * LANES : (k - first + 1) * LANES].T
                if k == CHUNKS - 1:
                    turned = turned + extra
                out_ref[pl.ds(k, DEV, stride=CHUNKS), :] = turned


def macro_strain_rows(tail):
    local = tail[TAIL + NODES : TAIL + NODES + 1].astype(jnp.int32)
    upper = (local >> 6) == 1
    ex = (local >> 3) & 7
    point = [jnp.where(((local >> k) & 1) == 1, HIGH, LOW) for k in range(3)]
    shape = [(1.0 - point[k], point[k]) for k in range(3)]
    sub = sublane_iota()
    hits = (sub == ex, sub == ((ex + 1) & 7))
    slopes = []
    for i in range(3):
        own = [tail[TAIL + 16 * i + 8 * y : TAIL + 16 * i + 8 * y + 8] for y in range(2)]
        rows = [own[0], own[1], next_row_lanes(own[0])]
        planes = [rows, [above_lanes(row) for row in rows]]
        at = {}
        for az in range(2):
            for ay in range(2):
                chosen = jnp.where(upper, planes[az][ay + 1], planes[az][ay])
                for ax in range(2):
                    at[az, ay, ax] = jnp.sum(
                        jnp.where(hits[ax], chosen, 0.0), axis=0, keepdims=True
                    )
        sx, sy, sz = shape
        slope = [0.0, 0.0, 0.0]
        for first in range(2):
            for second in range(2):
                slope[0] = slope[0] + sz[first] * sy[second] * (
                    at[first, second, 1] - at[first, second, 0]
                )
                slope[1] = slope[1] + sz[first] * sx[second] * (
                    at[first, 1, second] - at[first, 0, second]
                )
                slope[2] = slope[2] + sy[first] * sx[second] * (
                    at[1, first, second] - at[0, first, second]
                )
        slopes.append(slope)
    return [
        slopes[0][0],
        slopes[1][1],
        slopes[2][2],
        slopes[1][2] + slopes[2][1],
        slopes[0][2] + slopes[2][0],
        slopes[0][1] + slopes[1][0],
    ]


def tile_at(ref, base, row):
    return ref[pl.ds(base + row * 8, 8), :]


def solve_kernel(
    recv_ref,
    phase_ref,
    moduli_ref,
    slot_ref,
    load_ref,
    ret_ref,
    w_out,
    p_out,
    q_out,
    step_ref,
    w_ref,
    p_ref,
    q_ref,
    sig_ref,
    lam_ref,
    mu_ref,
    mu2_ref,
    scratch,
    sems,
):
    saves = [
        pltpu.make_async_copy(src, dst, sems.at[k])
        for k, (src, dst) in enumerate(((w_ref, w_out), (p_ref, p_out), (q_ref, q_out)))
    ]

    def save_plane(base):
        for i in range(3):
            rows = pl.ds(base + i * VOX * 8, 288)
            pltpu.make_async_copy(q_ref.at[rows], q_out.at[rows], sems.at[2]).start()

    zero = jnp.zeros((8, LANES), jnp.float32)
    phase = jnp.take_along_axis(phase_ref[...], device_at(lane_iota(VOX)), axis=1)
    mu = jnp.where(
        phase == 0, moduli_ref[1:2, 0:1], jnp.where(phase == 1, moduli_ref[1:2, 1:2], moduli_ref[1:2, 2:3])
    )
    lam_ref[...] = jnp.where(
        phase == 0, moduli_ref[0:1, 0:1], jnp.where(phase == 1, moduli_ref[0:1, 1:2], moduli_ref[0:1, 2:3])
    )
    mu_ref[...] = mu
    mu2_ref[...] = mu + mu
    same = (sublane_iota(DEV) == lane_iota(DEV)).astype(jnp.float32).astype(jnp.bfloat16)

    def unpack(k):
        block = recv_ref[pl.ds(k, DEV, stride=CHUNKS), :]
        turned = flip(same, block) if k % 4 == 1 else block.T
        start, stop = k * LANES, min((k + 1) * LANES, CASES * ROWS)
        while start < stop:
            case = start // ROWS
            end = min(stop, (case + 1) * ROWS)
            w_ref[pl.ds((start - case * ROWS) * 8 + case, end - start, stride=8), :] = turned[
                start - k * LANES : end - k * LANES
            ]
            start = end
        return turned

    macro = macro_strain_rows(unpack(CHUNKS - 1))
    for k in range(CHUNKS - 1):
        unpack(k)
    saves[0].start()
    sub = sublane_iota()
    imposed = [
        jnp.where(sub == 0, macro[m], jnp.where(sub == m + 1, 1.0, 0.0)) for m in range(6)
    ]

    def stress_pass(src, strain, keep, energy):
        def plane(a, carry):
            sums, work = list(carry[0]), carry[1]
            base = pl.multiple_of(a * 288, 8)
            ahead = pl.multiple_of(jnp.where(a == R - 1, 0, (a + 1) * 288), 8)
            voxel = a * 36
            line = [[tile_at(src, base, i * VOX + c) for c in range(R)] for i in range(3)]
            for b in range(R):
                nb = (b + 1) % R
                below = [
                    [tile_at(src, base, i * VOX + nb * R + c) for c in range(R)] for i in range(3)
                ]
                for c in range(R):
                    at = b * R + c
                    here = [line[i][c] for i in range(3)]
                    grad = [
                        [
                            tile_at(src, ahead, i * VOX + at) - here[i],
                            below[i][c] - here[i],
                            line[i][(c + 1) % R] - here[i],
                        ]
                        for i in range(3)
                    ]
                    eps = [
                        grad[0][0],
                        grad[1][1],
                        grad[2][2],
                        grad[1][2] + grad[2][1],
                        grad[0][2] + grad[2][0],
                        grad[0][1] + grad[1][0],
                    ]
                    if strain is not None:
                        eps = [eps[m] + strain[m] for m in range(6)]
                    lam = lam_ref[pl.ds(voxel + at, 8, stride=0), :]
                    mu1 = mu_ref[pl.ds(voxel + at, 8, stride=0), :]
                    mu2 = mu2_ref[pl.ds(voxel + at, 8, stride=0), :]
                    bulk = lam * (eps[0] + eps[1] + eps[2])
                    sig = [bulk + mu2 * eps[m] for m in range(3)]
                    sig += [mu1 * eps[m] for m in range(3, 6)]
                    for m in range(6):
                        sums[m] = sums[m] + sig[m]
                        if keep:
                            sig_ref[pl.ds(base + (m * VOX + at) * 8, 8), :] = sig[m]
                    if energy:
                        work = work + (
                            (sig[0] * eps[0] + sig[1] * eps[1])
                            + (sig[2] * eps[2] + sig[3] * eps[3])
                            + (sig[4] * eps[4] + sig[5] * eps[5])
                        )
                line = below
            return tuple(sums), work

        return lax.fori_loop(0, R, plane, ((zero,) * 6, zero), unroll=2)

    def force_pass(src, finish, dst):
        def plane(a, carry):
            totals = list(carry)
            base = pl.multiple_of(a * 288, 8)
            behind = pl.multiple_of(jnp.where(a == 0, (R - 1) * 288, (a - 1) * 288), 8)
            for b in range(R):
                pb = (b + R - 1) % R
                last = [tile_at(sig_ref, base, PAIRS[2][i] * VOX + b * R + R - 1) for i in range(3)]
                for c in range(R):
                    at = b * R + c
                    own = [tile_at(sig_ref, base, m * VOX + at) for m in range(6)]
                    for i in range(3):
                        gone = (own[PAIRS[0][i]] + own[PAIRS[1][i]]) + own[PAIRS[2][i]]
                        come = (
                            tile_at(sig_ref, behind, PAIRS[0][i] * VOX + at)
                            + tile_at(sig_ref, base, PAIRS[1][i] * VOX + pb * R + c)
                        ) + last[i]
                        value = finish(come, gone, tile_at(src, base, i * VOX + at))
                        dst[pl.ds(base + (i * VOX + at) * 8, 8), :] = value
                        totals[i] = totals[i] + value * value
                    last = [own[PAIRS[2][i]] for i in range(3)]
            return tuple(totals)

        totals = lax.fori_loop(0, R, plane, (zero,) * 3, unroll=2)
        return (totals[0] + totals[1]) + totals[2]

    mean0, _ = stress_pass(w_ref, imposed, True, False)
    square0 = force_pass(w_ref, lambda come, gone, w: (gone - come) - STAB * w, p_ref)
    saves[1].start()
    mean1, work1 = stress_pass(p_ref, None, True, True)
    step0 = square0 / (work1 + STAB * square0)
    kept = 1.0 - STAB * step0
    square1 = force_pass(p_ref, lambda come, gone, p: kept * p - step0 * (come - gone), q_ref)
    ratio = square1 / square0

    def direction(a, carry):
        base = pl.multiple_of(a * 288, 8)
        for at in range(36):
            for i in range(3):
                q_ref[pl.ds(base + (i * VOX + at) * 8, 8), :] = tile_at(
                    q_ref, base, i * VOX + at
                ) + ratio * tile_at(p_ref, base, i * VOX + at)
        save_plane(base)
        return carry

    lax.fori_loop(0, R, direction, 0)
    length = square1 + ratio * square1
    mean2, work2 = stress_pass(q_ref, None, False, True)
    step1 = square1 / (work2 + STAB * length)
    step_ref[0:8, :] = step0
    step_ref[8:16, :] = step1
    mean = [(mean0[m] + step0 * mean1[m] + step1 * mean2[m]) * (1.0 / VOX) for m in range(6)]

    shared = place_of(slot_ref[...] >> 7).astype(jnp.float32)
    shared = jnp.broadcast_to(shared, (8, LANES))
    for m in range(6):
        shared = jnp.where(sub == m, mean[m][0:1], shared)
    terms = [mean[m][m + 1 : m + 2] for m in range(6)]
    for first, second in OFF_DIAGONAL:
        terms.append(mean[first][second + 1 : second + 2] + mean[second][first + 1 : first + 2])
    own = jnp.concatenate(terms + [jnp.zeros((1, LANES), jnp.float32)], axis=0)
    left = previous_row_lanes(own)
    stacked = jnp.concatenate(
        [jnp.zeros((64, LANES), jnp.float32), own, left, below_lanes(own), below_lanes(left)],
        axis=0,
    )
    special = stacked.T + node_row(load_ref, scratch, 0)
    for peer in range(DEV):
        ret_ref[8 * peer : 8 * peer + 8, :] = shared
    ret_ref[pl.ds(7, DEV, stride=8), :] = special
    for save in saves:
        save.wait()


def update_kernel(w_ref, p_ref, q_ref, step_ref, out_ref):
    place = place_of(lane_iota(UPDATE))
    for case in range(CASES):
        first = step_ref[case : case + 1, :]
        second = step_ref[8 + case : 9 + case, :]
        rows = pl.ds(case, UPDATE, stride=8)
        value = w_ref[rows, :] + first * p_ref[rows, :] + second * q_ref[rows, :]
        out_ref[case] = jnp.take_along_axis(value, place, axis=1)


def row_of(value, index):
    return jnp.sum(jnp.where(sublane_iota(DEV) == index, value, 0), axis=0, keepdims=True)


def node_tile(row):
    sub = sublane_iota()
    wide = jnp.broadcast_to(row, (8, LANES))
    tile = wide
    for r in range(1, 6):
        tile = jnp.where(sub == r, pltpu.roll(wide, LANES - 8 * r, 1), tile)
    return tile


def final_kernel(
    recv_ref,
    me_ref,
    disp_ref,
    force_ref,
    weight_ref,
    place_ref,
    new_disp_ref,
    res_ref,
    norm_ref,
    scratch,
):
    me = me_ref[...]
    order = recv_ref[pl.ds(6, DEV, stride=8), :].astype(jnp.int32)
    special = recv_ref[pl.ds(7, DEV, stride=8), :]
    stress = [
        jnp.take_along_axis(recv_ref[pl.ds(m, DEV, stride=8), :].T, order, axis=1)
        for m in range(6)
    ]
    parts = split_bf16(jnp.concatenate(stress, axis=1))
    forces = None
    for order_sum in (2, 1, 0):
        for first in range(order_sum + 1):
            product = lax.dot_general(
                parts[first],
                force_ref[order_sum - first],
                (((1,), (0,)), ((), ())),
                preferred_element_type=jnp.float32,
            )
            forces = product if forces is None else forces + product
    home = sublane_iota(DEV)
    upper = forces[:, LANES:]
    lifted = jnp.where(home < 64, pltpu.roll(upper, 68, 0), pltpu.roll(upper, 64, 0))
    lifted = jnp.where(home < 4, 0.0, lifted)
    near = forces[:, :LANES] + lifted
    beside = jnp.where(home % 4 == 0, pltpu.roll(near, DEV - 3, 0), pltpu.roll(near, 1, 0))
    force = near + pltpu.roll(beside, LANES - NODES, 1)
    node = lane_iota(DEV) < NODES
    loads = jnp.where(node, special, 0.0)
    residual = jnp.where(node, special - force, 0.0)
    top = jnp.sum(jnp.sum(residual * residual, axis=0, keepdims=True), axis=1, keepdims=True)
    bottom = jnp.sum(jnp.sum(loads * loads, axis=0, keepdims=True), axis=1, keepdims=True)
    norm_ref[...] = jnp.sqrt(top / bottom)

    own_residual = row_of(residual, me)
    left = jnp.where(me % 4 == 0, me + 3, me - 1)
    under = jnp.where(me >= 64, 64, jnp.where(me < 4, 0, -60))
    turned = special.T
    corners = []
    for k, source in enumerate((me, left, me - under, left - under)):
        picks = jnp.broadcast_to(row_of(order, source), (16, LANES))
        terms = jnp.take_along_axis(turned[64 + 16 * k : 80 + 16 * k], picks, axis=1)
        corner = []
        for i in range(3):
            total = jnp.zeros((8, LANES), jnp.float32)
            for n, (_, _, t) in enumerate(diagonal_terms(i)):
                at = (i * 6 + n) * 8
                total = total + weight_ref[at : at + 8, :] * terms[t : t + 1]
            corner.append(total)
        corners.append(jnp.concatenate(corner, axis=0))
    pieces = split_bf16(jnp.concatenate(corners, axis=1))
    diagonal = jnp.zeros((24, LANES), jnp.float32)
    for piece in pieces:
        diagonal = diagonal + lax.dot_general(
            piece, place_ref[...], (((1,), (0,)), ((), ())), preferred_element_type=jnp.float32
        )
    lane = lane_iota(8)
    same = lane // 16 == sublane_iota()
    row = jnp.zeros((1, LANES), jnp.float32)
    for i in range(3):
        part = jnp.sum(jnp.where(same, diagonal[8 * i : 8 * i + 8], 0.0), axis=0, keepdims=True)
        for shift in (64, 32, 16):
            part = part + pltpu.roll(part, shift, 1)
        row = jnp.where(lane_iota() // 16 == i, part, row)
    moved = node_row(disp_ref, scratch, 0) + own_residual / jnp.maximum(row, FLOOR)
    for value, ref in ((moved, new_disp_ref), (own_residual, res_ref)):
        tile = node_tile(value)
        for i in range(3):
            ref[i, 0] = tile[2 * i : 2 * i + 2, 0:8]


def in_hbm(value):
    return pltpu.with_memory_space_constraint(value, pltpu.HBM)


def exchange(value):
    return lax.all_to_all(value, AXES, split_axis=0, concat_axis=0, tiled=True)


def run_pack(micro_state, state_slot, home_slot, displacement):
    return pl.pallas_call(
        pack_kernel,
        out_shape=jax.ShapeDtypeStruct((DEV * CHUNKS, LANES), jnp.float32),
        in_specs=[HBM] * 4,
        out_specs=VMEM,
        scratch_shapes=[
            pltpu.VMEM((WIDE, LANES), jnp.float32),
            pltpu.VMEM((1, LANES), jnp.int32),
            pltpu.VMEM((1, LANES), jnp.int32),
            pltpu.VMEM(displacement.shape, jnp.float32),
            pltpu.VMEM((8, LANES), jnp.float32),
            pltpu.SemaphoreType.DMA((PARTS + 3,)),
        ],
        compiler_params=pltpu.CompilerParams(vmem_limit_bytes=12 << 20),
        name="pack",
    )(
        in_hbm(micro_state.reshape(CASES * ROWS, LANES)),
        in_hbm(state_slot.reshape(1, LANES)),
        in_hbm(home_slot.reshape(1, LANES)),
        in_hbm(displacement),
    )


def run_solve(received, phases, phase_moduli, home_slot, load):
    f32 = jnp.float32
    big = pltpu.HBM((ROWS * 8, LANES), f32)
    return pl.pallas_call(
        solve_kernel,
        out_shape=(
            jax.ShapeDtypeStruct((DEV * 8, LANES), f32),
            big,
            big,
            big,
            jax.ShapeDtypeStruct((16, LANES), f32),
        ),
        in_specs=[VMEM, VMEM, VMEM, VMEM, VMEM],
        out_specs=[VMEM, HBM, HBM, HBM, VMEM],
        scratch_shapes=[
            pltpu.VMEM((ROWS * 8, LANES), f32),
            pltpu.VMEM((ROWS * 8, LANES), f32),
            pltpu.VMEM((ROWS * 8, LANES), f32),
            pltpu.VMEM((6 * VOX * 8, LANES), f32),
            pltpu.VMEM((VOX, LANES), f32),
            pltpu.VMEM((VOX, LANES), f32),
            pltpu.VMEM((VOX, LANES), f32),
            pltpu.VMEM((8, LANES), f32),
            pltpu.SemaphoreType.DMA((3,)),
        ],
        compiler_params=pltpu.CompilerParams(vmem_limit_bytes=32 << 20),
        name="solve",
    )(received, phases, phase_moduli, home_slot.reshape(1, LANES), load)


def run_update(w, p, q, steps):
    return pl.pallas_call(
        update_kernel,
        out_shape=jax.ShapeDtypeStruct((CASES, ROWS, LANES), jnp.float32),
        grid=(ROWS // UPDATE,),
        in_specs=[pl.BlockSpec((UPDATE * 8, LANES), lambda k: (k, 0))] * 3
        + [pl.BlockSpec((16, LANES), lambda k: (0, 0))],
        out_specs=pl.BlockSpec((CASES, UPDATE, LANES), lambda k: (0, k, 0)),
        compiler_params=pltpu.CompilerParams(vmem_limit_bytes=8 << 20),
        cost_estimate=pl.CostEstimate(
            flops=20_000_000, bytes_accessed=10_000_000, transcendentals=0
        ),
        name="update",
    )(in_hbm(w), in_hbm(p), in_hbm(q), steps)


def run_final(returned, me, displacement):
    force_table, weight_table, place_table = assembly_tables()
    node_shape = jax.ShapeDtypeStruct(displacement.shape, jnp.float32)
    return pl.pallas_call(
        final_kernel,
        out_shape=(node_shape, node_shape, jax.ShapeDtypeStruct((1, 1), jnp.float32)),
        in_specs=[VMEM] * 6,
        out_specs=[VMEM] * 3,
        scratch_shapes=[pltpu.VMEM((8, LANES), jnp.float32)],
        compiler_params=pltpu.CompilerParams(vmem_limit_bytes=12 << 20),
        name="final",
    )(
        returned,
        me,
        displacement,
        jnp.asarray(np.stack(split_table(force_table))),
        jnp.asarray(weight_table),
        jnp.asarray(place_table.reshape(4 * LANES, LANES), jnp.bfloat16),
    )


def per_device(displacement, load, home_slot, micro_state, state_slot, phases, phase_moduli):
    sent = run_pack(micro_state, state_slot, home_slot, displacement)
    received = exchange(sent.reshape(DEV, 1, WIDE)).reshape(DEV * CHUNKS, LANES)
    answer, w, p, q, steps = run_solve(received, phases, phase_moduli, home_slot, load)
    returned = exchange(answer.reshape(DEV, 1, 8 * LANES)).reshape(DEV * 8, LANES)
    new_state = run_update(w, p, q, steps)
    me = jnp.full((1, LANES), lax.axis_index(AXES), jnp.int32)
    displaced, residual, rel_norm = run_final(returned, me, displacement)
    return (
        new_state.reshape(micro_state.shape),
        displaced,
        residual,
        rel_norm.reshape(()),
    )


def solution(mesh):
    split = Mesh(mesh.devices.reshape(-1, 2, mesh.shape["rve"]), SPLIT)
    return jax.shard_map(
        per_device,
        mesh=split,
        in_specs=(
            P(None, SUB, "rve", None),
            P(None, SUB, "rve", None),
            P(SPLIT),
            P(None, None, None, SPLIT),
            P(SPLIT),
            P(None, SPLIT),
            P(),
        ),
        out_specs=(
            P(None, None, None, SPLIT),
            P(None, SUB, "rve", None),
            P(None, SUB, "rve", None),
            P(),
        ),
        check_vma=False,
    )
```

```python
import math

import jax
import jax.numpy as jnp
import numpy as np
from jax import lax
from jax.experimental import pallas as pl
from jax.experimental.pallas import tpu as pltpu
from jax.sharding import Mesh
from jax.sharding import PartitionSpec as P

R = 6
VOX = R * R * R
ROWS = 3 * VOX
CASES = 7
DEV = 128
LANES = 128
CHUNKS = 36
WIDE = CHUNKS * LANES
TAIL = CASES * ROWS - (CHUNKS - 1) * LANES
NODES = 48
STAB = 0.1
FLOOR = 1.0
SPLIT = ("far", "core", "rve")
AXES = ("core", "far", "rve")
SUB = ("far", "core")
PAIRS = ((0, 5, 4), (5, 1, 3), (4, 3, 2))
STRAIN_OF = ((0, 4, 5), (5, 1, 3), (4, 3, 2))
OFF_DIAGONAL = ((0, 4), (0, 5), (4, 5), (1, 3), (1, 5), (3, 5), (2, 3), (2, 4), (3, 4))
LOW = 0.5 - 0.5 / math.sqrt(3.0)
HIGH = 0.5 + 0.5 / math.sqrt(3.0)
HIGHEST = lax.Precision.HIGHEST
VMEM = pl.BlockSpec(memory_space=pltpu.VMEM)
SMEM = pl.BlockSpec(memory_space=pltpu.SMEM)
HBM = pl.BlockSpec(memory_space=pltpu.HBM)
CUTS = (0, 4, 36)
PARTS = len(CUTS) - 1
STEP = 4
UPDATE = 72


def strain_table():
    places = (LOW, HIGH)
    table = np.zeros((8, 8, 3, 6))
    for gauss in range(8):
        at = (places[gauss % 2], places[gauss // 2 % 2], places[gauss // 4])
        for corner in range(8):
            bits = (corner % 2, corner // 2 % 2, corner // 4)
            weight = [at[k] if bits[k] else 1.0 - at[k] for k in range(3)]
            sign = [1.0 if bits[k] else -1.0 for k in range(3)]
            dx = sign[0] * weight[1] * weight[2]
            dy = weight[0] * sign[1] * weight[2]
            dz = weight[0] * weight[1] * sign[2]
            table[gauss, corner, 0, [0, 4, 5]] = (dx, dz, dy)
            table[gauss, corner, 1, [1, 3, 5]] = (dy, dz, dx)
            table[gauss, corner, 2, [2, 3, 4]] = (dz, dy, dx)
    return table


def term_index(first, second):
    if first == second:
        return first
    return 6 + OFF_DIAGONAL.index((min(first, second), max(first, second)))


def diagonal_terms(component):
    m = STRAIN_OF[component]
    pairs = [(m[0], m[0]), (m[1], m[1]), (m[2], m[2]), (m[0], m[1]), (m[0], m[2]), (m[1], m[2])]
    return [(a, b, term_index(a, b)) for a, b in pairs]


def assembly_tables():
    table = strain_table()
    force = np.zeros((6, LANES, 2 * LANES), np.float32)
    weights = np.zeros((3, 6, 8, LANES), np.float32)
    place = np.zeros((4, LANES, LANES), np.float32)
    for j in range(LANES):
        ly, ex, gauss = j // 64, j // 8 % 8, j % 8
        for corner in range(8):
            az, row, col = corner // 4, ly + corner // 2 % 2, (ex + corner % 2) % 8
            for i in range(3):
                lane = az * LANES + (NODES if row == 2 else 0) + i * 16 + row % 2 * 8 + col
                for m in STRAIN_OF[i]:
                    force[m, j, lane] += 0.125 * table[gauss, corner, i, m]
                for n, (first, second, _) in enumerate(diagonal_terms(i)):
                    weights[i, n, corner, j] = (
                        0.125 * table[gauss, corner, i, first] * table[gauss, corner, i, second]
                    )
            place[az * 2 + (1 if row == 2 else 0), j, corner * 16 + row % 2 * 8 + col] = 1.0
    return force.reshape(6 * LANES, 2 * LANES), weights.reshape(18 * 8, LANES), place


def split_table(table):
    high = table.astype(jnp.bfloat16)
    rest = table - high.astype(np.float32)
    middle = rest.astype(jnp.bfloat16)
    return high, middle, (rest - middle.astype(np.float32)).astype(jnp.bfloat16)


def lane_iota(rows=1):
    return lax.broadcasted_iota(jnp.int32, (rows, LANES), 1)


def sublane_iota(rows=8):
    return lax.broadcasted_iota(jnp.int32, (rows, LANES), 0)


def node_row(ref, scratch, offset):
    scratch[...] = jnp.zeros((8, LANES), jnp.float32)
    for i in range(3):
        scratch[2 * i : 2 * i + 2, 0:8] = ref[i, 0]
    tile = scratch[...]
    total = jnp.zeros((1, LANES), jnp.float32)
    for row in range(6):
        total = total + pltpu.roll(tile[row : row + 1], offset + 8 * row, 1)
    return total


def previous_row_lanes(value):
    lane = lane_iota(value.shape[0])
    return jnp.where(lane % 4 == 0, pltpu.roll(value, LANES - 3, 1), pltpu.roll(value, 1, 1))


def next_row_lanes(value):
    lane = lane_iota(value.shape[0])
    return jnp.where(lane % 4 == 3, pltpu.roll(value, 3, 1), pltpu.roll(value, LANES - 1, 1))


def below_lanes(value):
    lane = lane_iota(value.shape[0])
    moved = jnp.where(lane < 64, pltpu.roll(value, 68, 1), pltpu.roll(value, 64, 1))
    return jnp.where(lane < 4, 0.0, moved)


def above_lanes(value):
    lane = lane_iota(value.shape[0])
    moved = jnp.where(lane < 64, pltpu.roll(value, 64, 1), pltpu.roll(value, 60, 1))
    return jnp.where(lane >= 124, 0.0, moved)


def device_at(place):
    return ((place >> 2) & 15) * 8 + (place >> 6) * 4 + (place & 3)


def place_of(device):
    return ((device >> 2) & 1) * 64 + (device >> 3) * 4 + (device & 3)


def part_copy(src, dst, sems, part):
    start, stop = CUTS[part] * LANES, min(CUTS[part + 1] * LANES, CASES * ROWS)
    rows = pl.ds(start, stop - start)
    return pltpu.make_async_copy(src.at[rows], dst.at[rows], sems.at[part])


def split_bf16(value):
    high = value.astype(jnp.bfloat16)
    rest = value - high.astype(jnp.float32)
    middle = rest.astype(jnp.bfloat16)
    low = (rest - middle.astype(jnp.float32)).astype(jnp.bfloat16)
    return high, middle, low


def flip(same, block):
    high, middle, low = (
        lax.dot_general(
            same, part, (((1,), (1,)), ((), ())), preferred_element_type=jnp.float32
        )
        for part in split_bf16(block)
    )
    return (high + middle) + low


def pack_kernel(
    state_ref,
    state_slot_hbm,
    home_slot_hbm,
    disp_hbm,
    out_ref,
    held_ref,
    state_slot_ref,
    home_slot_ref,
    disp_ref,
    scratch,
    sems,
):
    small = [
        pltpu.make_async_copy(src, dst, sems.at[PARTS + k])
        for k, (src, dst) in enumerate(
            (
                (state_slot_hbm, state_slot_ref),
                (home_slot_hbm, home_slot_ref),
                (disp_hbm, disp_ref),
            )
        )
    ]
    for copy in small:
        copy.start()
    for part in range(PARTS):
        part_copy(state_ref, held_ref, sems, part).start()
    owner = device_at(sublane_iota(DEV))
    lane = lane_iota(DEV)
    for copy in small:
        copy.wait()
    choose = ((state_slot_ref[...] >> 7) == owner).astype(jnp.float32).astype(jnp.bfloat16)
    twice = jnp.concatenate([choose, choose], axis=1)
    home = (home_slot_ref[...] >> 7) == owner
    local = jnp.sum(jnp.where(home, lane, 0).astype(jnp.float32), axis=1, keepdims=True)
    extra = node_row(disp_ref, scratch, TAIL) + jnp.where(lane == TAIL + NODES, local, 0.0)
    held_ref[CASES * ROWS :, :] = jnp.zeros((WIDE - CASES * ROWS, LANES), jnp.float32)
    for part in range(PARTS):
        part_copy(state_ref, held_ref, sems, part).wait()
        for first in range(CUTS[part], CUTS[part + 1], STEP):
            high, middle, low = split_bf16(held_ref[first * LANES : (first + STEP) * LANES, :])
            picked = lax.dot_general(
                jnp.concatenate([high, middle], axis=1),
                twice,
                (((1,), (1,)), ((), ())),
                preferred_element_type=jnp.float32,
            )
            picked = picked + lax.dot_general(
                low, choose, (((1,), (1,)), ((), ())), preferred_element_type=jnp.float32
            )
            for k in range(first, first + STEP):
                turned = picked[(k - first) * LANES : (k - first + 1) * LANES].T
                if k == CHUNKS - 1:
                    turned = turned + extra
                out_ref[pl.ds(k, DEV, stride=CHUNKS), :] = turned


def macro_strain_rows(tail):
    local = tail[TAIL + NODES : TAIL + NODES + 1].astype(jnp.int32)
    upper = (local >> 6) == 1
    ex = (local >> 3) & 7
    point = [jnp.where(((local >> k) & 1) == 1, HIGH, LOW) for k in range(3)]
    shape = [(1.0 - point[k], point[k]) for k in range(3)]
    sub = sublane_iota()
    hits = (sub == ex, sub == ((ex + 1) & 7))
    slopes = []
    for i in range(3):
        own = [tail[TAIL + 16 * i + 8 * y : TAIL + 16 * i + 8 * y + 8] for y in range(2)]
        rows = [own[0], own[1], next_row_lanes(own[0])]
        planes = [rows, [above_lanes(row) for row in rows]]
        at = {}
        for az in range(2):
            for ay in range(2):
                chosen = jnp.where(upper, planes[az][ay + 1], planes[az][ay])
                for ax in range(2):
                    at[az, ay, ax] = jnp.sum(
                        jnp.where(hits[ax], chosen, 0.0), axis=0, keepdims=True
                    )
        sx, sy, sz = shape
        slope = [0.0, 0.0, 0.0]
        for first in range(2):
            for second in range(2):
                slope[0] = slope[0] + sz[first] * sy[second] * (
                    at[first, second, 1] - at[first, second, 0]
                )
                slope[1] = slope[1] + sz[first] * sx[second] * (
                    at[first, 1, second] - at[first, 0, second]
                )
                slope[2] = slope[2] + sy[first] * sx[second] * (
                    at[1, first, second] - at[0, first, second]
                )
        slopes.append(slope)
    return [
        slopes[0][0],
        slopes[1][1],
        slopes[2][2],
        slopes[1][2] + slopes[2][1],
        slopes[0][2] + slopes[2][0],
        slopes[0][1] + slopes[1][0],
    ]


def tile_at(ref, base, row):
    return ref[pl.ds(base + row * 8, 8), :]


def solve_kernel(
    recv_ref,
    phase_ref,
    moduli_ref,
    slot_ref,
    load_ref,
    ret_ref,
    w_out,
    p_out,
    q_out,
    step_ref,
    w_ref,
    p_ref,
    q_ref,
    sig_ref,
    lam_ref,
    mu_ref,
    mu2_ref,
    scratch,
    sems,
):
    saves = [
        pltpu.make_async_copy(src, dst, sems.at[k])
        for k, (src, dst) in enumerate(((w_ref, w_out), (p_ref, p_out), (q_ref, q_out)))
    ]

    def save_plane(base):
        for i in range(3):
            rows = pl.ds(base + i * VOX * 8, 288)
            pltpu.make_async_copy(q_ref.at[rows], q_out.at[rows], sems.at[2]).start()

    zero = jnp.zeros((8, LANES), jnp.float32)
    phase = jnp.take_along_axis(phase_ref[...], device_at(lane_iota(VOX)), axis=1)
    mu = jnp.where(
        phase == 0, moduli_ref[1:2, 0:1], jnp.where(phase == 1, moduli_ref[1:2, 1:2], moduli_ref[1:2, 2:3])
    )
    lam_ref[...] = jnp.where(
        phase == 0, moduli_ref[0:1, 0:1], jnp.where(phase == 1, moduli_ref[0:1, 1:2], moduli_ref[0:1, 2:3])
    )
    mu_ref[...] = mu
    mu2_ref[...] = mu + mu
    same = (sublane_iota(DEV) == lane_iota(DEV)).astype(jnp.float32).astype(jnp.bfloat16)

    def unpack(k):
        block = recv_ref[pl.ds(k, DEV, stride=CHUNKS), :]
        turned = flip(same, block) if k % 4 == 1 else block.T
        start, stop = k * LANES, min((k + 1) * LANES, CASES * ROWS)
        while start < stop:
            case = start // ROWS
            end = min(stop, (case + 1) * ROWS)
            w_ref[pl.ds((start - case * ROWS) * 8 + case, end - start, stride=8), :] = turned[
                start - k * LANES : end - k * LANES
            ]
            start = end
        return turned

    macro = macro_strain_rows(unpack(CHUNKS - 1))
    for k in range(CHUNKS - 1):
        unpack(k)
    saves[0].start()
    sub = sublane_iota()
    imposed = [
        jnp.where(sub == 0, macro[m], jnp.where(sub == m + 1, 1.0, 0.0)) for m in range(6)
    ]

    def stress_pass(src, strain, keep, energy):
        def plane(a, carry):
            sums, work = list(carry[0]), carry[1]
            base = pl.multiple_of(a * 288, 8)
            ahead = pl.multiple_of(jnp.where(a == R - 1, 0, (a + 1) * 288), 8)
            voxel = a * 36
            line = [[tile_at(src, base, i * VOX + c) for c in range(R)] for i in range(3)]
            for b in range(R):
                nb = (b + 1) % R
                below = [
                    [tile_at(src, base, i * VOX + nb * R + c) for c in range(R)] for i in range(3)
                ]
                for c in range(R):
                    at = b * R + c
                    here = [line[i][c] for i in range(3)]
                    grad = [
                        [
                            tile_at(src, ahead, i * VOX + at) - here[i],
                            below[i][c] - here[i],
                            line[i][(c + 1) % R] - here[i],
                        ]
                        for i in range(3)
                    ]
                    eps = [
                        grad[0][0],
                        grad[1][1],
                        grad[2][2],
                        grad[1][2] + grad[2][1],
                        grad[0][2] + grad[2][0],
                        grad[0][1] + grad[1][0],
                    ]
                    if strain is not None:
                        eps = [eps[m] + strain[m] for m in range(6)]
                    lam = lam_ref[pl.ds(voxel + at, 8, stride=0), :]
                    mu1 = mu_ref[pl.ds(voxel + at, 8, stride=0), :]
                    mu2 = mu2_ref[pl.ds(voxel + at, 8, stride=0), :]
                    bulk = lam * (eps[0] + eps[1] + eps[2])
                    sig = [bulk + mu2 * eps[m] for m in range(3)]
                    sig += [mu1 * eps[m] for m in range(3, 6)]
                    for m in range(6):
                        sums[m] = sums[m] + sig[m]
                        if keep:
                            sig_ref[pl.ds(base + (m * VOX + at) * 8, 8), :] = sig[m]
                    if energy:
                        work = work + (
                            (sig[0] * eps[0] + sig[1] * eps[1])
                            + (sig[2] * eps[2] + sig[3] * eps[3])
                            + (sig[4] * eps[4] + sig[5] * eps[5])
                        )
                line = below
            return tuple(sums), work

        return lax.fori_loop(0, R, plane, ((zero,) * 6, zero), unroll=3)

    def force_pass(src, finish, dst):
        def plane(a, carry):
            totals = list(carry)
            base = pl.multiple_of(a * 288, 8)
            behind = pl.multiple_of(jnp.where(a == 0, (R - 1) * 288, (a - 1) * 288), 8)
            for b in range(R):
                pb = (b + R - 1) % R
                last = [tile_at(sig_ref, base, PAIRS[2][i] * VOX + b * R + R - 1) for i in range(3)]
                for c in range(R):
                    at = b * R + c
                    own = [tile_at(sig_ref, base, m * VOX + at) for m in range(6)]
                    for i in range(3):
                        gone = (own[PAIRS[0][i]] + own[PAIRS[1][i]]) + own[PAIRS[2][i]]
                        come = (
                            tile_at(sig_ref, behind, PAIRS[0][i] * VOX + at)
                            + tile_at(sig_ref, base, PAIRS[1][i] * VOX + pb * R + c)
                        ) + last[i]
                        value = finish(come, gone, tile_at(src, base, i * VOX + at))
                        dst[pl.ds(base + (i * VOX + at) * 8, 8), :] = value
                        totals[i] = totals[i] + value * value
                    last = [own[PAIRS[2][i]] for i in range(3)]
            return tuple(totals)

        totals = lax.fori_loop(0, R, plane, (zero,) * 3, unroll=3)
        return (totals[0] + totals[1]) + totals[2]

    mean0, _ = stress_pass(w_ref, imposed, True, False)
    square0 = force_pass(w_ref, lambda come, gone, w: (gone - come) - STAB * w, p_ref)
    saves[1].start()
    mean1, work1 = stress_pass(p_ref, None, True, True)
    step0 = square0 / (work1 + STAB * square0)
    kept = 1.0 - STAB * step0
    square1 = force_pass(p_ref, lambda come, gone, p: kept * p - step0 * (come - gone), q_ref)
    ratio = square1 / square0

    def direction(a, carry):
        base = pl.multiple_of(a * 288, 8)
        for at in range(36):
            for i in range(3):
                q_ref[pl.ds(base + (i * VOX + at) * 8, 8), :] = tile_at(
                    q_ref, base, i * VOX + at
                ) + ratio * tile_at(p_ref, base, i * VOX + at)
        save_plane(base)
        return carry

    lax.fori_loop(0, R, direction, 0, unroll=3)
    length = square1 + ratio * square1
    mean2, work2 = stress_pass(q_ref, None, False, True)
    step1 = square1 / (work2 + STAB * length)
    step_ref[0:8, :] = step0
    step_ref[8:16, :] = step1
    mean = [(mean0[m] + step0 * mean1[m] + step1 * mean2[m]) * (1.0 / VOX) for m in range(6)]

    shared = place_of(slot_ref[...] >> 7).astype(jnp.float32)
    shared = jnp.broadcast_to(shared, (8, LANES))
    for m in range(6):
        shared = jnp.where(sub == m, mean[m][0:1], shared)
    terms = [mean[m][m + 1 : m + 2] for m in range(6)]
    for first, second in OFF_DIAGONAL:
        terms.append(mean[first][second + 1 : second + 2] + mean[second][first + 1 : first + 2])
    own = jnp.concatenate(terms + [jnp.zeros((1, LANES), jnp.float32)], axis=0)
    left = previous_row_lanes(own)
    stacked = jnp.concatenate(
        [jnp.zeros((64, LANES), jnp.float32), own, left, below_lanes(own), below_lanes(left)],
        axis=0,
    )
    special = stacked.T + node_row(load_ref, scratch, 0)
    for peer in range(DEV):
        ret_ref[8 * peer : 8 * peer + 8, :] = shared
    ret_ref[pl.ds(7, DEV, stride=8), :] = special
    for save in saves:
        save.wait()


def update_kernel(w_ref, p_ref, q_ref, step_ref, out_ref):
    place = place_of(lane_iota(UPDATE))
    for case in range(CASES):
        first = step_ref[case : case + 1, :]
        second = step_ref[8 + case : 9 + case, :]
        rows = pl.ds(case, UPDATE, stride=8)
        value = w_ref[rows, :] + first * p_ref[rows, :] + second * q_ref[rows, :]
        out_ref[case] = jnp.take_along_axis(value, place, axis=1)


def row_of(value, index):
    return jnp.sum(jnp.where(sublane_iota(DEV) == index, value, 0), axis=0, keepdims=True)


def node_tile(row):
    sub = sublane_iota()
    wide = jnp.broadcast_to(row, (8, LANES))
    tile = wide
    for r in range(1, 6):
        tile = jnp.where(sub == r, pltpu.roll(wide, LANES - 8 * r, 1), tile)
    return tile


def final_kernel(
    recv_ref,
    me_ref,
    disp_ref,
    force_ref,
    weight_ref,
    place_ref,
    new_disp_ref,
    res_ref,
    norm_ref,
    scratch,
):
    me = me_ref[...]
    order = recv_ref[pl.ds(6, DEV, stride=8), :].astype(jnp.int32)
    special = recv_ref[pl.ds(7, DEV, stride=8), :]
    stress = [
        jnp.take_along_axis(recv_ref[pl.ds(m, DEV, stride=8), :].T, order, axis=1)
        for m in range(6)
    ]
    parts = split_bf16(jnp.concatenate(stress, axis=1))
    forces = None
    for order_sum in (2, 1, 0):
        for first in range(order_sum + 1):
            product = lax.dot_general(
                parts[first],
                force_ref[order_sum - first],
                (((1,), (0,)), ((), ())),
                preferred_element_type=jnp.float32,
            )
            forces = product if forces is None else forces + product
    home = sublane_iota(DEV)
    upper = forces[:, LANES:]
    lifted = jnp.where(home < 64, pltpu.roll(upper, 68, 0), pltpu.roll(upper, 64, 0))
    lifted = jnp.where(home < 4, 0.0, lifted)
    near = forces[:, :LANES] + lifted
    beside = jnp.where(home % 4 == 0, pltpu.roll(near, DEV - 3, 0), pltpu.roll(near, 1, 0))
    force = near + pltpu.roll(beside, LANES - NODES, 1)
    node = lane_iota(DEV) < NODES
    loads = jnp.where(node, special, 0.0)
    residual = jnp.where(node, special - force, 0.0)
    top = jnp.sum(jnp.sum(residual * residual, axis=0, keepdims=True), axis=1, keepdims=True)
    bottom = jnp.sum(jnp.sum(loads * loads, axis=0, keepdims=True), axis=1, keepdims=True)
    norm_ref[...] = jnp.sqrt(top / bottom)

    own_residual = row_of(residual, me)
    left = jnp.where(me % 4 == 0, me + 3, me - 1)
    under = jnp.where(me >= 64, 64, jnp.where(me < 4, 0, -60))
    turned = special.T
    corners = []
    for k, source in enumerate((me, left, me - under, left - under)):
        picks = jnp.broadcast_to(row_of(order, source), (16, LANES))
        terms = jnp.take_along_axis(turned[64 + 16 * k : 80 + 16 * k], picks, axis=1)
        corner = []
        for i in range(3):
            total = jnp.zeros((8, LANES), jnp.float32)
            for n, (_, _, t) in enumerate(diagonal_terms(i)):
                at = (i * 6 + n) * 8
                total = total + weight_ref[at : at + 8, :] * terms[t : t + 1]
            corner.append(total)
        corners.append(jnp.concatenate(corner, axis=0))
    pieces = split_bf16(jnp.concatenate(corners, axis=1))
    diagonal = jnp.zeros((24, LANES), jnp.float32)
    for piece in pieces:
        diagonal = diagonal + lax.dot_general(
            piece, place_ref[...], (((1,), (0,)), ((), ())), preferred_element_type=jnp.float32
        )
    lane = lane_iota(8)
    same = lane // 16 == sublane_iota()
    row = jnp.zeros((1, LANES), jnp.float32)
    for i in range(3):
        part = jnp.sum(jnp.where(same, diagonal[8 * i : 8 * i + 8], 0.0), axis=0, keepdims=True)
        for shift in (64, 32, 16):
            part = part + pltpu.roll(part, shift, 1)
        row = jnp.where(lane_iota() // 16 == i, part, row)
    moved = node_row(disp_ref, scratch, 0) + own_residual / jnp.maximum(row, FLOOR)
    for value, ref in ((moved, new_disp_ref), (own_residual, res_ref)):
        tile = node_tile(value)
        for i in range(3):
            ref[i, 0] = tile[2 * i : 2 * i + 2, 0:8]


def in_hbm(value):
    return pltpu.with_memory_space_constraint(value, pltpu.HBM)


def exchange(value):
    return lax.all_to_all(value, AXES, split_axis=0, concat_axis=0, tiled=True)


def run_pack(micro_state, state_slot, home_slot, displacement):
    return pl.pallas_call(
        pack_kernel,
        out_shape=jax.ShapeDtypeStruct((DEV * CHUNKS, LANES), jnp.float32),
        in_specs=[HBM] * 4,
        out_specs=VMEM,
        scratch_shapes=[
            pltpu.VMEM((WIDE, LANES), jnp.float32),
            pltpu.VMEM((1, LANES), jnp.int32),
            pltpu.VMEM((1, LANES), jnp.int32),
            pltpu.VMEM(displacement.shape, jnp.float32),
            pltpu.VMEM((8, LANES), jnp.float32),
            pltpu.SemaphoreType.DMA((PARTS + 3,)),
        ],
        compiler_params=pltpu.CompilerParams(vmem_limit_bytes=12 << 20),
        name="pack",
    )(
        in_hbm(micro_state.reshape(CASES * ROWS, LANES)),
        in_hbm(state_slot.reshape(1, LANES)),
        in_hbm(home_slot.reshape(1, LANES)),
        in_hbm(displacement),
    )


def run_solve(received, phases, phase_moduli, home_slot, load):
    f32 = jnp.float32
    big = pltpu.HBM((ROWS * 8, LANES), f32)
    return pl.pallas_call(
        solve_kernel,
        out_shape=(
            jax.ShapeDtypeStruct((DEV * 8, LANES), f32),
            big,
            big,
            big,
            jax.ShapeDtypeStruct((16, LANES), f32),
        ),
        in_specs=[VMEM, VMEM, VMEM, VMEM, VMEM],
        out_specs=[VMEM, HBM, HBM, HBM, VMEM],
        scratch_shapes=[
            pltpu.VMEM((ROWS * 8, LANES), f32),
            pltpu.VMEM((ROWS * 8, LANES), f32),
            pltpu.VMEM((ROWS * 8, LANES), f32),
            pltpu.VMEM((6 * VOX * 8, LANES), f32),
            pltpu.VMEM((VOX, LANES), f32),
            pltpu.VMEM((VOX, LANES), f32),
            pltpu.VMEM((VOX, LANES), f32),
            pltpu.VMEM((8, LANES), f32),
            pltpu.SemaphoreType.DMA((3,)),
        ],
        compiler_params=pltpu.CompilerParams(vmem_limit_bytes=32 << 20),
        name="solve",
    )(received, phases, phase_moduli, home_slot.reshape(1, LANES), load)


def run_update(w, p, q, steps):
    return pl.pallas_call(
        update_kernel,
        out_shape=jax.ShapeDtypeStruct((CASES, ROWS, LANES), jnp.float32),
        grid=(ROWS // UPDATE,),
        in_specs=[pl.BlockSpec((UPDATE * 8, LANES), lambda k: (k, 0))] * 3
        + [pl.BlockSpec((16, LANES), lambda k: (0, 0))],
        out_specs=pl.BlockSpec((CASES, UPDATE, LANES), lambda k: (0, k, 0)),
        compiler_params=pltpu.CompilerParams(vmem_limit_bytes=8 << 20),
        cost_estimate=pl.CostEstimate(
            flops=20_000_000, bytes_accessed=10_000_000, transcendentals=0
        ),
        name="update",
    )(in_hbm(w), in_hbm(p), in_hbm(q), steps)


def run_final(returned, me, displacement):
    force_table, weight_table, place_table = assembly_tables()
    node_shape = jax.ShapeDtypeStruct(displacement.shape, jnp.float32)
    return pl.pallas_call(
        final_kernel,
        out_shape=(node_shape, node_shape, jax.ShapeDtypeStruct((1, 1), jnp.float32)),
        in_specs=[VMEM] * 6,
        out_specs=[VMEM] * 3,
        scratch_shapes=[pltpu.VMEM((8, LANES), jnp.float32)],
        compiler_params=pltpu.CompilerParams(vmem_limit_bytes=12 << 20),
        name="final",
    )(
        returned,
        me,
        displacement,
        jnp.asarray(np.stack(split_table(force_table))),
        jnp.asarray(weight_table),
        jnp.asarray(place_table.reshape(4 * LANES, LANES), jnp.bfloat16),
    )


def per_device(displacement, load, home_slot, micro_state, state_slot, phases, phase_moduli):
    sent = run_pack(micro_state, state_slot, home_slot, displacement)
    received = exchange(sent.reshape(DEV, 1, WIDE)).reshape(DEV * CHUNKS, LANES)
    answer, w, p, q, steps = run_solve(received, phases, phase_moduli, home_slot, load)
    returned = exchange(answer.reshape(DEV, 1, 8 * LANES)).reshape(DEV * 8, LANES)
    new_state = run_update(w, p, q, steps)
    me = jnp.full((1, LANES), lax.axis_index(AXES), jnp.int32)
    displaced, residual, rel_norm = run_final(returned, me, displacement)
    return (
        new_state.reshape(micro_state.shape),
        displaced,
        residual,
        rel_norm.reshape(()),
    )


def solution(mesh):
    split = Mesh(mesh.devices.reshape(-1, 2, mesh.shape["rve"]), SPLIT)
    return jax.shard_map(
        per_device,
        mesh=split,
        in_specs=(
            P(None, SUB, "rve", None),
            P(None, SUB, "rve", None),
            P(SPLIT),
            P(None, None, None, SPLIT),
            P(SPLIT),
            P(None, SPLIT),
            P(),
        ),
        out_specs=(
            P(None, None, None, SPLIT),
            P(None, SUB, "rve", None),
            P(None, SUB, "rve", None),
            P(),
        ),
        check_vma=False,
    )
```
